32 devices in a mesh: tm: 4 (over y, x), space: 8 (over z, core).
Axes of the slice: x: 2, y: 2, z: 4, core: 2. Of those that a mesh axis runs over, the one named last changes fastest.
Arguments:
- residual: float32 [64, 64, 8, 128], P('tm', 'space'), may hold values from -24 to 24
- capacity: float32 [64, 8, 128], P('space'), may hold values from 0.25 to 4
Outputs:
- preconditioned: float32 [64, 64, 8, 128], P('tm', 'space')
The draws below stay inside these ranges and needn't reach their ends.
All inputs are finite; a program needn't handle non-finite values.
Results may differ from the reference program's by a relative error of at most 0.0003.
Values sent between devices are 32-bit elements; how exact they have to be, the bound alone decides.
A program may use at most 64 MiB of HBM per device.

```python
import math
import jax
import jax.numpy as jnp
from jax import lax

NY = 8
NZ = 128
TSTEPS = 64
GRID_DEPTH = 4
SMOOTH = 2
COARSE_SWEEPS = 6
NX = 64


def draw_residual(key, part):
    extents = (TSTEPS, NX, NY, NZ)
    return jnp.clip(4.0 * jax.random.normal(jax.random.fold_in(key, 11), extents, jnp.float32), -24.0, 24.0)


def levels(stream_key, shape, shards, smallest, high):
    loudness = 1.0
    for dim, parts in shards:
        steps = jax.random.uniform(jax.random.fold_in(jax.random.fold_in(stream_key, 6), dim), (parts,), jnp.float32, smallest / len(shards), high / len(shards))
        loudness = loudness * jnp.repeat(jnp.exp(steps), shape[dim] // parts).reshape((-1,) + (1,) * (len(shape) - 1 - dim))
    return loudness


def setup_inputs(seed: int = 0) -> dict:
    arg_keys = jax.random.split(jax.random.key(seed), 3)
    return {
        "residual": draw_residual(jax.random.fold_in(arg_keys[2], 71), 0),
        "capacity": jnp.clip(jnp.exp(math.log(4.0) - 2.7725887 * jax.random.uniform(arg_keys[1], (NX, NY, NZ), jnp.float32) ** levels(arg_keys[1], (NX, NY, NZ), ((0, 8),), -0.2, 0.2)), 0.25, 4.0),
    }


ALPHA_CORNER = 0.01
STEP_SIZE = 0.5
DIFFUSE = 2.0
ADVECT = (0.2, -0.15, 0.1)
OMEGA = 0.7
HIGHEST = lax.Precision.HIGHEST


def level_coefficients(per_level_values):
    spread = DIFFUSE / 4.0 ** per_level_values
    drifts = tuple(component / 2.0 ** per_level_values for component in ADVECT)
    return spread, drifts


def pad_second(volume, position):
    widths = [(0, 0)] * volume.ndim
    widths[position] = (1, 1)
    return jnp.pad(volume, widths)


def apply_operator(padded, current_capacity, spectral_shifts, per_level_values):
    spread, drifts = level_coefficients(per_level_values)
    centre = padded[:, :, 1:-1]
    upper_first = padded[:, :, 2:]
    lower_first = padded[:, :, :-2]
    wide_second = pad_second(centre, 3)
    upper_second = wide_second[:, :, :, 2:]
    lower_second = wide_second[:, :, :, :-2]
    wide_third = pad_second(centre, 4)
    upper_third = wide_third[:, :, :, :, 2:]
    lower_third = wide_third[:, :, :, :, :-2]
    stencil = spread * (6.0 * centre - upper_first - lower_first - upper_second - lower_second - upper_third - lower_third)
    stencil = stencil + drifts[0] * (upper_first - lower_first) + drifts[1] * (upper_second - lower_second) + drifts[2] * (upper_third - lower_third)
    first_shift, second_shift, third_shift = spectral_shifts
    real_part = centre[0]
    imag_part = centre[1]
    shifted = jnp.stack([current_capacity * (first_shift * real_part - second_shift * imag_part), current_capacity * (second_shift * real_part + third_shift * imag_part)])
    return stencil + shifted


def inverse_diagonal(current_capacity, spectral_shifts, per_level_values):
    spread, drifts = level_coefficients(per_level_values)
    first_shift, second_shift, third_shift = spectral_shifts
    top_left = current_capacity * first_shift + 6.0 * spread
    coupling = current_capacity * second_shift
    bottom_right = current_capacity * third_shift + 6.0 * spread
    determinant = top_left * bottom_right + coupling * coupling
    return bottom_right / determinant, coupling / determinant, top_left / determinant


def damped_update(residual_now, inverse):
    diagonal_a, diagonal_b, diagonal_c = inverse
    return OMEGA * jnp.stack([diagonal_a * residual_now[0] + diagonal_b * residual_now[1], diagonal_c * residual_now[1] - diagonal_b * residual_now[0]])


def restrict_to_coarse(volume):
    leading = volume.shape[:-3]
    first_extent, second_extent, third_extent = volume.shape[-3:]
    blocks = volume.reshape(leading + (first_extent // 2, 2, second_extent // 2, 2, third_extent // 2, 2))
    lead_count = len(leading)
    return jnp.mean(blocks, axis=(lead_count + 1, lead_count + 3, lead_count + 5))


def prolong_cells(volume):
    leading = volume.shape[:-3]
    first_extent, second_extent, third_extent = volume.shape[-3:]
    expanded = jnp.broadcast_to(volume[..., :, None, :, None, :, None], leading + (first_extent, 2, second_extent, 2, third_extent, 2))
    return expanded.reshape(leading + (2 * first_extent, 2 * second_extent, 2 * third_extent))


def shift_values(frequency, length):
    ratio_step = ALPHA_CORNER ** (1.0 / length)
    phases = (2.0 * math.pi / length) * frequency.astype(jnp.float32)
    first_shift = (1.0 - ratio_step * jnp.cos(phases)) / STEP_SIZE
    second_shift = ratio_step * jnp.sin(phases) / STEP_SIZE
    return tuple(column.reshape(-1, 1, 1, 1) for column in (first_shift, second_shift, first_shift))


def multigrid_cycle(per_level_values, forcing_term, capacity_fields, spectral_shifts):
    current_capacity = capacity_fields[per_level_values]
    inverse = inverse_diagonal(current_capacity, spectral_shifts, per_level_values)
    coarsest = per_level_values == GRID_DEPTH - 1
    current = damped_update(forcing_term, inverse)
    for repeat in range((COARSE_SWEEPS if coarsest else SMOOTH) - 1):
        current = current + damped_update(forcing_term - apply_operator(pad_second(current, 2), current_capacity, spectral_shifts, per_level_values), inverse)
    if coarsest:
        return current
    coarse_right_hand = restrict_to_coarse(forcing_term - apply_operator(pad_second(current, 2), current_capacity, spectral_shifts, per_level_values))
    coarse_solution = multigrid_cycle(per_level_values + 1, coarse_right_hand, capacity_fields, spectral_shifts)
    current = current + prolong_cells(coarse_solution)
    for repeat in range(SMOOTH):
        current = current + damped_update(forcing_term - apply_operator(pad_second(current, 2), current_capacity, spectral_shifts, per_level_values), inverse)
    return current


def reference(residual, capacity):
    length = residual.shape[0]
    ratio_step = ALPHA_CORNER ** (1.0 / length)
    moments = jnp.arange(length, dtype=jnp.float32)
    weights = jnp.power(ratio_step, moments)
    scaled = residual * weights[:, None, None, None]
    capacity_fields = [capacity]
    for per_level_values in range(1, GRID_DEPTH):
        capacity_fields.append(restrict_to_coarse(capacity_fields[-1]))
    integers = jnp.arange(length, dtype=jnp.int32)

    def one_frequency(summed, frequency):
        phases = (2.0 * math.pi / length) * ((integers * frequency) % length).astype(jnp.float32)
        cosines = jnp.cos(phases)
        sines = jnp.sin(phases)
        real_part = jnp.tensordot(cosines, scaled, axes=1, precision=HIGHEST)
        imag_part = -jnp.tensordot(sines, scaled, axes=1, precision=HIGHEST)
        forcing_term = jnp.stack([real_part, imag_part])[:, None]
        spectral_shifts = shift_values(frequency[None], length)
        solution_field = multigrid_cycle(0, forcing_term, capacity_fields, spectral_shifts)[:, 0]
        summed = summed + cosines[:, None, None, None] * solution_field[0] - sines[:, None, None, None] * solution_field[1]
        return summed, None

    summed, unused = lax.scan(one_frequency, jnp.zeros(residual.shape, jnp.float32), integers)
    return summed / length / weights[:, None, None, None]
```

```python
import functools
import math

import jax
import jax.numpy as jnp
import numpy as np
from jax import lax
from jax.experimental import pallas as pl
from jax.experimental.pallas import tpu as pltpu
from jax.sharding import PartitionSpec as P

GRID_DEPTH = 4
SMOOTH = 2
COARSE_SWEEPS = 6


ALPHA_CORNER = 0.01
STEP_SIZE = 0.5
DIFFUSE = 2.0
ADVECT = (0.2, -0.15, 0.1)
OMEGA = 0.7
HIGHEST = lax.Precision.HIGHEST


def extended(array, sides, width):
    for axis, dim in sides:
        peers, length = (lax.axis_size(axis), array.shape[dim])
        up = [(i, (i + 1) % peers) for i in range(peers - 1)]
        down = [(j, i) for i, j in up]
        last = lax.slice_in_dim(array, length - width, length, axis=dim)
        initial = lax.slice_in_dim(array, 0, width, axis=dim)
        before = lax.ppermute(last, axis, up)
        after = lax.ppermute(initial, axis, down)
        array = jnp.concatenate([before, array, after], axis=dim)
    return array


def level_coefficients(per_level_values):
    spread = DIFFUSE / 4.0**per_level_values
    drifts = tuple((component / 2.0**per_level_values for component in ADVECT))
    return (spread, drifts)


def pad_second(volume, position):
    widths = [(0, 0)] * volume.ndim
    widths[position] = (1, 1)
    return jnp.pad(volume, widths)


def apply_operator(padded, current_capacity, spectral_shifts, per_level_values):
    spread, drifts = level_coefficients(per_level_values)
    centre = padded[:, :, 1:-1]
    upper_first = padded[:, :, 2:]
    lower_first = padded[:, :, :-2]
    wide_second = pad_second(centre, 3)
    upper_second = wide_second[:, :, :, 2:]
    lower_second = wide_second[:, :, :, :-2]
    wide_third = pad_second(centre, 4)
    upper_third = wide_third[:, :, :, :, 2:]
    lower_third = wide_third[:, :, :, :, :-2]
    stencil = spread * (
        6.0 * centre
        - upper_first
        - lower_first
        - upper_second
        - lower_second
        - upper_third
        - lower_third
    )
    stencil = (
        stencil
        + drifts[0] * (upper_first - lower_first)
        + drifts[1] * (upper_second - lower_second)
        + drifts[2] * (upper_third - lower_third)
    )
    first_shift, second_shift, third_shift = spectral_shifts
    real_part = centre[0]
    imag_part = centre[1]
    shifted = jnp.stack(
        [
            current_capacity * (first_shift * real_part - second_shift * imag_part),
            current_capacity * (second_shift * real_part + third_shift * imag_part),
        ]
    )
    return stencil + shifted


def inverse_diagonal(current_capacity, spectral_shifts, per_level_values):
    spread, drifts = level_coefficients(per_level_values)
    first_shift, second_shift, third_shift = spectral_shifts
    top_left = current_capacity * first_shift + 6.0 * spread
    coupling = current_capacity * second_shift
    bottom_right = current_capacity * third_shift + 6.0 * spread
    determinant = top_left * bottom_right + coupling * coupling
    return (bottom_right / determinant, coupling / determinant, top_left / determinant)


def damped_update(residual_now, inverse):
    diagonal_a, diagonal_b, diagonal_c = inverse
    return OMEGA * jnp.stack(
        [
            diagonal_a * residual_now[0] + diagonal_b * residual_now[1],
            diagonal_c * residual_now[1] - diagonal_b * residual_now[0],
        ]
    )


def restrict_to_coarse(volume):
    leading = volume.shape[:-3]
    first_extent, second_extent, third_extent = volume.shape[-3:]
    blocks = volume.reshape(
        leading + (first_extent // 2, 2, second_extent // 2, 2, third_extent // 2, 2)
    )
    lead_count = len(leading)
    return jnp.mean(blocks, axis=(lead_count + 1, lead_count + 3, lead_count + 5))


def prolong_cells(volume):
    leading = volume.shape[:-3]
    first_extent, second_extent, third_extent = volume.shape[-3:]
    expanded = jnp.broadcast_to(
        volume[..., :, None, :, None, :, None],
        leading + (first_extent, 2, second_extent, 2, third_extent, 2),
    )
    return expanded.reshape(leading + (2 * first_extent, 2 * second_extent, 2 * third_extent))


def shift_values(frequency, length):
    ratio_step = ALPHA_CORNER ** (1.0 / length)
    phases = 2.0 * math.pi / length * frequency.astype(jnp.float32)
    first_shift = (1.0 - ratio_step * jnp.cos(phases)) / STEP_SIZE
    second_shift = ratio_step * jnp.sin(phases) / STEP_SIZE
    leading = frequency == 0
    second_shift = jnp.where(leading, 0.0, second_shift)
    third_shift = jnp.where(leading, (1.0 + ratio_step) / STEP_SIZE, first_shift)
    return tuple(
        (column.reshape(-1, 1, 1, 1) for column in (first_shift, second_shift, third_shift))
    )


def phase_grid(row_count, length):
    integers = (
        jnp.arange(row_count, dtype=jnp.int32)[:, None]
        * jnp.arange(length, dtype=jnp.int32)[None, :]
        % length
    )
    return 2.0 * math.pi / length * integers.astype(jnp.float32)


def pad_faces(volume):
    return extended(volume, (("space", 2),), 1)


def multigrid_cycle(
    per_level_values,
    forcing_term,
    capacity_fields,
    spectral_shifts,
    shared_values,
    assemble_level,
    assemble_parts,
):
    current_capacity = capacity_fields[per_level_values]
    inverse = inverse_diagonal(current_capacity, spectral_shifts, per_level_values)
    coarsest = per_level_values == GRID_DEPTH - 1
    current = damped_update(forcing_term, inverse)
    for repeat in range((COARSE_SWEEPS if coarsest else SMOOTH) - 1):
        current = current + damped_update(
            forcing_term
            - apply_operator(
                pad_faces(current), current_capacity, spectral_shifts, per_level_values
            ),
            inverse,
        )
    if coarsest:
        return current
    coarse_right_hand = restrict_to_coarse(
        forcing_term
        - apply_operator(pad_faces(current), current_capacity, spectral_shifts, per_level_values)
    )
    coarse_solution = multigrid_cycle(
        per_level_values + 1,
        coarse_right_hand,
        capacity_fields,
        spectral_shifts,
        shared_values,
        assemble_level,
        assemble_parts,
    )
    current = current + prolong_cells(coarse_solution)
    for repeat in range(SMOOTH):
        current = current + damped_update(
            forcing_term
            - apply_operator(
                pad_faces(current), current_capacity, spectral_shifts, per_level_values
            ),
            inverse,
        )
    return current


def on_device(residual, capacity):
    steps_here, thickness, extent_second, extent_third = residual.shape
    length = lax.axis_size("tm") * steps_here
    ratio_step = ALPHA_CORNER ** (1.0 / length)
    moments = (lax.axis_index("tm") * steps_here + jnp.arange(steps_here, dtype=jnp.int32)).astype(
        jnp.float32
    )
    scaled = (residual * jnp.power(ratio_step, moments)[:, None, None, None]).reshape(
        steps_here, -1
    )
    series = lax.all_to_all(scaled, "tm", split_axis=1, concat_axis=0, tiled=True)
    all_weights = jnp.power(ratio_step, jnp.arange(length, dtype=jnp.float32))
    alternate = 1.0 - 2.0 * (jnp.arange(length, dtype=jnp.int32) % 2).astype(jnp.float32)
    capacity_fields = [capacity]
    for per_level_values in range(1, GRID_DEPTH):
        capacity_fields.append(restrict_to_coarse(capacity_fields[-1]))
    halves = length // 2
    phases = phase_grid(halves, length)
    first_row = jnp.arange(halves, dtype=jnp.int32)[:, None] == 0
    forward = jnp.concatenate(
        [jnp.cos(phases), jnp.where(first_row, alternate[None, :], -jnp.sin(phases))], axis=0
    )
    spectrum = jnp.dot(forward, series, precision=HIGHEST).reshape(2, halves, -1)
    received = lax.all_to_all(spectrum, "tm", split_axis=1, concat_axis=2, tiled=True)
    slot_count = steps_here // 2
    frequency = lax.axis_index("tm") * slot_count + jnp.arange(slot_count, dtype=jnp.int32)
    spectral_shifts = shift_values(frequency, length)
    field_list = received.reshape(2, slot_count, thickness, extent_second, extent_third)
    solved_fields = multigrid_cycle(
        0, field_list, capacity_fields, spectral_shifts, False, GRID_DEPTH, None
    )
    flattened = solved_fields.reshape(2, slot_count, -1)
    returned = lax.all_to_all(flattened, "tm", split_axis=2, concat_axis=1, tiled=True)
    halves = length // 2
    phases = jnp.transpose(phase_grid(halves, length))
    first_column = jnp.arange(halves, dtype=jnp.int32)[None, :] == 0
    real_columns = jnp.where(first_column, 1.0, 2.0 * jnp.cos(phases)) / length
    imag_columns = jnp.where(first_column, alternate[:, None], -2.0 * jnp.sin(phases)) / length
    inverse_table = jnp.concatenate([real_columns, imag_columns], axis=1)
    values = jnp.dot(
        inverse_table,
        returned.reshape(returned.shape[0] * returned.shape[1], -1),
        precision=HIGHEST,
    )
    values = values / all_weights[:, None]
    result = lax.all_to_all(values, "tm", split_axis=0, concat_axis=1, tiled=True)
    return result.reshape(residual.shape)


MESH = pl.DeviceIdType.MESH


def real_transform(values):
    count = len(values)
    if count == 1:
        return [(values[0], None)]
    evens, odds = real_transform(values[0::2]), real_transform(values[1::2])
    half = count // 2
    if count == 2:
        return [(evens[0][0] + odds[0][0], None), (evens[0][0] - odds[0][0], None)]
    found = [None] * (half + 1)
    found[0] = (evens[0][0] + odds[0][0], None)
    found[half] = (evens[0][0] - odds[0][0], None)
    found[half // 2] = (evens[half // 2][0], -odds[half // 2][0])
    for k in range(1, half // 2):
        cosine, sine = math.cos(2 * math.pi * k / count), -math.sin(2 * math.pi * k / count)
        (er, ei), (or_, oi) = evens[k], odds[k]
        tr, ti = cosine * or_ - sine * oi, cosine * oi + sine * or_
        found[k] = (er + tr, ei + ti)
        found[half - k] = (er - tr, ti - ei)
    return found


def real_inverse(modes):
    half = len(modes) - 1
    if half == 0:
        return [modes[0][0]]
    count = 2 * half
    if half == 1:
        return [modes[0][0] + modes[1][0], modes[0][0] - modes[1][0]]
    evens, odds = [None] * (half // 2 + 1), [None] * (half // 2 + 1)
    evens[0] = (modes[0][0] + modes[half][0], None)
    odds[0] = (modes[0][0] - modes[half][0], None)
    middle = modes[half // 2]
    evens[half // 2] = (2.0 * middle[0], None)
    odds[half // 2] = (-2.0 * middle[1], None)
    for k in range(1, half // 2):
        cosine, sine = math.cos(2 * math.pi * k / count), math.sin(2 * math.pi * k / count)
        (ar, ai), (br, bi) = modes[k], modes[half - k]
        dr, di = ar - br, ai + bi
        evens[k] = (ar + br, ai - bi)
        odds[k] = (cosine * dr - sine * di, cosine * di + sine * dr)
    first, second = real_inverse(evens), real_inverse(odds)
    return [part for pair in zip(first, second) for part in pair]


def pair_sum(value, distance):
    for axis in (-2, -1):
        dim = value.ndim + axis
        extent = value.shape[dim]
        upper = pltpu.roll(value, extent - distance, dim)
        lower = pltpu.roll(value, distance, dim)
        place = lax.broadcasted_iota(jnp.int32, value.shape, dim)
        value = value + jnp.where((place // distance) % 2 == 0, upper, lower)
    return value


def block_mean(value, distance):
    shape = (value.shape[0] // 2, 2) + value.shape[1:]
    paired = value.reshape(shape)
    return 0.125 * pair_sum(paired[:, 0] + paired[:, 1], distance)


def neighbour_weights(level, shape):
    spread, drifts = level_coefficients(level)
    distance = 2**level
    along_first = (drifts[0] - spread, -drifts[0] - spread)
    masked = []
    for dim in (0, 1):
        place = lax.broadcasted_iota(jnp.int32, shape, dim)
        upper = jnp.where(place < shape[dim] - distance, drifts[dim + 1] - spread, 0.0)
        lower = jnp.where(place >= distance, -drifts[dim + 1] - spread, 0.0)
        masked.append((upper, lower))
    return along_first, masked, distance


def neighbours(wide, weights):
    along_first, masked, distance = weights
    centre = wide[1:-1]
    total = along_first[0] * wide[2:] + along_first[1] * wide[:-2]
    for dim in (0, 1):
        extent = centre.shape[dim + 1]
        if distance >= extent:
            continue
        upper, lower = masked[dim]
        total = total + upper[None] * pltpu.roll(centre, extent - distance, dim + 1)
        total = total + lower[None] * pltpu.roll(centre, distance, dim + 1)
    return total


def blocks_of(extent, largest, body):
    block = min(extent, largest)

    def step(i, carry):
        body(pl.multiple_of(i * block, block), block)
        return carry

    if extent == block:
        body(0, block)
    else:
        lax.fori_loop(0, extent // block, step, 0)


BLOCK = 64


def prepare_level(level, caps, inverses, shifts):
    spread, unused = level_coefficients(level)
    s1, s2, s3 = shifts

    def body(start, block):
        cap = caps[level][pl.ds(start, block)]
        top, coupling, bottom = cap * s1 + 6.0 * spread, cap * s2, cap * s3 + 6.0 * spread
        scale = OMEGA / (top * bottom + coupling * coupling)
        inverses[level][pl.ds(start, block), 0] = bottom * scale
        inverses[level][pl.ds(start, block), 1] = coupling * scale
        inverses[level][pl.ds(start, block), 2] = top * scale
        if level + 1 < GRID_DEPTH:
            half = block // 2
            caps[level + 1][pl.ds(start // 2, half)] = block_mean(cap, 2**level)

    blocks_of(caps[level].shape[0], BLOCK, body)


def smooth_first(forcing, target, inverse):
    def body(start, block):
        here = pl.ds(start, block)
        a, b, c = inverse[here, 0], inverse[here, 1], inverse[here, 2]
        re, im = forcing[here, 0], forcing[here, 1]
        there = pl.ds(start + 1, block)
        target[there, 0] = a * re + b * im
        target[there, 1] = c * im - b * re

    blocks_of(forcing.shape[0], BLOCK, body)


def smooth(forcing, source, target, inverse, weights, offset=1, coarse=None):
    def body(start, block):
        here = pl.ds(start, block)
        wide_re = source[pl.ds(start, block + 2), 0]
        wide_im = source[pl.ds(start, block + 2), 1]
        r0 = forcing[here, 0] - neighbours(wide_re, weights)
        r1 = forcing[here, 1] - neighbours(wide_im, weights)
        a, b, c = inverse[here, 0], inverse[here, 1], inverse[here, 2]
        there = pl.ds(start + offset, block)
        target[there, 0] = (1.0 - OMEGA) * wide_re[1:-1] + (a * r0 + b * r1)
        target[there, 1] = (1.0 - OMEGA) * wide_im[1:-1] + (c * r1 - b * r0)

    blocks_of(forcing.shape[0], BLOCK, body)


def restrict_residual(level, forcing, source, cap, shifts, weights, target):
    spread, unused = level_coefficients(level)
    s1, s2, s3 = shifts

    def body(start, block):
        here = pl.ds(start, block)
        wide_re = source[pl.ds(start, block + 2), 0]
        wide_im = source[pl.ds(start, block + 2), 1]
        re, im = wide_re[1:-1], wide_im[1:-1]
        field = cap[here]
        r0 = forcing[here, 0] - neighbours(wide_re, weights)
        r1 = forcing[here, 1] - neighbours(wide_im, weights)
        r0 = r0 - (6.0 * spread * re + field * (s1 * re - s2 * im))
        r1 = r1 - (6.0 * spread * im + field * (s2 * re + s3 * im))
        half = pl.ds(start // 2, block // 2)
        target[half, 0] = block_mean(r0, 2**level)
        target[half, 1] = block_mean(r1, 2**level)

    blocks_of(forcing.shape[0], BLOCK, body)


def add_coarse(target, coarse):
    def body(start, block):
        half = block // 2
        for part in (0, 1):
            extra = coarse[pl.ds(start // 2 + 1, half), part]
            spread = jnp.broadcast_to(extra[:, None], (half, 2) + extra.shape[1:])
            there = pl.ds(start + 1, block)
            target[there, part] = target[there, part] + spread.reshape((block,) + extra.shape[1:])

    blocks_of(target.shape[0] - 2, BLOCK, body)


def cycle(level, forcings, caps, inverses, firsts, seconds, shifts, result):
    forcing, inverse = forcings[level], inverses[level]
    here, other = firsts[level], seconds[level]
    weights = neighbour_weights(level, forcing.shape[-2:])
    coarsest = level == GRID_DEPTH - 1
    smooth_first(forcing, here, inverse)
    for repeat in range((COARSE_SWEEPS if coarsest else SMOOTH) - 1):
        smooth(forcing, here, other, inverse, weights)
        here, other = other, here
    if coarsest:
        return here
    restrict_residual(level, forcing, here, caps[level], shifts, weights, forcings[level + 1])
    coarse = cycle(level + 1, forcings, caps, inverses, firsts, seconds, shifts, None)
    add_coarse(here, coarse)
    for repeat in range(SMOOTH):
        last = repeat == SMOOTH - 1 and result is not None
        target = result if last else other
        smooth(forcing, here, target, inverse, weights, offset=0 if last else 1)
        here, other = target, here
    return here


def complex_transform(values, sign):
    count = len(values)
    if count == 1:
        return values
    evens, odds = complex_transform(values[0::2], sign), complex_transform(values[1::2], sign)
    first, second = [], []
    for k in range(count // 2):
        (er, ei), (or_, oi) = evens[k], odds[k]
        tr, ti = turned(or_, oi, k, count, sign)
        first.append((er + tr, ei + ti))
        second.append((er - tr, ei - ti))
    return first + second


def turned(re, im, k, count, sign):
    if k == 0:
        return re, im
    if 4 * k == count:
        return (-im, re) if sign > 0 else (im, -re)
    cosine, sine = math.cos(2 * math.pi * k / count), sign * math.sin(2 * math.pi * k / count)
    return cosine * re - sine * im, cosine * im + sine * re


def odd_transform(values):
    half = len(values) // 2
    folded = [turned(values[s], -values[s + half], s, 4 * half, -1) for s in range(half)]
    return complex_transform(folded, -1)


def odd_inverse(modes):
    half = len(modes)
    folded = complex_transform(modes, 1)
    first, second = [], []
    for s, (re, im) in enumerate(folded):
        re, im = turned(re, im, s, 4 * half, 1)
        first.append(2.0 * re)
        second.append(-2.0 * im)
    return first + second


def parity(shape, dim):
    return lax.broadcasted_iota(jnp.int32, shape, dim) % 2 == 0


def shifted(value, step, dim):
    return pltpu.roll(value, step % value.shape[dim], dim)


def pack_means(first, second, even_row, even_lane):
    rows = []
    for a, b in zip(first, second):
        left = jnp.where(even_row, a, shifted(b, 1, 0))
        right = jnp.where(even_row, shifted(a, -1, 0), b)
        rows.append(left + right)
    re, im = rows
    left = jnp.where(even_lane, re, shifted(im, 1, 1))
    right = jnp.where(even_lane, shifted(re, -1, 1), im)
    return left + right


def pack_cells(first, second, even_row, even_lane):
    re = jnp.where(even_row, first[0], second[0])
    im = jnp.where(even_row, first[1], second[1])
    return jnp.where(even_lane, re, im)


def unpack_cells(tile, even_row, even_lane):
    found = []
    for rows in (
        jnp.where(even_row, tile, shifted(tile, 1, 0)),
        jnp.where(even_row, shifted(tile, -1, 0), tile),
    ):
        re = jnp.where(even_lane, rows, shifted(rows, 1, 1))
        im = jnp.where(even_lane, shifted(rows, -1, 1), rows)
        found.append((re, im))
    return found


def neighbour_sum(below, here, above, weights):
    along_first, masked, distance = weights
    total = along_first[0] * above + along_first[1] * below
    for dim in (0, 1):
        upper, lower = masked[dim]
        total = total + upper * shifted(here, -distance, dim)
        total = total + lower * shifted(here, distance, dim)
    return total


def updated(forcing, inverse, columns, weights):
    results, rest = [], []
    for part in (0, 1):
        below, here, above = (column[part] for column in columns)
        rest.append(forcing[part] - neighbour_sum(below, here, above, weights))
    a, b, c = inverse
    r0, r1 = rest
    results.append((1.0 - OMEGA) * columns[1][0] + (a * r0 + b * r1))
    results.append((1.0 - OMEGA) * columns[1][1] + (c * r1 - b * r0))
    return results


HALO = 2


def whole_kernel(groups, slabs, shift_table, residual_hbm, capacity_hbm, out_ref, *scratch):
    (
        res, loc, far, seq, sendx, field, inverse0, vone, vtwo, coarse_out, gathered, back, edges,
        result, merged, wave, gotb, outgoing, table,
    ) = scratch[:19]
    depth = GRID_DEPTH
    rest = scratch[19:]
    forcings = (None,) + rest[: depth - 1]
    rest = rest[depth - 1 :]
    caps, rest = rest[:depth], rest[depth:]
    inverses = (None,) + rest[: depth - 1]
    rest = rest[depth - 1 :]
    firsts = (None,) + rest[: depth - 1]
    rest = rest[depth - 1 :]
    seconds = (None,) + rest[: depth - 1]
    rest = rest[depth - 1 :]
    (
        own, far_send, far_recv, loc_send, loc_recv, x_send, x_recv, d_send, d_recv, h_send, h_recv,
        e_send, e_recv, g_send, g_recv, b_send, b_recv, r_send, r_recv, w_send, w_recv, o_send,
        o_recv, c_send, c_recv, ready,
    ) = rest
    steps, thick = res.shape[:2]
    half = thick // 2
    slots = field.shape[1] // 2
    wide = thick + 2 * HALO
    length = groups * steps
    rate = ALPHA_CORNER ** (1.0 / length)
    tile = res.shape[-2:]
    m, s = lax.axis_index("tm"), lax.axis_index("space")
    y, x = m // 2, lax.rem(m, 2)
    z, c = s // 2, lax.rem(s, 2)
    layers = slabs // 2
    sig = lax.rem(y + z, 2)
    slab = 2 * z + sig
    keeper = sig == c
    is_low, is_high = slab == 0, slab == slabs - 1

    def at(ty, tx, tz, tc):
        return (2 * ty + tx, 2 * tz + tc)

    def plane_of(h, i):
        return i if h == 0 else thick - 1 - i

    def drain(ref, semaphore):
        pltpu.make_async_copy(ref, ref, semaphore).wait()

    def send(source, target, send_sem, recv_sem, device):
        pltpu.make_async_remote_copy(
            src_ref=source,
            dst_ref=target,
            send_sem=send_sem,
            recv_sem=recv_sem,
            device_id=device,
            device_id_type=MESH,
        ).start()

    takes = []
    for i in range(half):
        for h in (0, 1):
            p = plane_of(h, i)
            copy = pltpu.make_async_copy(residual_hbm.at[:, p], res.at[:, p], own.at[p])
            copy.start()
            takes.append((p, copy))
    own_slab = pl.ds(HALO + s * thick, thick)
    take_capacity = pltpu.make_async_copy(capacity_hbm, caps[0].at[own_slab], own.at[thick])
    take_capacity.start()

    barrier = pltpu.get_barrier_semaphore()
    below, above = z > 0, z < layers - 1
    sides = jnp.where(below, 1, 0) + jnp.where(above, 1, 0)

    def greet(device):
        pl.semaphore_signal(barrier, inc=1, device_id=device, device_id_type=MESH)

    greet(at(1 - y, x, z, 0))
    greet(at(1 - y, x, z, 1))
    for there, dz in ((below, -1), (above, 1)):

        @pl.when(there)
        def _():
            greet(at(y, x, z + dz, 0))
            greet(at(y, x, z + dz, 1))

    greet(at(y, 1 - x, z, c))
    greet(at(y, x, z, 1 - c))

    for level in range(1, depth):
        for buffer in (firsts[level], seconds[level]):
            empty = jnp.zeros(buffer.shape[1:], jnp.float32)
            buffer[0] = empty
            buffer[buffer.shape[0] - 1] = empty
    for k in range(shift_table.shape[0]):
        for column in range(3):
            table[k, column] = jnp.float32(shift_table[k, column])
    caps[0][pl.ds(0, HALO)] = jnp.ones((HALO,) + tile, jnp.float32)
    caps[0][pl.ds(HALO + slabs * thick, HALO)] = jnp.ones((HALO,) + tile, jnp.float32)

    @pl.when(is_low)
    def _():
        for j in range(HALO):
            field[j] = jnp.zeros(field.shape[1:], jnp.float32)
        vtwo[0] = jnp.zeros(vtwo.shape[1:], jnp.float32)

    @pl.when(is_high)
    def _():
        for j in range(HALO):
            field[wide - 1 - j] = jnp.zeros(field.shape[1:], jnp.float32)
        vtwo[wide - 1] = jnp.zeros(vtwo.shape[1:], jnp.float32)

    pl.semaphore_wait(barrier, 4 + 2 * sides)

    waited = {}
    for p, copy in takes:
        waited[p] = copy

    for i in range(half):
        for h in (0, 1):
            waited[plane_of(h, i)].wait()

        @pl.when(keeper)
        def _():
            for h in (0, 1):
                p = plane_of(h, i)

                @pl.when(c == h)
                def _():
                    pltpu.make_async_copy(res.at[:, p], loc.at[i], loc_recv.at[i]).start()

                @pl.when(c != h)
                def _():
                    send(res.at[:, p], loc.at[i], loc_send.at[i], loc_recv.at[i], at(y, x, z, 1 - c))

        @pl.when(jnp.logical_not(keeper))
        def _():
            for h in (0, 1):
                p = plane_of(h, i)
                send(
                    res.at[:, p], far.at[i], far_send.at[i, h], far_recv.at[i], at(1 - y, x, z, h)
                )

    for turn in range(layers - 1):
        for there, dz in ((below, -1), (above, 1)):

            @pl.when(there)
            def _():
                pl.semaphore_signal(
                    ready.at[turn], inc=1, device_id=at(y, x, z + dz, c), device_id_type=MESH
                )

        pl.semaphore_wait(ready.at[turn], sides)

    take_capacity.wait()
    for d in range(1, layers):
        send(
            caps[0].at[own_slab],
            caps[0].at[own_slab],
            c_send.at[d],
            c_recv.at[d],
            (m, lax.rem(s + 2 * d, slabs)),
        )

    def rows_from(d):
        return pl.ds(HALO + lax.rem(s + slabs - 2 * d, slabs) * thick, thick)

    def forward_cap(d):
        rows = rows_from(d)
        send(
            caps[0].at[rows],
            caps[0].at[rows],
            c_send.at[layers + d],
            c_recv.at[layers + d],
            at(y, x, z, 1 - c),
        )

    forward_cap(0)

    def power(ty):
        exponent = [rate ** (a * length // 2 + b * steps) for a in (0, 1) for b in (0, 1)]
        low = jnp.where(x == 0, jnp.float32(exponent[0]), jnp.float32(exponent[1]))
        high = jnp.where(x == 0, jnp.float32(exponent[2]), jnp.float32(exponent[3]))
        return jnp.where(ty == 0, low, high)

    here_power, there_power = power(y), power(1 - y)
    sign = jnp.where(y == 0, 1.0, -1.0).astype(jnp.float32)
    first_x = x == 0
    keep_own = jnp.where(first_x, here_power, sign * here_power)
    keep_far = jnp.where(first_x, there_power, -sign * there_power)
    give_own = jnp.where(first_x, sign * here_power, here_power)
    give_far = jnp.where(first_x, -sign * there_power, there_power)

    def combine(i):
        drain(loc.at[i], loc_recv.at[i])
        drain(far.at[i], far_recv.at[i])
        for t in range(steps):
            a, b = loc[i, t] * (rate**t), far[i, t] * (rate**t)
            sendx[i, t] = give_own * a + give_far * b
        send(
            sendx.at[i],
            seq.at[i, pl.ds(x * steps, steps)],
            x_send.at[i],
            x_recv.at[i],
            at(y, 1 - x, z, c),
        )
        for t in range(steps):
            a, b = loc[i, t] * (rate**t), far[i, t] * (rate**t)
            seq[i, x * steps + t] = keep_own * a + keep_far * b

    in_layer = c != sig
    halo_y = jnp.where(in_layer, 1 - y, y)
    halo_z = jnp.where(in_layer, z, z + 2 * c - 1)
    halo_there = jnp.logical_or(in_layer, jnp.logical_and(halo_z >= 0, halo_z < layers))

    def transform(i):
        drain(sendx.at[i], x_recv.at[i])
        plane = jnp.where(c == 0, i, thick - 1 - i) + HALO

        @pl.when(x == 0)
        def _():
            modes = real_transform([seq[i, t] for t in range(2 * steps)])
            field[plane, 0, 0] = modes[0][0]
            field[plane, 0, 1] = modes[steps][0]
            for k in range(1, steps):
                field[plane, k, 0] = modes[k][0]
                field[plane, k, 1] = modes[k][1]

        @pl.when(x == 1)
        def _():
            modes = odd_transform([seq[i, t] for t in range(2 * steps)])
            for k in range(steps):
                field[plane, k, 0] = modes[k][0]
                field[plane, k, 1] = modes[k][1]

        given = field.at[plane, pl.ds((1 - c) * slots, slots)]
        send(given, given, d_send.at[i], d_recv.at[i], at(y, x, z, 1 - c))
        if i < HALO:
            target = plane + thick * (1 - 2 * c)

            @pl.when(halo_there)
            def _():
                for k in (0, 1):
                    part = pl.ds(k * slots, slots)
                    send(
                        field.at[plane, part],
                        field.at[target, part],
                        h_send.at[i, k],
                        h_recv.at[1 - c, i],
                        at(halo_y, x, halo_z, k),
                    )

    def shifts_of(slot):
        return tuple(table[slot, column] for column in range(3))

    def coarse_tables():
        for d in range(1, layers):
            drain(caps[0].at[rows_from(d)], c_recv.at[d])
            forward_cap(d)
        for d in range(layers):
            drain(caps[0].at[own_slab], c_recv.at[layers + d])
        solver_shifts = shifts_of(x * 2 * slots + c * slots + slab)
        cells = caps[0][pl.ds(HALO, slabs * thick)]
        caps[1][...] = block_mean(cells, 1)
        for level in range(1, depth):
            prepare_level(level, caps, inverses, solver_shifts)

    spread0, unused = level_coefficients(0)

    def fine_tables():
        inside = [jnp.float32(1.0)] * wide
        for j in range(HALO):
            inside[j] = jnp.where(is_low, 0.0, 1.0).astype(jnp.float32)
            inside[wide - 1 - j] = jnp.where(is_high, 0.0, 1.0).astype(jnp.float32)

        def body(f, carry):
            s1, s2, s3 = shifts_of(x * 2 * slots + c * slots + f)
            for j in range(wide):
                cap = caps[0][slab * thick + j]
                top, coupling = cap * s1 + 6.0 * spread0, cap * s2
                bottom = cap * s3 + 6.0 * spread0
                scale = (OMEGA * inside[j]) / (top * bottom + coupling * coupling)
                inverse0[f, j, 0] = bottom * scale
                inverse0[f, j, 1] = coupling * scale
                inverse0[f, j, 2] = top * scale
            return carry

        lax.fori_loop(0, slots, body, 0)

    combine(0)
    combine(1)
    coarse_tables()
    combine(2)
    transform(0)
    fine_tables()
    combine(3)
    for i in range(1, half):
        transform(i)

    even_row, even_lane = parity(tile, 0), parity(tile, 1)
    weights = neighbour_weights(0, tile)

    def slot_at(i):
        total, unit, rest_g, rest_i = 0, 1, slab, i
        while unit < slots:
            bit = lax.rem(lax.rem(rest_g, 2) + lax.rem(rest_i, 2), 2)
            total = total + unit * bit
            rest_g, rest_i = rest_g // 2, rest_i // 2
            unit *= 2
        return total

    def member(g):
        gz, gs = g // 2, lax.rem(g, 2)
        return at(lax.rem(gs + gz, 2), x, gz, c)

    for i in range(half):
        drain(field.at[0, pl.ds(0, slots)], d_recv.at[i])
    for side, there in ((0, jnp.logical_not(is_low)), (1, jnp.logical_not(is_high))):

        @pl.when(there)
        def _():
            for i in range(HALO):
                drain(field.at[0, pl.ds(0, slots)], h_recv.at[side, i])

    def down(i, carry):
        f = slot_at(slots - 1 - i)
        q = c * slots + f
        s1, s2, s3 = shifts_of(x * 2 * slots + q)
        for j in range(wide):
            re, im = field[j, q, 0], field[j, q, 1]
            a, b, d = (inverse0[f, j, k] for k in range(3))
            vone[j, 0] = a * re + b * im
            vone[j, 1] = d * im - b * re
        for j in range(1, wide - 1):
            columns = [(vone[k, 0], vone[k, 1]) for k in (j - 1, j, j + 1)]
            parts = updated(
                (field[j, q, 0], field[j, q, 1]),
                [inverse0[f, j, k] for k in range(3)],
                columns,
                weights,
            )
            vtwo[j, f, 0] = parts[0]
            vtwo[j, f, 1] = parts[1]
        for pair in range(thick // 4):
            packed = []
            for plane in (0, 1):
                sums = [0.0, 0.0]
                for k in (0, 1):
                    j = HALO + 4 * pair + 2 * plane + k
                    cap = caps[0][slab * thick + j]
                    near = [(vtwo[n, f, 0], vtwo[n, f, 1]) for n in (j - 1, j, j + 1)]
                    re, im = near[1]
                    turn = (s1 * re - s2 * im, s2 * re + s3 * im)
                    for part in (0, 1):
                        total = field[j, q, part] - neighbour_sum(
                            near[0][part], near[1][part], near[2][part], weights
                        )
                        total = total - (6.0 * spread0 * near[1][part] + cap * turn[part])
                        sums[part] = sums[part] + total
                packed.append(sums)
            coarse_out[f, pair] = 0.125 * pack_means(packed[0], packed[1], even_row, even_lane)

        tiles = pl.ds(slab * (thick // 4), thick // 4)

        @pl.when(f != slab)
        def _():
            send(coarse_out.at[f], gathered.at[tiles], g_send, g_recv, member(f))

        @pl.when(f == slab)
        def _():
            for pair in range(thick // 4):
                gathered[slab * (thick // 4) + pair] = coarse_out[f, pair]

        return carry

    lax.fori_loop(0, slots, down, 0)

    low_y, low_z = jnp.where(sig == 0, y, 1 - y), jnp.where(sig == 0, z - 1, z)
    high_y, high_z = jnp.where(sig == 0, 1 - y, y), jnp.where(sig == 0, z, z + 1)

    @pl.when(jnp.logical_not(is_low))
    def _():
        send(
            vtwo.at[HALO + 1], vtwo.at[wide - 1], e_send.at[0], e_recv.at[1], at(low_y, x, low_z, c)
        )

    @pl.when(jnp.logical_not(is_high))
    def _():
        send(
            vtwo.at[wide - HALO - 2], vtwo.at[0], e_send.at[1], e_recv.at[0],
            at(high_y, x, high_z, c),
        )

    others = gathered.at[pl.ds(0, (slabs - 1) * (thick // 4))]
    drain(others, g_recv)
    for j in range(slabs * thick // 4):
        first, second = unpack_cells(gathered[j], even_row, even_lane)
        for k, parts in enumerate((first, second)):
            forcings[1][2 * j + k, 0] = parts[0]
            forcings[1][2 * j + k, 1] = parts[1]
    solver_shifts = shifts_of(x * 2 * slots + c * slots + slab)
    coarse = cycle(1, forcings, caps, inverses, firsts, seconds, solver_shifts, None)
    for j in range(slabs * thick // 4 + 1):
        back[j] = pack_cells(
            (coarse[2 * j, 0], coarse[2 * j, 1]),
            (coarse[2 * j + 1, 0], coarse[2 * j + 1, 1]),
            even_row,
            even_lane,
        )
    span = thick // 4 + 1

    def give(i, carry):
        g = slot_at(slots - i)
        send(
            back.at[pl.ds(g * (thick // 4), span)], edges.at[slab], b_send, b_recv.at[slab],
            member(g),
        )
        return carry

    lax.fori_loop(1, slots, give, 0)
    for k in range(span):
        edges[slab, k] = back[slab * (thick // 4) + k]

    for side, there in ((0, jnp.logical_not(is_low)), (1, jnp.logical_not(is_high))):

        @pl.when(there)
        def _():
            drain(vtwo.at[0], e_recv.at[side])
            drain(vtwo.at[0], e_send.at[side])

    def up(i, carry):
        f = slot_at(i)
        q = c * slots + f

        @pl.when(i > 0)
        def _():
            drain(edges.at[0], b_recv.at[f])

        for k in range(span):
            for n, extra in enumerate(unpack_cells(edges[f, k], even_row, even_lane)):
                for j in (4 * k + 2 * n, 4 * k + 2 * n + 1):
                    for part in (0, 1):
                        vone[j, part] = vtwo[j, f, part] + extra[part]
        for j in range(1, wide - 1):
            columns = [(vone[k, 0], vone[k, 1]) for k in (j - 1, j, j + 1)]
            parts = updated(
                (field[j, q, 0], field[j, q, 1]),
                [inverse0[f, j, k] for k in range(3)],
                columns,
                weights,
            )
            vtwo[j, f, 0] = parts[0]
            vtwo[j, f, 1] = parts[1]
        for j in range(HALO, wide - HALO):
            columns = [(vtwo[k, f, 0], vtwo[k, f, 1]) for k in (j - 1, j, j + 1)]
            parts = updated(
                (field[j, q, 0], field[j, q, 1]),
                [inverse0[f, j, k] for k in range(3)],
                columns,
                weights,
            )
            result[f, j - HALO, 0] = parts[0]
            result[f, j - HALO, 1] = parts[1]
        send(
            result.at[f, pl.ds((1 - c) * half, half)], merged.at[q], r_send, r_recv,
            at(y, x, z, 1 - c),
        )
        for k in range(half):
            merged[q, k] = result[f, c * half + k]
        return carry

    lax.fori_loop(0, slots, up, 0)
    drain(merged.at[pl.ds(0, slots)], r_recv)

    def invert(i):
        @pl.when(x == 0)
        def _():
            modes = [(merged[0, i, 0], None)]
            modes += [(merged[k, i, 0], merged[k, i, 1]) for k in range(1, steps)]
            modes += [(merged[0, i, 1], None)]
            for t, value in enumerate(real_inverse(modes)):
                wave[i, t] = value

        @pl.when(x == 1)
        def _():
            modes = [(merged[k, i, 0], merged[k, i, 1]) for k in range(steps)]
            for t, value in enumerate(odd_inverse(modes)):
                wave[i, t] = value

        send(
            wave.at[i, pl.ds((1 - x) * steps, steps)], gotb.at[i], w_send.at[i], w_recv.at[i],
            at(y, 1 - x, z, c),
        )

    inverse_here = 1.0 / (here_power * length)
    inverse_there = 1.0 / (there_power * length)
    own_sign = jnp.where(first_x, 1.0, sign).astype(jnp.float32)
    got_sign = jnp.where(first_x, sign, 1.0).astype(jnp.float32)
    far_own = jnp.where(first_x, 1.0, -sign).astype(jnp.float32)
    far_got = jnp.where(first_x, -sign, 1.0).astype(jnp.float32)

    def finish(i):
        drain(gotb.at[i], w_recv.at[i])
        p = c * half + i
        for t in range(steps):
            mine = wave[i, x * steps + t] * (rate**-t)
            got = gotb[i, t] * (rate**-t)
            outgoing[i, 1, t] = (far_own * inverse_there) * mine + (far_got * inverse_there) * got
        send(
            outgoing.at[i, 1], out_ref.at[:, p], o_send.at[i, 1], o_recv.at[c, i],
            at(1 - y, x, z, sig),
        )
        for t in range(steps):
            mine = wave[i, x * steps + t] * (rate**-t)
            got = gotb[i, t] * (rate**-t)
            outgoing[i, 0, t] = (own_sign * inverse_here) * mine + (got_sign * inverse_here) * got

        @pl.when(keeper)
        def _():
            for t in range(steps):
                out_ref[t, p] = outgoing[i, 0, t]

        @pl.when(jnp.logical_not(keeper))
        def _():
            send(
                outgoing.at[i, 0], out_ref.at[:, p], o_send.at[i, 0], o_recv.at[c, i],
                at(y, x, z, 1 - c),
            )

    for i in range(half):
        invert(i)
        if i > 0:
            finish(i - 1)
    finish(half - 1)

    block = loc.at[0]
    for i in range(half):

        @pl.when(keeper)
        def _():
            drain(block, o_recv.at[1 - c, i])
            drain(block, loc_send.at[i])

        @pl.when(jnp.logical_not(keeper))
        def _():
            for h in (0, 1):
                drain(block, o_recv.at[h, i])
                drain(block, far_send.at[i, h])
            drain(block, o_send.at[i, 0])

        drain(block, o_send.at[i, 1])
        drain(block, x_send.at[i])
        drain(block, w_send.at[i])
        drain(field.at[0, pl.ds(0, slots)], d_send.at[i])
        if i < HALO:

            @pl.when(halo_there)
            def _():
                for k in (0, 1):
                    drain(field.at[0, pl.ds(0, slots)], h_send.at[i, k])

    drain(others, g_send)
    drain(edges.at[pl.ds(0, slots - 1)], b_send)
    drain(merged.at[pl.ds(0, slots)], r_send)
    for d in range(1, layers):
        drain(caps[0].at[own_slab], c_send.at[d])
    for d in range(layers):
        drain(caps[0].at[own_slab], c_send.at[layers + d])


def level_extents(extent):
    return [extent // 2**level for level in range(GRID_DEPTH)]


def fused(groups, slabs, residual, capacity):
    steps, thick, second, third = residual.shape
    length = groups * steps
    half, slots = thick // 2, steps // 2
    extent, wide = slabs * thick, thick + 2 * HALO
    tile = (second, third)
    ratio_step = ALPHA_CORNER ** (1.0 / length)
    numbers = [2 * k for k in range(steps)] + [4 * k + 1 for k in range(steps)]
    angle = 2.0 * np.pi / length * np.array(numbers)
    table = np.stack(
        [
            (1.0 - ratio_step * np.cos(angle)) / STEP_SIZE,
            ratio_step * np.sin(angle) / STEP_SIZE,
            (1.0 - ratio_step * np.cos(angle)) / STEP_SIZE,
        ],
        axis=1,
    )
    table[0, 1], table[0, 2] = 0.0, (1.0 + ratio_step) / STEP_SIZE
    extents = level_extents(extent)
    vmem = lambda *shape: pltpu.VMEM(shape + tile, jnp.float32)
    sems = lambda *shape: pltpu.SemaphoreType.DMA(shape)
    one = pltpu.SemaphoreType.DMA
    layers, quarter = slabs // 2, thick // 4
    scratch = [
        vmem(steps, thick),
        vmem(half, steps),
        vmem(half, steps),
        vmem(half, 2 * steps),
        vmem(half, steps),
        vmem(wide, 2 * slots, 2),
        vmem(slots, wide, 3),
        vmem(wide, 2),
        vmem(wide, slots, 2),
        vmem(slots, quarter),
        vmem(slabs * quarter),
        vmem(slabs * quarter + 1),
        vmem(slots, quarter + 1),
        vmem(slots, thick, 2),
        vmem(2 * slots, half, 2),
        vmem(half, 2 * steps),
        vmem(half, steps),
        vmem(half, 2, steps),
        pltpu.SMEM(table.shape, jnp.float32),
        *[vmem(n, 2) for n in extents[1:]],
        vmem(extent + 2 * HALO),
        *[vmem(n) for n in extents[1:]],
        *[vmem(n, 3) for n in extents[1:]],
        *[vmem(n + 2, 2) for n in extents[1:]],
        *[vmem(n + 2, 2) for n in extents[1:]],
        sems(thick + 1),
        sems(half, 2),
        sems(half),
        sems(half),
        sems(half),
        sems(half),
        sems(half),
        sems(half),
        sems(half),
        sems(HALO, 2),
        sems(2, HALO),
        sems(2),
        sems(2),
        one,
        one,
        one,
        sems(slots),
        one,
        one,
        sems(half),
        sems(half),
        sems(half, 2),
        sems(2, half),
        sems(2 * layers),
        sems(2 * layers),
        pltpu.SemaphoreType.REGULAR((layers - 1,)),
    ]
    return pl.pallas_call(
        functools.partial(whole_kernel, groups, slabs, table),
        out_shape=jax.ShapeDtypeStruct(residual.shape, jnp.float32),
        in_specs=[
            pl.BlockSpec(memory_space=pltpu.HBM),
            pl.BlockSpec(memory_space=pltpu.HBM),
        ],
        out_specs=pl.BlockSpec(memory_space=pltpu.VMEM),
        scratch_shapes=scratch,
        compiler_params=pltpu.CompilerParams(
            collective_id=0, has_side_effects=True, vmem_limit_bytes=32 * 2**20
        ),
    )(residual, capacity)


def fits_fused(groups, slabs, residual):
    steps, thick, second, third = residual.shape
    length = groups * steps
    power = length & (length - 1) == 0
    return (
        power
        and groups == 4
        and slabs % 2 == 0
        and slabs == length // 8
        and thick == 8
        and all(n % 2 == 0 and n % min(n, BLOCK) == 0 for n in level_extents(slabs * thick))
        and (second, third) == (8, 128)
    )


def either(residual, capacity):
    groups, slabs = lax.axis_size("tm"), lax.axis_size("space")
    if fits_fused(groups, slabs, residual):
        return fused(groups, slabs, residual, capacity)
    return on_device(residual, capacity)


def solution(mesh):
    return jax.shard_map(
        either,
        mesh=mesh,
        in_specs=(P("tm", "space", None, None), P("space", None, None)),
        out_specs=P("tm", "space", None, None),
        check_vma=False,
    )
```

```python
import functools
import math

import jax
import jax.numpy as jnp
import numpy as np
from jax import lax
from jax.experimental import pallas as pl
from jax.experimental.pallas import tpu as pltpu
from jax.sharding import PartitionSpec as P

GRID_DEPTH = 4
SMOOTH = 2
COARSE_SWEEPS = 6


ALPHA_CORNER = 0.01
STEP_SIZE = 0.5
DIFFUSE = 2.0
ADVECT = (0.2, -0.15, 0.1)
OMEGA = 0.7
HIGHEST = lax.Precision.HIGHEST


def extended(array, sides, width):
    for axis, dim in sides:
        peers, length = (lax.axis_size(axis), array.shape[dim])
        up = [(i, (i + 1) % peers) for i in range(peers - 1)]
        down = [(j, i) for i, j in up]
        last = lax.slice_in_dim(array, length - width, length, axis=dim)
        initial = lax.slice_in_dim(array, 0, width, axis=dim)
        before = lax.ppermute(last, axis, up)
        after = lax.ppermute(initial, axis, down)
        array = jnp.concatenate([before, array, after], axis=dim)
    return array


def level_coefficients(per_level_values):
    spread = DIFFUSE / 4.0**per_level_values
    drifts = tuple((component / 2.0**per_level_values for component in ADVECT))
    return (spread, drifts)


def pad_second(volume, position):
    widths = [(0, 0)] * volume.ndim
    widths[position] = (1, 1)
    return jnp.pad(volume, widths)


def apply_operator(padded, current_capacity, spectral_shifts, per_level_values):
    spread, drifts = level_coefficients(per_level_values)
    centre = padded[:, :, 1:-1]
    upper_first = padded[:, :, 2:]
    lower_first = padded[:, :, :-2]
    wide_second = pad_second(centre, 3)
    upper_second = wide_second[:, :, :, 2:]
    lower_second = wide_second[:, :, :, :-2]
    wide_third = pad_second(centre, 4)
    upper_third = wide_third[:, :, :, :, 2:]
    lower_third = wide_third[:, :, :, :, :-2]
    stencil = spread * (
        6.0 * centre
        - upper_first
        - lower_first
        - upper_second
        - lower_second
        - upper_third
        - lower_third
    )
    stencil = (
        stencil
        + drifts[0] * (upper_first - lower_first)
        + drifts[1] * (upper_second - lower_second)
        + drifts[2] * (upper_third - lower_third)
    )
    first_shift, second_shift, third_shift = spectral_shifts
    real_part = centre[0]
    imag_part = centre[1]
    shifted = jnp.stack(
        [
            current_capacity * (first_shift * real_part - second_shift * imag_part),
            current_capacity * (second_shift * real_part + third_shift * imag_part),
        ]
    )
    return stencil + shifted


def inverse_diagonal(current_capacity, spectral_shifts, per_level_values):
    spread, drifts = level_coefficients(per_level_values)
    first_shift, second_shift, third_shift = spectral_shifts
    top_left = current_capacity * first_shift + 6.0 * spread
    coupling = current_capacity * second_shift
    bottom_right = current_capacity * third_shift + 6.0 * spread
    determinant = top_left * bottom_right + coupling * coupling
    return (bottom_right / determinant, coupling / determinant, top_left / determinant)


def damped_update(residual_now, inverse):
    diagonal_a, diagonal_b, diagonal_c = inverse
    return OMEGA * jnp.stack(
        [
            diagonal_a * residual_now[0] + diagonal_b * residual_now[1],
            diagonal_c * residual_now[1] - diagonal_b * residual_now[0],
        ]
    )


def restrict_to_coarse(volume):
    leading = volume.shape[:-3]
    first_extent, second_extent, third_extent = volume.shape[-3:]
    blocks = volume.reshape(
        leading + (first_extent // 2, 2, second_extent // 2, 2, third_extent // 2, 2)
    )
    lead_count = len(leading)
    return jnp.mean(blocks, axis=(lead_count + 1, lead_count + 3, lead_count + 5))


def prolong_cells(volume):
    leading = volume.shape[:-3]
    first_extent, second_extent, third_extent = volume.shape[-3:]
    expanded = jnp.broadcast_to(
        volume[..., :, None, :, None, :, None],
        leading + (first_extent, 2, second_extent, 2, third_extent, 2),
    )
    return expanded.reshape(leading + (2 * first_extent, 2 * second_extent, 2 * third_extent))


def shift_values(frequency, length):
    ratio_step = ALPHA_CORNER ** (1.0 / length)
    phases = 2.0 * math.pi / length * frequency.astype(jnp.float32)
    first_shift = (1.0 - ratio_step * jnp.cos(phases)) / STEP_SIZE
    second_shift = ratio_step * jnp.sin(phases) / STEP_SIZE
    leading = frequency == 0
    second_shift = jnp.where(leading, 0.0, second_shift)
    third_shift = jnp.where(leading, (1.0 + ratio_step) / STEP_SIZE, first_shift)
    return tuple(
        (column.reshape(-1, 1, 1, 1) for column in (first_shift, second_shift, third_shift))
    )


def phase_grid(row_count, length):
    integers = (
        jnp.arange(row_count, dtype=jnp.int32)[:, None]
        * jnp.arange(length, dtype=jnp.int32)[None, :]
        % length
    )
    return 2.0 * math.pi / length * integers.astype(jnp.float32)


def pad_faces(volume):
    return extended(volume, (("space", 2),), 1)


def multigrid_cycle(
    per_level_values,
    forcing_term,
    capacity_fields,
    spectral_shifts,
    shared_values,
    assemble_level,
    assemble_parts,
):
    current_capacity = capacity_fields[per_level_values]
    inverse = inverse_diagonal(current_capacity, spectral_shifts, per_level_values)
    coarsest = per_level_values == GRID_DEPTH - 1
    current = damped_update(forcing_term, inverse)
    for repeat in range((COARSE_SWEEPS if coarsest else SMOOTH) - 1):
        current = current + damped_update(
            forcing_term
            - apply_operator(
                pad_faces(current), current_capacity, spectral_shifts, per_level_values
            ),
            inverse,
        )
    if coarsest:
        return current
    coarse_right_hand = restrict_to_coarse(
        forcing_term
        - apply_operator(pad_faces(current), current_capacity, spectral_shifts, per_level_values)
    )
    coarse_solution = multigrid_cycle(
        per_level_values + 1,
        coarse_right_hand,
        capacity_fields,
        spectral_shifts,
        shared_values,
        assemble_level,
        assemble_parts,
    )
    current = current + prolong_cells(coarse_solution)
    for repeat in range(SMOOTH):
        current = current + damped_update(
            forcing_term
            - apply_operator(
                pad_faces(current), current_capacity, spectral_shifts, per_level_values
            ),
            inverse,
        )
    return current


def on_device(residual, capacity):
    steps_here, thickness, extent_second, extent_third = residual.shape
    length = lax.axis_size("tm") * steps_here
    ratio_step = ALPHA_CORNER ** (1.0 / length)
    moments = (lax.axis_index("tm") * steps_here + jnp.arange(steps_here, dtype=jnp.int32)).astype(
        jnp.float32
    )
    scaled = (residual * jnp.power(ratio_step, moments)[:, None, None, None]).reshape(
        steps_here, -1
    )
    series = lax.all_to_all(scaled, "tm", split_axis=1, concat_axis=0, tiled=True)
    all_weights = jnp.power(ratio_step, jnp.arange(length, dtype=jnp.float32))
    alternate = 1.0 - 2.0 * (jnp.arange(length, dtype=jnp.int32) % 2).astype(jnp.float32)
    capacity_fields = [capacity]
    for per_level_values in range(1, GRID_DEPTH):
        capacity_fields.append(restrict_to_coarse(capacity_fields[-1]))
    halves = length // 2
    phases = phase_grid(halves, length)
    first_row = jnp.arange(halves, dtype=jnp.int32)[:, None] == 0
    forward = jnp.concatenate(
        [jnp.cos(phases), jnp.where(first_row, alternate[None, :], -jnp.sin(phases))], axis=0
    )
    spectrum = jnp.dot(forward, series, precision=HIGHEST).reshape(2, halves, -1)
    received = lax.all_to_all(spectrum, "tm", split_axis=1, concat_axis=2, tiled=True)
    slot_count = steps_here // 2
    frequency = lax.axis_index("tm") * slot_count + jnp.arange(slot_count, dtype=jnp.int32)
    spectral_shifts = shift_values(frequency, length)
    field_list = received.reshape(2, slot_count, thickness, extent_second, extent_third)
    solved_fields = multigrid_cycle(
        0, field_list, capacity_fields, spectral_shifts, False, GRID_DEPTH, None
    )
    flattened = solved_fields.reshape(2, slot_count, -1)
    returned = lax.all_to_all(flattened, "tm", split_axis=2, concat_axis=1, tiled=True)
    halves = length // 2
    phases = jnp.transpose(phase_grid(halves, length))
    first_column = jnp.arange(halves, dtype=jnp.int32)[None, :] == 0
    real_columns = jnp.where(first_column, 1.0, 2.0 * jnp.cos(phases)) / length
    imag_columns = jnp.where(first_column, alternate[:, None], -2.0 * jnp.sin(phases)) / length
    inverse_table = jnp.concatenate([real_columns, imag_columns], axis=1)
    values = jnp.dot(
        inverse_table,
        returned.reshape(returned.shape[0] * returned.shape[1], -1),
        precision=HIGHEST,
    )
    values = values / all_weights[:, None]
    result = lax.all_to_all(values, "tm", split_axis=0, concat_axis=1, tiled=True)
    return result.reshape(residual.shape)


MESH = pl.DeviceIdType.MESH


def real_transform(values):
    count = len(values)
    if count == 1:
        return [(values[0], None)]
    evens, odds = real_transform(values[0::2]), real_transform(values[1::2])
    half = count // 2
    if count == 2:
        return [(evens[0][0] + odds[0][0], None), (evens[0][0] - odds[0][0], None)]
    found = [None] * (half + 1)
    found[0] = (evens[0][0] + odds[0][0], None)
    found[half] = (evens[0][0] - odds[0][0], None)
    found[half // 2] = (evens[half // 2][0], -odds[half // 2][0])
    for k in range(1, half // 2):
        cosine, sine = math.cos(2 * math.pi * k / count), -math.sin(2 * math.pi * k / count)
        (er, ei), (or_, oi) = evens[k], odds[k]
        tr, ti = cosine * or_ - sine * oi, cosine * oi + sine * or_
        found[k] = (er + tr, ei + ti)
        found[half - k] = (er - tr, ti - ei)
    return found


def real_inverse(modes):
    half = len(modes) - 1
    if half == 0:
        return [modes[0][0]]
    count = 2 * half
    if half == 1:
        return [modes[0][0] + modes[1][0], modes[0][0] - modes[1][0]]
    evens, odds = [None] * (half // 2 + 1), [None] * (half // 2 + 1)
    evens[0] = (modes[0][0] + modes[half][0], None)
    odds[0] = (modes[0][0] - modes[half][0], None)
    middle = modes[half // 2]
    evens[half // 2] = (2.0 * middle[0], None)
    odds[half // 2] = (-2.0 * middle[1], None)
    for k in range(1, half // 2):
        cosine, sine = math.cos(2 * math.pi * k / count), math.sin(2 * math.pi * k / count)
        (ar, ai), (br, bi) = modes[k], modes[half - k]
        dr, di = ar - br, ai + bi
        evens[k] = (ar + br, ai - bi)
        odds[k] = (cosine * dr - sine * di, cosine * di + sine * dr)
    first, second = real_inverse(evens), real_inverse(odds)
    return [part for pair in zip(first, second) for part in pair]


def pair_sum(value, distance):
    for axis in (-2, -1):
        dim = value.ndim + axis
        extent = value.shape[dim]
        upper = pltpu.roll(value, extent - distance, dim)
        lower = pltpu.roll(value, distance, dim)
        place = lax.broadcasted_iota(jnp.int32, value.shape, dim)
        value = value + jnp.where((place // distance) % 2 == 0, upper, lower)
    return value


def block_mean(value, distance):
    shape = (value.shape[0] // 2, 2) + value.shape[1:]
    paired = value.reshape(shape)
    return 0.125 * pair_sum(paired[:, 0] + paired[:, 1], distance)


def neighbour_weights(level, shape):
    spread, drifts = level_coefficients(level)
    distance = 2**level
    along_first = (drifts[0] - spread, -drifts[0] - spread)
    masked = []
    for dim in (0, 1):
        place = lax.broadcasted_iota(jnp.int32, shape, dim)
        upper = jnp.where(place < shape[dim] - distance, drifts[dim + 1] - spread, 0.0)
        lower = jnp.where(place >= distance, -drifts[dim + 1] - spread, 0.0)
        masked.append((upper, lower))
    return along_first, masked, distance


def complex_transform(values, sign):
    count = len(values)
    if count == 1:
        return values
    evens, odds = complex_transform(values[0::2], sign), complex_transform(values[1::2], sign)
    first, second = [], []
    for k in range(count // 2):
        (er, ei), (or_, oi) = evens[k], odds[k]
        tr, ti = turned(or_, oi, k, count, sign)
        first.append((er + tr, ei + ti))
        second.append((er - tr, ei - ti))
    return first + second


def turned(re, im, k, count, sign):
    if k == 0:
        return re, im
    if 4 * k == count:
        return (-im, re) if sign > 0 else (im, -re)
    cosine, sine = math.cos(2 * math.pi * k / count), sign * math.sin(2 * math.pi * k / count)
    return cosine * re - sine * im, cosine * im + sine * re


def odd_transform(values):
    half = len(values) // 2
    folded = [turned(values[s], -values[s + half], s, 4 * half, -1) for s in range(half)]
    return complex_transform(folded, -1)


def odd_inverse(modes):
    half = len(modes)
    folded = complex_transform(modes, 1)
    first, second = [], []
    for s, (re, im) in enumerate(folded):
        re, im = turned(re, im, s, 4 * half, 1)
        first.append(2.0 * re)
        second.append(-2.0 * im)
    return first + second


def parity(shape, dim):
    return lax.broadcasted_iota(jnp.int32, shape, dim) % 2 == 0


def shifted(value, step, dim):
    return pltpu.roll(value, step % value.shape[dim], dim)


def pack_means(first, second, even_row, even_lane):
    rows = []
    for a, b in zip(first, second):
        left = jnp.where(even_row, a, shifted(b, 1, 0))
        right = jnp.where(even_row, shifted(a, -1, 0), b)
        rows.append(left + right)
    re, im = rows
    left = jnp.where(even_lane, re, shifted(im, 1, 1))
    right = jnp.where(even_lane, shifted(re, -1, 1), im)
    return left + right


def unpack_cells(tile, even_row, even_lane):
    found = []
    for rows in (
        jnp.where(even_row, tile, shifted(tile, 1, 0)),
        jnp.where(even_row, shifted(tile, -1, 0), tile),
    ):
        re = jnp.where(even_lane, rows, shifted(rows, 1, 1))
        im = jnp.where(even_lane, shifted(rows, -1, 1), rows)
        found.append((re, im))
    return found


def neighbour_sum(below, here, above, weights):
    along_first, masked, distance = weights
    total = along_first[0] * above + along_first[1] * below
    for dim in (0, 1):
        upper, lower = masked[dim]
        total = total + upper * shifted(here, -distance, dim)
        total = total + lower * shifted(here, distance, dim)
    return total


def updated(forcing, inverse, columns, weights):
    results, rest = [], []
    for part in (0, 1):
        below, here, above = (column[part] for column in columns)
        rest.append(forcing[part] - neighbour_sum(below, here, above, weights))
    a, b, c = inverse
    r0, r1 = rest
    results.append((1.0 - OMEGA) * columns[1][0] + (a * r0 + b * r1))
    results.append((1.0 - OMEGA) * columns[1][1] + (c * r1 - b * r0))
    return results


def compact_rest(forcing, values, weights, even_row):
    along_first, masked, distance = weights
    found = [[None, None] for here in forcing]
    for part in (0, 1):
        column = [value[part] for value in values]
        ups = [shifted(v, -1, 0) for v in column]
        downs = [shifted(v, 1, 0) for v in column]
        for j, value in enumerate(column):
            zero = jnp.zeros_like(value)
            after = downs[j + 1] if j + 1 < len(column) else zero
            before = ups[j - 1] if j > 0 else zero
            total = along_first[0] * jnp.where(even_row, ups[j], after)
            total = total + along_first[1] * jnp.where(even_row, before, downs[j])
            for dim in (0, 1):
                if distance < value.shape[dim]:
                    upper, lower = masked[dim]
                    total = total + upper * shifted(value, -distance, dim)
                    total = total + lower * shifted(value, distance, dim)
            found[j][part] = forcing[j][part] - total
    return found


def compact_sweep(forcing, values, table, weights, even_row):
    found = []
    for j, (r0, r1) in enumerate(compact_rest(forcing, values, weights, even_row)):
        a, b, c = (table[j, k] for k in range(3))
        re, im = values[j]
        found.append(
            (
                (1.0 - OMEGA) * re + (a * r0 + b * r1),
                (1.0 - OMEGA) * im + (c * r1 - b * r0),
            )
        )
    return found


def compact_restrict(values, distance, even_row):
    found = []
    for pair in zip(values[0::2], values[1::2]):
        parts = []
        for first, second in zip(*pair):
            left = jnp.where(even_row, first, shifted(second, 1, 0))
            total = left + jnp.where(even_row, shifted(first, -1, 0), second)
            for dim in (0, 1):
                place = lax.broadcasted_iota(jnp.int32, total.shape, dim)
                upper, lower = shifted(total, -distance, dim), shifted(total, distance, dim)
                total = total + jnp.where((place // distance) % 2 == 0, upper, lower)
            parts.append(0.125 * total)
        found.append(parts)
    return found


def compact_cycle(level, forcing, tables, shifts, even_row):
    table = tables[level]
    spread, unused = level_coefficients(level)
    s1, s2, s3 = shifts
    weights = neighbour_weights(level, forcing[0][0].shape)
    values = []
    for j, (re, im) in enumerate(forcing):
        a, b, c = (table[j, k] for k in range(3))
        values.append((a * re + b * im, c * im - b * re))
    coarsest = level == GRID_DEPTH - 1
    for repeat in range((COARSE_SWEEPS if coarsest else SMOOTH) - 1):
        values = compact_sweep(forcing, values, table, weights, even_row)
    if coarsest:
        return values
    rest = compact_rest(forcing, values, weights, even_row)
    for j, (re, im) in enumerate(values):
        cap = table[j, 3]
        rest[j][0] = rest[j][0] - (6.0 * spread * re + cap * (s1 * re - s2 * im))
        rest[j][1] = rest[j][1] - (6.0 * spread * im + cap * (s2 * re + s3 * im))
    coarse = compact_cycle(
        level + 1, compact_restrict(rest, 2**level, even_row), tables, shifts, even_row
    )
    for j, value in enumerate(coarse):
        values[2 * j] = tuple(
            old + jnp.where(even_row, v, shifted(v, 1, 0)) for old, v in zip(values[2 * j], value)
        )
        values[2 * j + 1] = tuple(
            old + jnp.where(even_row, shifted(v, -1, 0), v)
            for old, v in zip(values[2 * j + 1], value)
        )
    for repeat in range(SMOOTH):
        values = compact_sweep(forcing, values, table, weights, even_row)
    return values


def compact_table(level, caps, table, shifts, even_row):
    spread, unused = level_coefficients(level)
    s1, s2, s3 = shifts
    for j in range(table.shape[0]):
        cap = jnp.where(even_row, caps[2 * j], caps[2 * j + 1])
        top, coupling, bottom = cap * s1 + 6.0 * spread, cap * s2, cap * s3 + 6.0 * spread
        scale = OMEGA / (top * bottom + coupling * coupling)
        table[j, 0] = bottom * scale
        table[j, 1] = coupling * scale
        table[j, 2] = top * scale
        table[j, 3] = cap


HALO = 2
TOGETHER = 2
PARTS = 2


def whole_kernel(groups, slabs, shift_table, residual_hbm, capacity_hbm, out_ref, *scratch):
    (
        res, loc, far, seq, sendx, field, inverse0, vtwo, coarse_out, gathered, back, edges,
        result, merged, wave, gotb, outgoing, table, near_cap,
    ) = scratch[:19]
    depth = GRID_DEPTH
    rest = scratch[19:]
    caps, rest = rest[:depth], rest[depth:]
    tables, rest = (None,) + rest[: depth - 1], rest[depth - 1 :]
    (
        own, far_send, far_recv, loc_send, loc_recv, x_send, x_recv, d_send, d_recv, h_send, h_recv,
        e_send, e_recv, g_send, g_recv, b_send, b_recv, r_send, r_recv, w_send, w_recv, o_send,
        o_recv, c_send, c_recv, n_send, n_recv, ready,
    ) = rest
    steps, thick = res.shape[:2]
    half = thick // 2
    slots = field.shape[1] // 2
    wide = thick + 2 * HALO
    length = groups * steps
    rate = ALPHA_CORNER ** (1.0 / length)
    tile = res.shape[-2:]
    m, s = lax.axis_index("tm"), lax.axis_index("space")
    y, x = m // 2, lax.rem(m, 2)
    z, c = s // 2, lax.rem(s, 2)
    layers = slabs // 2
    sig = lax.rem(y + z, 2)
    slab = 2 * z + sig
    keeper = sig == c
    side = lax.rem(c + x, 2)
    part_steps = steps // PARTS
    is_low, is_high = slab == 0, slab == slabs - 1

    def at(ty, tx, tz, tc):
        return (2 * ty + tx, 2 * tz + tc)

    def plane_of(h, i):
        return i if h == 0 else thick - 1 - i

    def drain(ref, semaphore):
        pltpu.make_async_copy(ref, ref, semaphore).wait()

    def send(source, target, send_sem, recv_sem, device):
        pltpu.make_async_remote_copy(
            src_ref=source,
            dst_ref=target,
            send_sem=send_sem,
            recv_sem=recv_sem,
            device_id=device,
            device_id_type=MESH,
        ).start()

    takes = []
    for i in range(half):
        for h in (0, 1):
            p = plane_of(h, i)
            copy = pltpu.make_async_copy(residual_hbm.at[:, p], res.at[:, p], own.at[p])
            copy.start()
            takes.append((p, copy))
    own_slab = pl.ds(s * thick, thick)
    take_capacity = pltpu.make_async_copy(capacity_hbm, caps[0].at[own_slab], own.at[thick])
    take_capacity.start()
    near_slab = pl.ds((2 + c) * thick, thick)
    take_near = pltpu.make_async_copy(capacity_hbm, near_cap.at[near_slab], own.at[thick + 1])
    take_near.start()

    barrier = pltpu.get_barrier_semaphore()
    below, above = z > 0, z < layers - 1
    sides = jnp.where(below, 1, 0) + jnp.where(above, 1, 0)

    def greet(device):
        pl.semaphore_signal(barrier, inc=1, device_id=device, device_id_type=MESH)

    greet(at(1 - y, x, z, 0))
    greet(at(1 - y, x, z, 1))
    for there, dz in ((below, -1), (above, 1)):

        @pl.when(there)
        def _():
            greet(at(y, x, z + dz, 0))
            greet(at(y, x, z + dz, 1))

    greet(at(y, 1 - x, z, 1 - c))
    greet(at(y, x, z, 1 - c))

    for k in range(shift_table.shape[0]):
        for column in range(3):
            table[k, column] = jnp.float32(shift_table[k, column])
    ones = jnp.ones((thick,) + tile, jnp.float32)

    @pl.when(jnp.logical_not(below))
    def _():
        near_cap[pl.ds(thick, thick)] = ones

    @pl.when(jnp.logical_not(above))
    def _():
        near_cap[pl.ds(4 * thick, thick)] = ones

    @pl.when(is_low)
    def _():
        for j in range(HALO):
            field[j] = jnp.zeros(field.shape[1:], jnp.float32)
        vtwo[0] = jnp.zeros(vtwo.shape[1:], jnp.float32)

    @pl.when(is_high)
    def _():
        for j in range(HALO):
            field[wide - 1 - j] = jnp.zeros(field.shape[1:], jnp.float32)
        vtwo[wide - 1] = jnp.zeros(vtwo.shape[1:], jnp.float32)

    pl.semaphore_wait(barrier, 4 + 2 * sides)

    waited = {}
    for p, copy in takes:
        waited[p] = copy

    for i in range(half):
        for h in (0, 1):
            waited[plane_of(h, i)].wait()

        @pl.when(keeper)
        def _():
            for h in (0, 1):
                p = plane_of(h, i)

                @pl.when(side == h)
                def _():
                    pltpu.make_async_copy(res.at[:, p], loc.at[i], loc_recv.at[i]).start()

                @pl.when(side != h)
                def _():
                    send(res.at[:, p], loc.at[i], loc_send.at[i], loc_recv.at[i], at(y, x, z, 1 - c))

        @pl.when(jnp.logical_not(keeper))
        def _():
            for k in range(PARTS):
                span = pl.ds(k * part_steps, part_steps)
                for h in (0, 1):
                    send(
                        res.at[span, plane_of(h, i)], far.at[i, span], far_send.at[i, k, h],
                        far_recv.at[i, k], at(1 - y, x, z, lax.rem(h + x, 2)),
                    )

    take_near.wait()
    send(
        near_cap.at[near_slab], near_cap.at[near_slab], n_send.at[2], n_recv.at[2],
        at(y, x, z, 1 - c),
    )
    near_there = jnp.where(c == 0, below, above)

    @pl.when(near_there)
    def _():
        for k in (0, 1):
            send(
                near_cap.at[near_slab],
                near_cap.at[pl.ds((4 - 3 * c) * thick, thick)],
                n_send.at[k],
                n_recv.at[1 - c],
                at(y, x, z + 2 * c - 1, k),
            )

    def tell_sides(turn):
        for there, dz in ((below, -1), (above, 1)):

            @pl.when(there)
            def _():
                pl.semaphore_signal(
                    ready.at[turn], inc=1, device_id=at(y, x, z + dz, c), device_id_type=MESH
                )

    def hear_sides(turn):
        pl.semaphore_wait(ready.at[turn], sides)

    def share_capacity():
        take_capacity.wait()
        for d in range(1, layers):
            send(
                caps[0].at[own_slab],
                caps[0].at[own_slab],
                c_send.at[d],
                c_recv.at[d],
                (m, lax.rem(s + 2 * d, slabs)),
            )
        forward_cap(0)

    def rows_from(d):
        return pl.ds(lax.rem(s + slabs - 2 * d, slabs) * thick, thick)

    def forward_cap(d):
        rows = rows_from(d)
        send(
            caps[0].at[rows],
            caps[0].at[rows],
            c_send.at[layers + d],
            c_recv.at[layers + d],
            at(y, x, z, 1 - c),
        )

    def power(ty):
        exponent = [rate ** (a * length // 2 + b * steps) for a in (0, 1) for b in (0, 1)]
        low = jnp.where(x == 0, jnp.float32(exponent[0]), jnp.float32(exponent[1]))
        high = jnp.where(x == 0, jnp.float32(exponent[2]), jnp.float32(exponent[3]))
        return jnp.where(ty == 0, low, high)

    here_power, there_power = power(y), power(1 - y)
    sign = jnp.where(y == 0, 1.0, -1.0).astype(jnp.float32)
    first_x = x == 0
    keep_own = jnp.where(first_x, here_power, sign * here_power)
    keep_far = jnp.where(first_x, there_power, -sign * there_power)
    give_own = jnp.where(first_x, sign * here_power, here_power)
    give_far = jnp.where(first_x, -sign * there_power, there_power)

    def combine(i):
        drain(loc.at[i], loc_recv.at[i])
        for k in range(PARTS):
            span = pl.ds(k * part_steps, part_steps)
            drain(far.at[i, span], far_recv.at[i, k])
            for t in range(k * part_steps, (k + 1) * part_steps):
                a, b = loc[i, t] * (rate**t), far[i, t] * (rate**t)
                sendx[i, t] = give_own * a + give_far * b
            send(
                sendx.at[i, span],
                seq.at[i, pl.ds(x * steps + k * part_steps, part_steps)],
                x_send.at[i, k],
                x_recv.at[i, k],
                at(y, 1 - x, z, 1 - c),
            )
            for t in range(k * part_steps, (k + 1) * part_steps):
                a, b = loc[i, t] * (rate**t), far[i, t] * (rate**t)
                seq[i, x * steps + t] = keep_own * a + keep_far * b

    in_layer = side != sig
    halo_y = jnp.where(in_layer, 1 - y, y)
    halo_z = jnp.where(in_layer, z, z + 2 * side - 1)
    halo_there = jnp.logical_or(in_layer, jnp.logical_and(halo_z >= 0, halo_z < layers))

    def transform(i):
        for k in range(PARTS):
            drain(sendx.at[i, pl.ds(0, part_steps)], x_recv.at[i, k])
        plane = jnp.where(side == 0, i, thick - 1 - i) + HALO

        @pl.when(x == 0)
        def _():
            modes = real_transform([seq[i, t] for t in range(2 * steps)])
            field[plane, 0, 0] = modes[0][0]
            field[plane, 0, 1] = modes[steps][0]
            for k in range(1, steps):
                field[plane, k, 0] = modes[k][0]
                field[plane, k, 1] = modes[k][1]

        @pl.when(x == 1)
        def _():
            modes = odd_transform([seq[i, t] for t in range(2 * steps)])
            for k in range(steps):
                field[plane, k, 0] = modes[k][0]
                field[plane, k, 1] = modes[k][1]

        given = field.at[plane, pl.ds((1 - c) * slots, slots)]
        send(given, given, d_send.at[i], d_recv.at[i], at(y, x, z, 1 - c))
        if i < HALO:
            target = plane + thick * (1 - 2 * side)

            @pl.when(halo_there)
            def _():
                for k in (0, 1):
                    part = pl.ds(k * slots, slots)
                    send(
                        field.at[plane, part],
                        field.at[target, part],
                        h_send.at[i, k],
                        h_recv.at[1 - side, i],
                        at(halo_y, x, halo_z, k),
                    )

    def shifts_of(slot):
        return tuple(table[slot, column] for column in range(3))

    even_row, even_lane = parity(tile, 0), parity(tile, 1)
    solver_shifts = shifts_of(x * 2 * slots + c * slots + slab)

    def pass_capacity():
        for d in range(1, layers):
            drain(caps[0].at[rows_from(d)], c_recv.at[d])
            forward_cap(d)

    def coarse_tables():
        for d in range(layers):
            drain(caps[0].at[own_slab], c_recv.at[layers + d])
        for level in range(1, depth):
            caps[level][...] = block_mean(caps[level - 1][...], 2 ** (level - 1))
            compact_table(level, caps[level], tables[level], solver_shifts, even_row)

    spread0, unused = level_coefficients(0)

    cap_base = (2 + sig) * thick - HALO

    def fine_tables():
        drain(near_cap.at[near_slab], n_recv.at[2])

        @pl.when(below)
        def _():
            drain(near_cap.at[near_slab], n_recv.at[0])

        @pl.when(above)
        def _():
            drain(near_cap.at[near_slab], n_recv.at[1])

        inside = [jnp.float32(1.0)] * wide
        for j in range(HALO):
            inside[j] = jnp.where(is_low, 0.0, 1.0).astype(jnp.float32)
            inside[wide - 1 - j] = jnp.where(is_high, 0.0, 1.0).astype(jnp.float32)

        def body(f, carry):
            s1, s2, s3 = shifts_of(x * 2 * slots + c * slots + f)
            for j in range(wide):
                cap = near_cap[cap_base + j]
                top, coupling = cap * s1 + 6.0 * spread0, cap * s2
                bottom = cap * s3 + 6.0 * spread0
                scale = (OMEGA * inside[j]) / (top * bottom + coupling * coupling)
                inverse0[f, j, 0] = bottom * scale
                inverse0[f, j, 1] = coupling * scale
                inverse0[f, j, 2] = top * scale
            return carry

        lax.fori_loop(0, slots, body, 0)

    for turn in range(layers - 1):
        tell_sides(turn)
        if turn > 0:
            combine(turn - 1)
        hear_sides(turn)
    share_capacity()
    for i in range(layers - 2, half):
        combine(i)
    for i in range(half):
        transform(i)
        if i == 1:
            fine_tables()
    pass_capacity()

    weights = neighbour_weights(0, tile)

    def slot_at(i):
        total, unit, rest_g, rest_i = 0, 1, slab, i
        while unit < slots:
            bit = lax.rem(lax.rem(rest_g, 2) + lax.rem(rest_i, 2), 2)
            total = total + unit * bit
            rest_g, rest_i = rest_g // 2, rest_i // 2
            unit *= 2
        return total

    def member(g):
        gz, gs = g // 2, lax.rem(g, 2)
        return at(lax.rem(gs + gz, 2), x, gz, c)

    for i in range(half):
        drain(field.at[0, pl.ds(0, slots)], d_recv.at[i])
    for end, there in ((0, jnp.logical_not(is_low)), (1, jnp.logical_not(is_high))):

        @pl.when(there)
        def _():
            for i in range(HALO):
                drain(field.at[0, pl.ds(0, slots)], h_recv.at[end, i])

    def load_slot(f):
        q = c * slots + f
        forcing = [(field[j, q, 0], field[j, q, 1]) for j in range(wide)]
        inverse = [[inverse0[f, j, k] for k in range(3)] for j in range(wide)]
        return forcing, inverse

    def residual_at(forcing, second, j, shifts):
        s1, s2, s3 = shifts
        cap = near_cap[cap_base + j]
        re, im = second[j]
        turn = (s1 * re - s2 * im, s2 * re + s3 * im)
        found = []
        for part in (0, 1):
            total = forcing[j][part] - neighbour_sum(
                *(second[n][part] for n in (j - 1, j, j + 1)), weights
            )
            found.append(total - (6.0 * spread0 * second[j][part] + cap * turn[part]))
        return found

    def down(i, carry):
        chosen = [slot_at(slots - 1 - TOGETHER * i - k) for k in range(TOGETHER)]
        loaded = [load_slot(f) for f in chosen]
        shifts = [shifts_of(x * 2 * slots + c * slots + f) for f in chosen]
        first = [[] for f in chosen]
        second = [[None] for f in chosen]
        for j in range(wide):
            for n, (forcing, inverse) in enumerate(loaded):
                (re, im), (a, b, d) = forcing[j], inverse[j]
                first[n].append((a * re + b * im, d * im - b * re))
        for j in range(1, wide - 1):
            for n, (forcing, inverse) in enumerate(loaded):
                second[n].append(updated(forcing[j], inverse[j], first[n][j - 1 : j + 2], weights))
                for part in (0, 1):
                    vtwo[j, chosen[n], part] = second[n][j][part]
        for pair in range(thick // 4):
            packed = [[[None, None], [None, None]] for f in chosen]
            for plane in (0, 1):
                for k in (0, 1):
                    for n, (forcing, inverse) in enumerate(loaded):
                        j = HALO + 4 * pair + 2 * plane + k
                        rest = residual_at(forcing, second[n], j, shifts[n])
                        for part in (0, 1):
                            sofar = packed[n][plane][part]
                            packed[n][plane][part] = rest[part] if k == 0 else sofar + rest[part]
            for n, f in enumerate(chosen):
                coarse_out[f, pair] = 0.125 * pack_means(*packed[n], even_row, even_lane)

        tiles = pl.ds(slab * (thick // 4), thick // 4)
        for f in chosen:

            @pl.when(f != slab)
            def _():
                send(coarse_out.at[f], gathered.at[tiles], g_send, g_recv, member(f))

            @pl.when(f == slab)
            def _():
                for pair in range(thick // 4):
                    gathered[slab * (thick // 4) + pair] = coarse_out[f, pair]

        return carry

    lax.fori_loop(0, slots // TOGETHER, down, 0)

    low_y, low_z = jnp.where(sig == 0, y, 1 - y), jnp.where(sig == 0, z - 1, z)
    high_y, high_z = jnp.where(sig == 0, 1 - y, y), jnp.where(sig == 0, z, z + 1)

    @pl.when(jnp.logical_not(is_low))
    def _():
        send(
            vtwo.at[HALO + 1], vtwo.at[wide - 1], e_send.at[0], e_recv.at[1], at(low_y, x, low_z, c)
        )

    @pl.when(jnp.logical_not(is_high))
    def _():
        send(
            vtwo.at[wide - HALO - 2], vtwo.at[0], e_send.at[1], e_recv.at[0],
            at(high_y, x, high_z, c),
        )

    coarse_tables()
    others = gathered.at[pl.ds(0, (slabs - 1) * (thick // 4))]
    drain(others, g_recv)
    tiles_in = slabs * thick // 4
    unpacked = []
    for j in range(tiles_in):
        cells = gathered[j]
        re = jnp.where(even_lane, cells, shifted(cells, 1, 1))
        im = jnp.where(even_lane, shifted(cells, -1, 1), cells)
        unpacked.append((re, im))
    coarse = compact_cycle(1, unpacked, tables, solver_shifts, even_row)
    packed_cells = [jnp.where(even_lane, re, im) for re, im in coarse]
    empty = jnp.zeros(tile, jnp.float32)
    for j in range(tiles_in + 1):
        back[j] = jnp.where(
            even_row,
            packed_cells[j] if j < tiles_in else empty,
            packed_cells[j - 1] if j > 0 else empty,
        )
    span = thick // 4 + 1

    def give(i, carry):
        g = slot_at(slots - i)
        send(
            back.at[pl.ds(g * (thick // 4), span)], edges.at[slab], b_send, b_recv.at[slab],
            member(g),
        )
        return carry

    lax.fori_loop(1, slots, give, 0)
    for k in range(span):
        edges[slab, k] = back[slab * (thick // 4) + k]

    for end, there in ((0, jnp.logical_not(is_low)), (1, jnp.logical_not(is_high))):

        @pl.when(there)
        def _():
            drain(vtwo.at[0], e_recv.at[end])
            drain(vtwo.at[0], e_send.at[end])

    def up(i, carry):
        chosen = [slot_at(TOGETHER * i + k) for k in range(TOGETHER)]
        for k, f in enumerate(chosen):

            @pl.when(TOGETHER * i + k > 0)
            def _():
                drain(edges.at[0], b_recv.at[f])

        loaded = [load_slot(f) for f in chosen]
        start = [[] for f in chosen]
        third = [[None] for f in chosen]
        for k in range(span):
            for n, f in enumerate(chosen):
                for u, extra in enumerate(unpack_cells(edges[f, k], even_row, even_lane)[::-1]):
                    for j in (4 * k + 2 * u, 4 * k + 2 * u + 1):
                        start[n].append([vtwo[j, f, part] + extra[part] for part in (0, 1)])
        for j in range(1, wide - 1):
            for n, (forcing, inverse) in enumerate(loaded):
                third[n].append(updated(forcing[j], inverse[j], start[n][j - 1 : j + 2], weights))
        for j in range(HALO, wide - HALO):
            for n, (forcing, inverse) in enumerate(loaded):
                parts = updated(forcing[j], inverse[j], third[n][j - 1 : j + 2], weights)
                for part in (0, 1):
                    result[chosen[n], j - HALO, part] = parts[part]
        for f in chosen:
            q = c * slots + f
            send(
                result.at[f, pl.ds((1 - side) * half, half)], merged.at[q], r_send, r_recv,
                at(y, x, z, 1 - c),
            )
            for k in range(half):
                merged[q, k] = result[f, side * half + k]
        return carry

    lax.fori_loop(0, slots // TOGETHER, up, 0)
    drain(merged.at[pl.ds(0, slots)], r_recv)

    def invert(i):
        @pl.when(x == 0)
        def _():
            modes = [(merged[0, i, 0], None)]
            modes += [(merged[k, i, 0], merged[k, i, 1]) for k in range(1, steps)]
            modes += [(merged[0, i, 1], None)]
            for t, value in enumerate(real_inverse(modes)):
                wave[i, t] = value

        @pl.when(x == 1)
        def _():
            modes = [(merged[k, i, 0], merged[k, i, 1]) for k in range(steps)]
            for t, value in enumerate(odd_inverse(modes)):
                wave[i, t] = value

        for k in range(PARTS):
            send(
                wave.at[i, pl.ds((1 - x) * steps + k * part_steps, part_steps)],
                gotb.at[i, pl.ds(k * part_steps, part_steps)], w_send.at[i, k], w_recv.at[i, k],
                at(y, 1 - x, z, 1 - c),
            )

    inverse_here = 1.0 / (here_power * length)
    inverse_there = 1.0 / (there_power * length)
    own_sign = jnp.where(first_x, 1.0, sign).astype(jnp.float32)
    got_sign = jnp.where(first_x, sign, 1.0).astype(jnp.float32)
    far_own = jnp.where(first_x, 1.0, -sign).astype(jnp.float32)
    far_got = jnp.where(first_x, -sign, 1.0).astype(jnp.float32)

    def finish(i, k):
        span = pl.ds(k * part_steps, part_steps)
        drain(gotb.at[i, span], w_recv.at[i, k])
        p = side * half + i
        for t in range(k * part_steps, (k + 1) * part_steps):
            mine = wave[i, x * steps + t] * (rate**-t)
            got = gotb[i, t] * (rate**-t)
            outgoing[i, 1, t] = (far_own * inverse_there) * mine + (far_got * inverse_there) * got
        send(
            outgoing.at[i, 1, span], out_ref.at[span, p], o_send.at[i, k, 1],
            o_recv.at[side, i, k], at(1 - y, x, z, sig),
        )

        def own_value(t):
            mine = wave[i, x * steps + t] * (rate**-t)
            got = gotb[i, t] * (rate**-t)
            return (own_sign * inverse_here) * mine + (got_sign * inverse_here) * got

        @pl.when(keeper)
        def _():
            for t in range(k * part_steps, (k + 1) * part_steps):
                out_ref[t, p] = own_value(t)

        @pl.when(jnp.logical_not(keeper))
        def _():
            for t in range(k * part_steps, (k + 1) * part_steps):
                outgoing[i, 0, t] = own_value(t)
            send(
                outgoing.at[i, 0, span], out_ref.at[span, p], o_send.at[i, k, 0],
                o_recv.at[side, i, k], at(y, x, z, 1 - c),
            )

    for i in range(half):
        invert(i)
    for i in range(half):
        for k in range(PARTS):
            finish(i, k)

    block = loc.at[0]
    piece = loc.at[0, pl.ds(0, part_steps)]
    for i in range(half):
        for k in range(PARTS):

            @pl.when(keeper)
            def _():
                drain(piece, o_recv.at[1 - side, i, k])

            @pl.when(jnp.logical_not(keeper))
            def _():
                for h in (0, 1):
                    drain(piece, o_recv.at[h, i, k])
                    drain(piece, far_send.at[i, k, h])
                drain(piece, o_send.at[i, k, 0])

            drain(piece, o_send.at[i, k, 1])
            drain(piece, x_send.at[i, k])
            drain(piece, w_send.at[i, k])

        @pl.when(keeper)
        def _():
            drain(block, loc_send.at[i])

        drain(field.at[0, pl.ds(0, slots)], d_send.at[i])
        if i < HALO:

            @pl.when(halo_there)
            def _():
                for k in (0, 1):
                    drain(field.at[0, pl.ds(0, slots)], h_send.at[i, k])

    drain(others, g_send)
    drain(edges.at[pl.ds(0, slots - 1)], b_send)
    drain(merged.at[pl.ds(0, slots)], r_send)
    drain(near_cap.at[near_slab], n_send.at[2])

    @pl.when(near_there)
    def _():
        for k in (0, 1):
            drain(near_cap.at[near_slab], n_send.at[k])

    for d in range(1, layers):
        drain(caps[0].at[own_slab], c_send.at[d])
    for d in range(layers):
        drain(caps[0].at[own_slab], c_send.at[layers + d])


def level_extents(extent):
    return [extent // 2**level for level in range(GRID_DEPTH)]


def fused(groups, slabs, residual, capacity):
    steps, thick, second, third = residual.shape
    length = groups * steps
    half, slots = thick // 2, steps // 2
    extent, wide = slabs * thick, thick + 2 * HALO
    tile = (second, third)
    ratio_step = ALPHA_CORNER ** (1.0 / length)
    numbers = [2 * k for k in range(steps)] + [4 * k + 1 for k in range(steps)]
    angle = 2.0 * np.pi / length * np.array(numbers)
    table = np.stack(
        [
            (1.0 - ratio_step * np.cos(angle)) / STEP_SIZE,
            ratio_step * np.sin(angle) / STEP_SIZE,
            (1.0 - ratio_step * np.cos(angle)) / STEP_SIZE,
        ],
        axis=1,
    )
    table[0, 1], table[0, 2] = 0.0, (1.0 + ratio_step) / STEP_SIZE
    extents = level_extents(extent)
    vmem = lambda *shape: pltpu.VMEM(shape + tile, jnp.float32)
    sems = lambda *shape: pltpu.SemaphoreType.DMA(shape)
    one = pltpu.SemaphoreType.DMA
    layers, quarter = slabs // 2, thick // 4
    scratch = [
        vmem(steps, thick),
        vmem(half, steps),
        vmem(half, steps),
        vmem(half, 2 * steps),
        vmem(half, steps),
        vmem(wide, 2 * slots, 2),
        vmem(slots, wide, 3),
        vmem(wide, slots, 2),
        vmem(slots, quarter),
        vmem(slabs * quarter),
        vmem(slabs * quarter + 1),
        vmem(slots, quarter + 1),
        vmem(slots, thick, 2),
        vmem(2 * slots, half, 2),
        vmem(half, 2 * steps),
        vmem(half, steps),
        vmem(half, 2, steps),
        pltpu.SMEM(table.shape, jnp.float32),
        vmem(6 * thick),
        *[vmem(n) for n in extents],
        *[vmem(n // 2, 4) for n in extents[1:]],
        sems(thick + 2),
        sems(half, PARTS, 2),
        sems(half, PARTS),
        sems(half),
        sems(half),
        sems(half, PARTS),
        sems(half, PARTS),
        sems(half),
        sems(half),
        sems(HALO, 2),
        sems(2, HALO),
        sems(2),
        sems(2),
        one,
        one,
        one,
        sems(slots),
        one,
        one,
        sems(half, PARTS),
        sems(half, PARTS),
        sems(half, PARTS, 2),
        sems(2, half, PARTS),
        sems(2 * layers),
        sems(2 * layers),
        sems(3),
        sems(3),
        pltpu.SemaphoreType.REGULAR((layers - 1,)),
    ]
    return pl.pallas_call(
        functools.partial(whole_kernel, groups, slabs, table),
        out_shape=jax.ShapeDtypeStruct(residual.shape, jnp.float32),
        in_specs=[
            pl.BlockSpec(memory_space=pltpu.HBM),
            pl.BlockSpec(memory_space=pltpu.HBM),
        ],
        out_specs=pl.BlockSpec(memory_space=pltpu.VMEM),
        scratch_shapes=scratch,
        compiler_params=pltpu.CompilerParams(
            collective_id=0, has_side_effects=True, vmem_limit_bytes=32 * 2**20
        ),
    )(*[pltpu.with_memory_space_constraint(a, pltpu.HBM) for a in (residual, capacity)])


def fits_fused(groups, slabs, residual):
    steps, thick, second, third = residual.shape
    length = groups * steps
    power = length & (length - 1) == 0
    return (
        power
        and groups == 4
        and slabs % 2 == 0
        and slabs == length // 8
        and thick == 8
        and all(n % 2 == 0 and n % n == 0 for n in level_extents(slabs * thick))
        and (second, third) == (8, 128)
    )


def either(residual, capacity):
    groups, slabs = lax.axis_size("tm"), lax.axis_size("space")
    if fits_fused(groups, slabs, residual):
        return fused(groups, slabs, residual, capacity)
    return on_device(residual, capacity)


def solution(mesh):
    return jax.shard_map(
        either,
        mesh=mesh,
        in_specs=(P("tm", "space", None, None), P("space", None, None)),
        out_specs=P("tm", "space", None, None),
        check_vma=False,
    )
```

```python
import functools
import math

import jax
import jax.numpy as jnp
import numpy as np
from jax import lax
from jax.experimental import pallas as pl
from jax.experimental.pallas import tpu as pltpu
from jax.sharding import PartitionSpec as P

GRID_DEPTH = 4
SMOOTH = 2
COARSE_SWEEPS = 6


ALPHA_CORNER = 0.01
STEP_SIZE = 0.5
DIFFUSE = 2.0
ADVECT = (0.2, -0.15, 0.1)
OMEGA = 0.7
HIGHEST = lax.Precision.HIGHEST


def extended(array, sides, width):
    for axis, dim in sides:
        peers, length = (lax.axis_size(axis), array.shape[dim])
        up = [(i, (i + 1) % peers) for i in range(peers - 1)]
        down = [(j, i) for i, j in up]
        last = lax.slice_in_dim(array, length - width, length, axis=dim)
        initial = lax.slice_in_dim(array, 0, width, axis=dim)
        before = lax.ppermute(last, axis, up)
        after = lax.ppermute(initial, axis, down)
        array = jnp.concatenate([before, array, after], axis=dim)
    return array


def level_coefficients(per_level_values):
    spread = DIFFUSE / 4.0**per_level_values
    drifts = tuple((component / 2.0**per_level_values for component in ADVECT))
    return (spread, drifts)


def pad_second(volume, position):
    widths = [(0, 0)] * volume.ndim
    widths[position] = (1, 1)
    return jnp.pad(volume, widths)


def apply_operator(padded, current_capacity, spectral_shifts, per_level_values):
    spread, drifts = level_coefficients(per_level_values)
    centre = padded[:, :, 1:-1]
    upper_first = padded[:, :, 2:]
    lower_first = padded[:, :, :-2]
    wide_second = pad_second(centre, 3)
    upper_second = wide_second[:, :, :, 2:]
    lower_second = wide_second[:, :, :, :-2]
    wide_third = pad_second(centre, 4)
    upper_third = wide_third[:, :, :, :, 2:]
    lower_third = wide_third[:, :, :, :, :-2]
    stencil = spread * (
        6.0 * centre
        - upper_first
        - lower_first
        - upper_second
        - lower_second
        - upper_third
        - lower_third
    )
    stencil = (
        stencil
        + drifts[0] * (upper_first - lower_first)
        + drifts[1] * (upper_second - lower_second)
        + drifts[2] * (upper_third - lower_third)
    )
    first_shift, second_shift, third_shift = spectral_shifts
    real_part = centre[0]
    imag_part = centre[1]
    shifted = jnp.stack(
        [
            current_capacity * (first_shift * real_part - second_shift * imag_part),
            current_capacity * (second_shift * real_part + third_shift * imag_part),
        ]
    )
    return stencil + shifted


def inverse_diagonal(current_capacity, spectral_shifts, per_level_values):
    spread, drifts = level_coefficients(per_level_values)
    first_shift, second_shift, third_shift = spectral_shifts
    top_left = current_capacity * first_shift + 6.0 * spread
    coupling = current_capacity * second_shift
    bottom_right = current_capacity * third_shift + 6.0 * spread
    determinant = top_left * bottom_right + coupling * coupling
    return (bottom_right / determinant, coupling / determinant, top_left / determinant)


def damped_update(residual_now, inverse):
    diagonal_a, diagonal_b, diagonal_c = inverse
    return OMEGA * jnp.stack(
        [
            diagonal_a * residual_now[0] + diagonal_b * residual_now[1],
            diagonal_c * residual_now[1] - diagonal_b * residual_now[0],
        ]
    )


def restrict_to_coarse(volume):
    leading = volume.shape[:-3]
    first_extent, second_extent, third_extent = volume.shape[-3:]
    blocks = volume.reshape(
        leading + (first_extent // 2, 2, second_extent // 2, 2, third_extent // 2, 2)
    )
    lead_count = len(leading)
    return jnp.mean(blocks, axis=(lead_count + 1, lead_count + 3, lead_count + 5))


def prolong_cells(volume):
    leading = volume.shape[:-3]
    first_extent, second_extent, third_extent = volume.shape[-3:]
    expanded = jnp.broadcast_to(
        volume[..., :, None, :, None, :, None],
        leading + (first_extent, 2, second_extent, 2, third_extent, 2),
    )
    return expanded.reshape(leading + (2 * first_extent, 2 * second_extent, 2 * third_extent))


def shift_values(frequency, length):
    ratio_step = ALPHA_CORNER ** (1.0 / length)
    phases = 2.0 * math.pi / length * frequency.astype(jnp.float32)
    first_shift = (1.0 - ratio_step * jnp.cos(phases)) / STEP_SIZE
    second_shift = ratio_step * jnp.sin(phases) / STEP_SIZE
    leading = frequency == 0
    second_shift = jnp.where(leading, 0.0, second_shift)
    third_shift = jnp.where(leading, (1.0 + ratio_step) / STEP_SIZE, first_shift)
    return tuple(
        (column.reshape(-1, 1, 1, 1) for column in (first_shift, second_shift, third_shift))
    )


def phase_grid(row_count, length):
    integers = (
        jnp.arange(row_count, dtype=jnp.int32)[:, None]
        * jnp.arange(length, dtype=jnp.int32)[None, :]
        % length
    )
    return 2.0 * math.pi / length * integers.astype(jnp.float32)


def pad_faces(volume):
    return extended(volume, (("space", 2),), 1)


def multigrid_cycle(
    per_level_values,
    forcing_term,
    capacity_fields,
    spectral_shifts,
    shared_values,
    assemble_level,
    assemble_parts,
):
    current_capacity = capacity_fields[per_level_values]
    inverse = inverse_diagonal(current_capacity, spectral_shifts, per_level_values)
    coarsest = per_level_values == GRID_DEPTH - 1
    current = damped_update(forcing_term, inverse)
    for repeat in range((COARSE_SWEEPS if coarsest else SMOOTH) - 1):
        current = current + damped_update(
            forcing_term
            - apply_operator(
                pad_faces(current), current_capacity, spectral_shifts, per_level_values
            ),
            inverse,
        )
    if coarsest:
        return current
    coarse_right_hand = restrict_to_coarse(
        forcing_term
        - apply_operator(pad_faces(current), current_capacity, spectral_shifts, per_level_values)
    )
    coarse_solution = multigrid_cycle(
        per_level_values + 1,
        coarse_right_hand,
        capacity_fields,
        spectral_shifts,
        shared_values,
        assemble_level,
        assemble_parts,
    )
    current = current + prolong_cells(coarse_solution)
    for repeat in range(SMOOTH):
        current = current + damped_update(
            forcing_term
            - apply_operator(
                pad_faces(current), current_capacity, spectral_shifts, per_level_values
            ),
            inverse,
        )
    return current


def on_device(residual, capacity):
    steps_here, thickness, extent_second, extent_third = residual.shape
    length = lax.axis_size("tm") * steps_here
    ratio_step = ALPHA_CORNER ** (1.0 / length)
    moments = (lax.axis_index("tm") * steps_here + jnp.arange(steps_here, dtype=jnp.int32)).astype(
        jnp.float32
    )
    scaled = (residual * jnp.power(ratio_step, moments)[:, None, None, None]).reshape(
        steps_here, -1
    )
    series = lax.all_to_all(scaled, "tm", split_axis=1, concat_axis=0, tiled=True)
    all_weights = jnp.power(ratio_step, jnp.arange(length, dtype=jnp.float32))
    alternate = 1.0 - 2.0 * (jnp.arange(length, dtype=jnp.int32) % 2).astype(jnp.float32)
    capacity_fields = [capacity]
    for per_level_values in range(1, GRID_DEPTH):
        capacity_fields.append(restrict_to_coarse(capacity_fields[-1]))
    halves = length // 2
    phases = phase_grid(halves, length)
    first_row = jnp.arange(halves, dtype=jnp.int32)[:, None] == 0
    forward = jnp.concatenate(
        [jnp.cos(phases), jnp.where(first_row, alternate[None, :], -jnp.sin(phases))], axis=0
    )
    spectrum = jnp.dot(forward, series, precision=HIGHEST).reshape(2, halves, -1)
    received = lax.all_to_all(spectrum, "tm", split_axis=1, concat_axis=2, tiled=True)
    slot_count = steps_here // 2
    frequency = lax.axis_index("tm") * slot_count + jnp.arange(slot_count, dtype=jnp.int32)
    spectral_shifts = shift_values(frequency, length)
    field_list = received.reshape(2, slot_count, thickness, extent_second, extent_third)
    solved_fields = multigrid_cycle(
        0, field_list, capacity_fields, spectral_shifts, False, GRID_DEPTH, None
    )
    flattened = solved_fields.reshape(2, slot_count, -1)
    returned = lax.all_to_all(flattened, "tm", split_axis=2, concat_axis=1, tiled=True)
    halves = length // 2
    phases = jnp.transpose(phase_grid(halves, length))
    first_column = jnp.arange(halves, dtype=jnp.int32)[None, :] == 0
    real_columns = jnp.where(first_column, 1.0, 2.0 * jnp.cos(phases)) / length
    imag_columns = jnp.where(first_column, alternate[:, None], -2.0 * jnp.sin(phases)) / length
    inverse_table = jnp.concatenate([real_columns, imag_columns], axis=1)
    values = jnp.dot(
        inverse_table,
        returned.reshape(returned.shape[0] * returned.shape[1], -1),
        precision=HIGHEST,
    )
    values = values / all_weights[:, None]
    result = lax.all_to_all(values, "tm", split_axis=0, concat_axis=1, tiled=True)
    return result.reshape(residual.shape)


MESH = pl.DeviceIdType.MESH


def real_transform(values):
    count = len(values)
    if count == 1:
        return [(values[0], None)]
    evens, odds = real_transform(values[0::2]), real_transform(values[1::2])
    half = count // 2
    if count == 2:
        return [(evens[0][0] + odds[0][0], None), (evens[0][0] - odds[0][0], None)]
    found = [None] * (half + 1)
    found[0] = (evens[0][0] + odds[0][0], None)
    found[half] = (evens[0][0] - odds[0][0], None)
    found[half // 2] = (evens[half // 2][0], -odds[half // 2][0])
    for k in range(1, half // 2):
        cosine, sine = math.cos(2 * math.pi * k / count), -math.sin(2 * math.pi * k / count)
        (er, ei), (or_, oi) = evens[k], odds[k]
        tr, ti = cosine * or_ - sine * oi, cosine * oi + sine * or_
        found[k] = (er + tr, ei + ti)
        found[half - k] = (er - tr, ti - ei)
    return found


def real_inverse(modes):
    half = len(modes) - 1
    if half == 0:
        return [modes[0][0]]
    count = 2 * half
    if half == 1:
        return [modes[0][0] + modes[1][0], modes[0][0] - modes[1][0]]
    evens, odds = [None] * (half // 2 + 1), [None] * (half // 2 + 1)
    evens[0] = (modes[0][0] + modes[half][0], None)
    odds[0] = (modes[0][0] - modes[half][0], None)
    middle = modes[half // 2]
    evens[half // 2] = (2.0 * middle[0], None)
    odds[half // 2] = (-2.0 * middle[1], None)
    for k in range(1, half // 2):
        cosine, sine = math.cos(2 * math.pi * k / count), math.sin(2 * math.pi * k / count)
        (ar, ai), (br, bi) = modes[k], modes[half - k]
        dr, di = ar - br, ai + bi
        evens[k] = (ar + br, ai - bi)
        odds[k] = (cosine * dr - sine * di, cosine * di + sine * dr)
    first, second = real_inverse(evens), real_inverse(odds)
    return [part for pair in zip(first, second) for part in pair]


def pair_sum(value, distance):
    for axis in (-2, -1):
        dim = value.ndim + axis
        extent = value.shape[dim]
        upper = pltpu.roll(value, extent - distance, dim)
        lower = pltpu.roll(value, distance, dim)
        place = lax.broadcasted_iota(jnp.int32, value.shape, dim)
        value = value + jnp.where((place // distance) % 2 == 0, upper, lower)
    return value


def block_mean(value, distance):
    shape = (value.shape[0] // 2, 2) + value.shape[1:]
    paired = value.reshape(shape)
    return 0.125 * pair_sum(paired[:, 0] + paired[:, 1], distance)


def neighbour_weights(level, shape):
    spread, drifts = level_coefficients(level)
    distance = 2**level
    along_first = (drifts[0] - spread, -drifts[0] - spread)
    masked = []
    for dim in (0, 1):
        place = lax.broadcasted_iota(jnp.int32, shape, dim)
        upper = jnp.where(place < shape[dim] - distance, drifts[dim + 1] - spread, 0.0)
        lower = jnp.where(place >= distance, -drifts[dim + 1] - spread, 0.0)
        masked.append((upper, lower))
    return along_first, masked, distance


def complex_transform(values, sign):
    count = len(values)
    if count == 1:
        return values
    evens, odds = complex_transform(values[0::2], sign), complex_transform(values[1::2], sign)
    first, second = [], []
    for k in range(count // 2):
        (er, ei), (or_, oi) = evens[k], odds[k]
        tr, ti = turned(or_, oi, k, count, sign)
        first.append((er + tr, ei + ti))
        second.append((er - tr, ei - ti))
    return first + second


def turned(re, im, k, count, sign):
    if k == 0:
        return re, im
    if 4 * k == count:
        return (-im, re) if sign > 0 else (im, -re)
    cosine, sine = math.cos(2 * math.pi * k / count), sign * math.sin(2 * math.pi * k / count)
    return cosine * re - sine * im, cosine * im + sine * re


def odd_transform(values):
    half = len(values) // 2
    folded = [turned(values[s], -values[s + half], s, 4 * half, -1) for s in range(half)]
    return complex_transform(folded, -1)


def odd_inverse(modes):
    half = len(modes)
    folded = complex_transform(modes, 1)
    first, second = [], []
    for s, (re, im) in enumerate(folded):
        re, im = turned(re, im, s, 4 * half, 1)
        first.append(2.0 * re)
        second.append(-2.0 * im)
    return first + second


def parity(shape, dim):
    return lax.broadcasted_iota(jnp.int32, shape, dim) % 2 == 0


def shifted(value, step, dim):
    return pltpu.roll(value, step % value.shape[dim], dim)


def pack_means(first, second, even_row, even_lane):
    rows = []
    for a, b in zip(first, second):
        left = jnp.where(even_row, a, shifted(b, 1, 0))
        right = jnp.where(even_row, shifted(a, -1, 0), b)
        rows.append(left + right)
    re, im = rows
    left = jnp.where(even_lane, re, shifted(im, 1, 1))
    right = jnp.where(even_lane, shifted(re, -1, 1), im)
    return left + right


def unpack_cells(tile, even_row, even_lane):
    found = []
    for rows in (
        jnp.where(even_row, tile, shifted(tile, 1, 0)),
        jnp.where(even_row, shifted(tile, -1, 0), tile),
    ):
        re = jnp.where(even_lane, rows, shifted(rows, 1, 1))
        im = jnp.where(even_lane, shifted(rows, -1, 1), rows)
        found.append((re, im))
    return found


def neighbour_sum(below, here, above, weights):
    along_first, masked, distance = weights
    total = along_first[0] * above + along_first[1] * below
    for dim in (0, 1):
        upper, lower = masked[dim]
        total = total + upper * shifted(here, -distance, dim)
        total = total + lower * shifted(here, distance, dim)
    return total


def updated(forcing, inverse, columns, weights):
    results, rest = [], []
    for part in (0, 1):
        below, here, above = (column[part] for column in columns)
        rest.append(forcing[part] - neighbour_sum(below, here, above, weights))
    a, b, c = inverse
    r0, r1 = rest
    results.append((1.0 - OMEGA) * columns[1][0] + (a * r0 + b * r1))
    results.append((1.0 - OMEGA) * columns[1][1] + (c * r1 - b * r0))
    return results


def compact_rest(forcing, values, weights, even_row):
    along_first, masked, distance = weights
    found = [[None, None] for here in forcing]
    for part in (0, 1):
        column = [value[part] for value in values]
        ups = [shifted(v, -1, 0) for v in column]
        downs = [shifted(v, 1, 0) for v in column]
        for j, value in enumerate(column):
            zero = jnp.zeros_like(value)
            after = downs[j + 1] if j + 1 < len(column) else zero
            before = ups[j - 1] if j > 0 else zero
            total = along_first[0] * jnp.where(even_row, ups[j], after)
            total = total + along_first[1] * jnp.where(even_row, before, downs[j])
            for dim in (0, 1):
                if distance < value.shape[dim]:
                    upper, lower = masked[dim]
                    total = total + upper * shifted(value, -distance, dim)
                    total = total + lower * shifted(value, distance, dim)
            found[j][part] = forcing[j][part] - total
    return found


def compact_sweep(forcing, values, table, weights, even_row):
    found = []
    for j, (r0, r1) in enumerate(compact_rest(forcing, values, weights, even_row)):
        a, b, c = (table[j, k] for k in range(3))
        re, im = values[j]
        found.append(
            (
                (1.0 - OMEGA) * re + (a * r0 + b * r1),
                (1.0 - OMEGA) * im + (c * r1 - b * r0),
            )
        )
    return found


def compact_restrict(values, distance, even_row):
    found = []
    for pair in zip(values[0::2], values[1::2]):
        parts = []
        for first, second in zip(*pair):
            left = jnp.where(even_row, first, shifted(second, 1, 0))
            total = left + jnp.where(even_row, shifted(first, -1, 0), second)
            for dim in (0, 1):
                place = lax.broadcasted_iota(jnp.int32, total.shape, dim)
                upper, lower = shifted(total, -distance, dim), shifted(total, distance, dim)
                total = total + jnp.where((place // distance) % 2 == 0, upper, lower)
            parts.append(0.125 * total)
        found.append(parts)
    return found


def compact_cycle(level, forcing, tables, shifts, even_row):
    table = tables[level]
    spread, unused = level_coefficients(level)
    s1, s2, s3 = shifts
    weights = neighbour_weights(level, forcing[0][0].shape)
    values = []
    for j, (re, im) in enumerate(forcing):
        a, b, c = (table[j, k] for k in range(3))
        values.append((a * re + b * im, c * im - b * re))
    coarsest = level == GRID_DEPTH - 1
    for repeat in range((COARSE_SWEEPS if coarsest else SMOOTH) - 1):
        values = compact_sweep(forcing, values, table, weights, even_row)
    if coarsest:
        return values
    rest = compact_rest(forcing, values, weights, even_row)
    for j, (re, im) in enumerate(values):
        cap = table[j, 3]
        rest[j][0] = rest[j][0] - (6.0 * spread * re + cap * (s1 * re - s2 * im))
        rest[j][1] = rest[j][1] - (6.0 * spread * im + cap * (s2 * re + s3 * im))
    coarse = compact_cycle(
        level + 1, compact_restrict(rest, 2**level, even_row), tables, shifts, even_row
    )
    for j, value in enumerate(coarse):
        values[2 * j] = tuple(
            old + jnp.where(even_row, v, shifted(v, 1, 0)) for old, v in zip(values[2 * j], value)
        )
        values[2 * j + 1] = tuple(
            old + jnp.where(even_row, shifted(v, -1, 0), v)
            for old, v in zip(values[2 * j + 1], value)
        )
    for repeat in range(SMOOTH):
        values = compact_sweep(forcing, values, table, weights, even_row)
    return values


def compact_table(level, caps, table, shifts, even_row):
    spread, unused = level_coefficients(level)
    s1, s2, s3 = shifts
    for j in range(table.shape[0]):
        cap = jnp.where(even_row, caps[2 * j], caps[2 * j + 1])
        top, coupling, bottom = cap * s1 + 6.0 * spread, cap * s2, cap * s3 + 6.0 * spread
        scale = OMEGA / (top * bottom + coupling * coupling)
        table[j, 0] = bottom * scale
        table[j, 1] = coupling * scale
        table[j, 2] = top * scale
        table[j, 3] = cap


HALO = 2
TOGETHER = 2
PARTS = 2


def whole_kernel(groups, slabs, shift_table, residual_hbm, capacity_hbm, out_ref, *scratch):
    (
        res, loc, far, seq, sendx, field, inverse0, vtwo, coarse_out, gathered, back, edges,
        result, merged, wave, gotb, outgoing, table, near_cap,
    ) = scratch[:19]
    depth = GRID_DEPTH
    rest = scratch[19:]
    caps, rest = rest[:depth], rest[depth:]
    tables, rest = (None,) + rest[: depth - 1], rest[depth - 1 :]
    (
        own, far_send, far_recv, loc_send, loc_recv, x_send, x_recv, d_send, d_recv, h_send, h_recv,
        e_send, e_recv, g_send, g_recv, b_send, b_recv, r_send, r_recv, w_send, w_recv, o_send,
        o_recv, c_send, c_recv, n_send, n_recv, ready,
    ) = rest
    steps, thick = res.shape[:2]
    half = thick // 2
    slots = field.shape[1] // 2
    wide = thick + 2 * HALO
    length = groups * steps
    rate = ALPHA_CORNER ** (1.0 / length)
    tile = res.shape[-2:]
    m, s = lax.axis_index("tm"), lax.axis_index("space")
    y, x = m // 2, lax.rem(m, 2)
    z, c = s // 2, lax.rem(s, 2)
    layers = slabs // 2
    sig = lax.rem(y + z, 2)
    slab = 2 * z + sig
    keeper = sig == c
    side = lax.rem(c + x, 2)
    part_steps = steps // PARTS
    is_low, is_high = slab == 0, slab == slabs - 1

    def at(ty, tx, tz, tc):
        return (2 * ty + tx, 2 * tz + tc)

    def plane_of(h, i):
        return i if h == 0 else thick - 1 - i

    def drain(ref, semaphore):
        pltpu.make_async_copy(ref, ref, semaphore).wait()

    def send(source, target, send_sem, recv_sem, device):
        pltpu.make_async_remote_copy(
            src_ref=source,
            dst_ref=target,
            send_sem=send_sem,
            recv_sem=recv_sem,
            device_id=device,
            device_id_type=MESH,
        ).start()

    take_residual = pltpu.make_async_copy(residual_hbm, res, own.at[0])
    take_residual.start()
    own_slab = pl.ds(s * thick, thick)
    take_capacity = pltpu.make_async_copy(capacity_hbm, caps[0].at[own_slab], own.at[1])
    take_capacity.start()
    near_slab = pl.ds((2 + c) * thick, thick)
    take_near = pltpu.make_async_copy(capacity_hbm, near_cap.at[near_slab], own.at[2])
    take_near.start()

    barrier = pltpu.get_barrier_semaphore()
    below, above = z > 0, z < layers - 1
    sides = jnp.where(below, 1, 0) + jnp.where(above, 1, 0)

    def greet(device):
        pl.semaphore_signal(barrier, inc=1, device_id=device, device_id_type=MESH)

    greet(at(1 - y, x, z, 0))
    greet(at(1 - y, x, z, 1))
    for there, dz in ((below, -1), (above, 1)):

        @pl.when(there)
        def _():
            greet(at(y, x, z + dz, 0))
            greet(at(y, x, z + dz, 1))

    greet(at(y, 1 - x, z, 1 - c))
    greet(at(y, x, z, 1 - c))

    for k in range(shift_table.shape[0]):
        for column in range(3):
            table[k, column] = jnp.float32(shift_table[k, column])
    ones = jnp.ones((thick,) + tile, jnp.float32)

    @pl.when(jnp.logical_not(below))
    def _():
        near_cap[pl.ds(thick, thick)] = ones

    @pl.when(jnp.logical_not(above))
    def _():
        near_cap[pl.ds(4 * thick, thick)] = ones

    @pl.when(is_low)
    def _():
        for j in range(HALO):
            field[j] = jnp.zeros(field.shape[1:], jnp.float32)
        vtwo[0] = jnp.zeros(vtwo.shape[1:], jnp.float32)

    @pl.when(is_high)
    def _():
        for j in range(HALO):
            field[wide - 1 - j] = jnp.zeros(field.shape[1:], jnp.float32)
        vtwo[wide - 1] = jnp.zeros(vtwo.shape[1:], jnp.float32)

    pl.semaphore_wait(barrier, 4 + 2 * sides)

    take_residual.wait()
    for i in range(half):

        @pl.when(keeper)
        def _():
            for h in (0, 1):
                p = plane_of(h, i)

                @pl.when(side == h)
                def _():
                    pltpu.make_async_copy(res.at[:, p], loc.at[i], loc_recv).start()

                @pl.when(side != h)
                def _():
                    send(res.at[:, p], loc.at[i], loc_send, loc_recv, at(y, x, z, 1 - c))

        @pl.when(jnp.logical_not(keeper))
        def _():
            for k in range(PARTS):
                span = pl.ds(k * part_steps, part_steps)
                for h in (0, 1):
                    send(
                        res.at[span, plane_of(h, i)], far.at[i, span], far_send,
                        far_recv.at[i, k], at(1 - y, x, z, lax.rem(h + x, 2)),
                    )

    take_near.wait()
    send(
        near_cap.at[near_slab], near_cap.at[near_slab], n_send.at[0], n_recv.at[2],
        at(y, x, z, 1 - c),
    )
    near_there = jnp.where(c == 0, below, above)

    @pl.when(near_there)
    def _():
        for k in (0, 1):
            send(
                near_cap.at[near_slab],
                near_cap.at[pl.ds((4 - 3 * c) * thick, thick)],
                n_send.at[1],
                n_recv.at[1 - c],
                at(y, x, z + 2 * c - 1, k),
            )

    def tell_sides(turn):
        for there, dz in ((below, -1), (above, 1)):

            @pl.when(there)
            def _():
                pl.semaphore_signal(
                    ready.at[turn], inc=1, device_id=at(y, x, z + dz, c), device_id_type=MESH
                )

    def hear_sides(turn):
        pl.semaphore_wait(ready.at[turn], sides)

    def share_capacity():
        take_capacity.wait()
        for d in range(1, layers):
            send(
                caps[0].at[own_slab],
                caps[0].at[own_slab],
                c_send,
                c_recv.at[d],
                (m, lax.rem(s + 2 * d, slabs)),
            )
        forward_cap(0)

    def rows_from(d):
        return pl.ds(lax.rem(s + slabs - 2 * d, slabs) * thick, thick)

    def forward_cap(d):
        rows = rows_from(d)
        send(
            caps[0].at[rows],
            caps[0].at[rows],
            c_send,
            c_recv.at[0],
            at(y, x, z, 1 - c),
        )

    def power(ty):
        exponent = [rate ** (a * length // 2 + b * steps) for a in (0, 1) for b in (0, 1)]
        low = jnp.where(x == 0, jnp.float32(exponent[0]), jnp.float32(exponent[1]))
        high = jnp.where(x == 0, jnp.float32(exponent[2]), jnp.float32(exponent[3]))
        return jnp.where(ty == 0, low, high)

    here_power, there_power = power(y), power(1 - y)
    sign = jnp.where(y == 0, 1.0, -1.0).astype(jnp.float32)
    first_x = x == 0
    keep_own = jnp.where(first_x, here_power, sign * here_power)
    keep_far = jnp.where(first_x, there_power, -sign * there_power)
    give_own = jnp.where(first_x, sign * here_power, here_power)
    give_far = jnp.where(first_x, -sign * there_power, there_power)

    def combine(i):
        if i == 0:
            drain(loc, loc_recv)
        for k in range(PARTS):
            span = pl.ds(k * part_steps, part_steps)
            drain(far.at[i, span], far_recv.at[i, k])
            for t in range(k * part_steps, (k + 1) * part_steps):
                a, b = loc[i, t] * (rate**t), far[i, t] * (rate**t)
                sendx[i, t] = give_own * a + give_far * b
            send(
                sendx.at[i, span],
                seq.at[i, pl.ds(x * steps + k * part_steps, part_steps)],
                x_send,
                x_recv.at[i, k],
                at(y, 1 - x, z, 1 - c),
            )
            for t in range(k * part_steps, (k + 1) * part_steps):
                a, b = loc[i, t] * (rate**t), far[i, t] * (rate**t)
                seq[i, x * steps + t] = keep_own * a + keep_far * b

    in_layer = side != sig
    halo_y = jnp.where(in_layer, 1 - y, y)
    halo_z = jnp.where(in_layer, z, z + 2 * side - 1)
    halo_there = jnp.logical_or(in_layer, jnp.logical_and(halo_z >= 0, halo_z < layers))

    def transform(i):
        for k in range(PARTS):
            drain(sendx.at[i, pl.ds(0, part_steps)], x_recv.at[i, k])
        plane = jnp.where(side == 0, i, thick - 1 - i) + HALO

        @pl.when(x == 0)
        def _():
            modes = real_transform([seq[i, t] for t in range(2 * steps)])
            field[plane, 0, 0] = modes[0][0]
            field[plane, 0, 1] = modes[steps][0]
            for k in range(1, steps):
                field[plane, k, 0] = modes[k][0]
                field[plane, k, 1] = modes[k][1]

        @pl.when(x == 1)
        def _():
            modes = odd_transform([seq[i, t] for t in range(2 * steps)])
            for k in range(steps):
                field[plane, k, 0] = modes[k][0]
                field[plane, k, 1] = modes[k][1]

        given = field.at[plane, pl.ds((1 - c) * slots, slots)]
        send(given, given, d_send, d_recv, at(y, x, z, 1 - c))
        if i < HALO:
            target = plane + thick * (1 - 2 * side)

            @pl.when(halo_there)
            def _():
                for k in (0, 1):
                    part = pl.ds(k * slots, slots)
                    send(
                        field.at[plane, part],
                        field.at[target, part],
                        h_send,
                        h_recv.at[1 - side],
                        at(halo_y, x, halo_z, k),
                    )

    def shifts_of(slot):
        return tuple(table[slot, column] for column in range(3))

    even_row, even_lane = parity(tile, 0), parity(tile, 1)
    solver_shifts = shifts_of(x * 2 * slots + (1 - c) * slots + slab)

    def pass_capacity():
        for d in range(1, layers):
            drain(caps[0].at[rows_from(d)], c_recv.at[d])
            forward_cap(d)

    def coarse_tables():
        drain(caps[0].at[pl.ds(0, layers * thick)], c_recv.at[0])
        for level in range(1, depth):
            caps[level][...] = block_mean(caps[level - 1][...], 2 ** (level - 1))
            compact_table(level, caps[level], tables[level], solver_shifts, even_row)

    spread0, unused = level_coefficients(0)

    cap_base = (2 + sig) * thick - HALO

    def fine_tables():
        drain(near_cap.at[near_slab], n_recv.at[2])

        @pl.when(below)
        def _():
            drain(near_cap.at[near_slab], n_recv.at[0])

        @pl.when(above)
        def _():
            drain(near_cap.at[near_slab], n_recv.at[1])

        inside = [jnp.float32(1.0)] * wide
        for j in range(HALO):
            inside[j] = jnp.where(is_low, 0.0, 1.0).astype(jnp.float32)
            inside[wide - 1 - j] = jnp.where(is_high, 0.0, 1.0).astype(jnp.float32)

        def body(f, carry):
            s1, s2, s3 = shifts_of(x * 2 * slots + c * slots + f)
            for j in range(wide):
                cap = near_cap[cap_base + j]
                top, coupling = cap * s1 + 6.0 * spread0, cap * s2
                bottom = cap * s3 + 6.0 * spread0
                scale = (OMEGA * inside[j]) / (top * bottom + coupling * coupling)
                inverse0[f, j, 0] = bottom * scale
                inverse0[f, j, 1] = coupling * scale
                inverse0[f, j, 2] = top * scale
            return carry

        lax.fori_loop(0, slots, body, 0)

    for turn in range(layers - 1):
        tell_sides(turn)
        if turn > 0:
            combine(turn - 1)
        hear_sides(turn)
    share_capacity()
    for i in range(layers - 2, half - 1):
        combine(i)
    transform(0)
    combine(half - 1)
    for i in range(1, half):
        transform(i)
        if i == 1:
            fine_tables()
    pass_capacity()

    weights = neighbour_weights(0, tile)

    def slot_at(i):
        total, unit, rest_g, rest_i = 0, 1, slab, i
        while unit < slots:
            bit = lax.rem(lax.rem(rest_g, 2) + lax.rem(rest_i, 2), 2)
            total = total + unit * bit
            rest_g, rest_i = rest_g // 2, rest_i // 2
            unit *= 2
        return total

    def member(g):
        gz, gs = g // 2, lax.rem(g, 2)
        return at(lax.rem(gs + gz, 2), x, gz, 1 - c)

    given_planes = field.at[pl.ds(0, half), pl.ds(0, slots)]
    halo_planes = field.at[pl.ds(0, HALO), pl.ds(0, slots)]
    drain(given_planes, d_recv)
    for end, there in ((0, jnp.logical_not(is_low)), (1, jnp.logical_not(is_high))):

        @pl.when(there)
        def _():
            drain(halo_planes, h_recv.at[end])

    def load_slot(f):
        q = c * slots + f
        forcing = [(field[j, q, 0], field[j, q, 1]) for j in range(wide)]
        inverse = [[inverse0[f, j, k] for k in range(3)] for j in range(wide)]
        return forcing, inverse

    def residual_at(forcing, second, j, shifts):
        s1, s2, s3 = shifts
        cap = near_cap[cap_base + j]
        re, im = second[j]
        turn = (s1 * re - s2 * im, s2 * re + s3 * im)
        found = []
        for part in (0, 1):
            total = forcing[j][part] - neighbour_sum(
                *(second[n][part] for n in (j - 1, j, j + 1)), weights
            )
            found.append(total - (6.0 * spread0 * second[j][part] + cap * turn[part]))
        return found

    def down(i, carry):
        chosen = [slot_at(slots - 1 - TOGETHER * i - k) for k in range(TOGETHER)]
        loaded = [load_slot(f) for f in chosen]
        shifts = [shifts_of(x * 2 * slots + c * slots + f) for f in chosen]
        first = [[] for f in chosen]
        second = [[None] for f in chosen]
        for j in range(wide):
            for n, (forcing, inverse) in enumerate(loaded):
                (re, im), (a, b, d) = forcing[j], inverse[j]
                first[n].append((a * re + b * im, d * im - b * re))
        for j in range(1, wide - 1):
            for n, (forcing, inverse) in enumerate(loaded):
                second[n].append(updated(forcing[j], inverse[j], first[n][j - 1 : j + 2], weights))
                for part in (0, 1):
                    vtwo[j, chosen[n], part] = second[n][j][part]
        for pair in range(thick // 4):
            packed = [[[None, None], [None, None]] for f in chosen]
            for plane in (0, 1):
                for k in (0, 1):
                    for n, (forcing, inverse) in enumerate(loaded):
                        j = HALO + 4 * pair + 2 * plane + k
                        rest = residual_at(forcing, second[n], j, shifts[n])
                        for part in (0, 1):
                            sofar = packed[n][plane][part]
                            packed[n][plane][part] = rest[part] if k == 0 else sofar + rest[part]
            for n, f in enumerate(chosen):
                coarse_out[f, pair] = 0.125 * pack_means(*packed[n], even_row, even_lane)

        tiles = pl.ds(slab * (thick // 4), thick // 4)
        for f in chosen:
            send(coarse_out.at[f], gathered.at[tiles], g_send, g_recv, member(f))

        return carry

    lax.fori_loop(0, slots // TOGETHER, down, 0)

    low_y, low_z = jnp.where(sig == 0, y, 1 - y), jnp.where(sig == 0, z - 1, z)
    high_y, high_z = jnp.where(sig == 0, 1 - y, y), jnp.where(sig == 0, z, z + 1)

    @pl.when(jnp.logical_not(is_low))
    def _():
        send(
            vtwo.at[HALO + 1], vtwo.at[wide - 1], e_send.at[0], e_recv.at[1], at(low_y, x, low_z, c)
        )

    @pl.when(jnp.logical_not(is_high))
    def _():
        send(
            vtwo.at[wide - HALO - 2], vtwo.at[0], e_send.at[1], e_recv.at[0],
            at(high_y, x, high_z, c),
        )

    coarse_tables()
    drain(gathered, g_recv)
    tiles_in = slabs * thick // 4
    unpacked = []
    for j in range(tiles_in):
        cells = gathered[j]
        re = jnp.where(even_lane, cells, shifted(cells, 1, 1))
        im = jnp.where(even_lane, shifted(cells, -1, 1), cells)
        unpacked.append((re, im))
    coarse = compact_cycle(1, unpacked, tables, solver_shifts, even_row)
    packed_cells = [jnp.where(even_lane, re, im) for re, im in coarse]
    empty = jnp.zeros(tile, jnp.float32)
    for j in range(tiles_in + 1):
        back[j] = jnp.where(
            even_row,
            packed_cells[j] if j < tiles_in else empty,
            packed_cells[j - 1] if j > 0 else empty,
        )
    span = thick // 4 + 1

    def give(i, carry):
        g = slot_at(slots - 1 - i)
        send(
            back.at[pl.ds(g * (thick // 4), span)], edges.at[slab], b_send, b_recv.at[slab],
            member(g),
        )
        return carry

    lax.fori_loop(0, slots, give, 0)

    for end, there in ((0, jnp.logical_not(is_low)), (1, jnp.logical_not(is_high))):

        @pl.when(there)
        def _():
            drain(vtwo.at[0], e_recv.at[end])
            drain(vtwo.at[0], e_send.at[end])

    def up(i, carry):
        chosen = [slot_at(TOGETHER * i + k) for k in range(TOGETHER)]
        for f in chosen:
            drain(edges.at[0], b_recv.at[f])

        loaded = [load_slot(f) for f in chosen]
        start = [[] for f in chosen]
        third = [[None] for f in chosen]
        for k in range(span):
            for n, f in enumerate(chosen):
                for u, extra in enumerate(unpack_cells(edges[f, k], even_row, even_lane)[::-1]):
                    for j in (4 * k + 2 * u, 4 * k + 2 * u + 1):
                        start[n].append([vtwo[j, f, part] + extra[part] for part in (0, 1)])
        for j in range(1, wide - 1):
            for n, (forcing, inverse) in enumerate(loaded):
                third[n].append(updated(forcing[j], inverse[j], start[n][j - 1 : j + 2], weights))
        for j in range(HALO, wide - HALO):
            for n, (forcing, inverse) in enumerate(loaded):
                parts = updated(forcing[j], inverse[j], third[n][j - 1 : j + 2], weights)
                for part in (0, 1):
                    result[chosen[n], j - HALO, part] = parts[part]
        for f in chosen:
            q = c * slots + f
            send(
                result.at[f, pl.ds((1 - side) * half, half)], merged.at[q], r_send, r_recv,
                at(y, x, z, 1 - c),
            )
            for k in range(half):
                merged[q, k] = result[f, side * half + k]
        return carry

    lax.fori_loop(0, slots // TOGETHER, up, 0)
    drain(merged.at[pl.ds(0, slots)], r_recv)

    def invert(i):
        @pl.when(x == 0)
        def _():
            modes = [(merged[0, i, 0], None)]
            modes += [(merged[k, i, 0], merged[k, i, 1]) for k in range(1, steps)]
            modes += [(merged[0, i, 1], None)]
            for t, value in enumerate(real_inverse(modes)):
                wave[i, t] = value

        @pl.when(x == 1)
        def _():
            modes = [(merged[k, i, 0], merged[k, i, 1]) for k in range(steps)]
            for t, value in enumerate(odd_inverse(modes)):
                wave[i, t] = value

        for k in range(PARTS):
            send(
                wave.at[i, pl.ds((1 - x) * steps + k * part_steps, part_steps)],
                gotb.at[i, pl.ds(k * part_steps, part_steps)], w_send, w_recv.at[i, k],
                at(y, 1 - x, z, 1 - c),
            )

    inverse_here = 1.0 / (here_power * length)
    inverse_there = 1.0 / (there_power * length)
    own_sign = jnp.where(first_x, 1.0, sign).astype(jnp.float32)
    got_sign = jnp.where(first_x, sign, 1.0).astype(jnp.float32)
    far_own = jnp.where(first_x, 1.0, -sign).astype(jnp.float32)
    far_got = jnp.where(first_x, -sign, 1.0).astype(jnp.float32)

    def finish(i, k):
        span = pl.ds(k * part_steps, part_steps)
        drain(gotb.at[i, span], w_recv.at[i, k])
        p = side * half + i
        for t in range(k * part_steps, (k + 1) * part_steps):
            mine = wave[i, x * steps + t] * (rate**-t)
            got = gotb[i, t] * (rate**-t)
            outgoing[1, i, t] = (far_own * inverse_there) * mine + (far_got * inverse_there) * got
        send(
            outgoing.at[1, i, span], out_ref.at[span, p], o_send.at[1], o_recv,
            at(1 - y, x, z, sig),
        )

        def own_value(t):
            mine = wave[i, x * steps + t] * (rate**-t)
            got = gotb[i, t] * (rate**-t)
            return (own_sign * inverse_here) * mine + (got_sign * inverse_here) * got

        @pl.when(keeper)
        def _():
            for t in range(k * part_steps, (k + 1) * part_steps):
                out_ref[t, p] = own_value(t)

        @pl.when(jnp.logical_not(keeper))
        def _():
            for t in range(k * part_steps, (k + 1) * part_steps):
                outgoing[0, i, t] = own_value(t)
            send(
                outgoing.at[0, i, span], out_ref.at[span, p], o_send.at[0], o_recv,
                at(y, x, z, 1 - c),
            )

    for i in range(half):
        invert(i)
    for i in range(half):
        for k in range(PARTS):
            finish(i, k)

    @pl.when(keeper)
    def _():
        drain(loc, o_recv)
        drain(loc, loc_send)

    @pl.when(jnp.logical_not(keeper))
    def _():
        drain(res, o_recv)
        drain(res, far_send)
        drain(loc, o_send.at[0])

    drain(loc, o_send.at[1])
    drain(loc, x_send)
    drain(loc, w_send)
    drain(given_planes, d_send)

    @pl.when(halo_there)
    def _():
        drain(field.at[pl.ds(0, 2 * HALO), pl.ds(0, slots)], h_send)

    drain(gathered, g_send)
    drain(edges, b_send)
    drain(merged.at[pl.ds(0, slots)], r_send)
    drain(near_cap.at[near_slab], n_send.at[0])

    @pl.when(near_there)
    def _():
        drain(near_cap.at[pl.ds(0, 2 * thick)], n_send.at[1])

    drain(caps[0].at[pl.ds(0, (2 * layers - 1) * thick)], c_send)


def level_extents(extent):
    return [extent // 2**level for level in range(GRID_DEPTH)]


def fused(groups, slabs, residual, capacity):
    steps, thick, second, third = residual.shape
    length = groups * steps
    half, slots = thick // 2, steps // 2
    extent, wide = slabs * thick, thick + 2 * HALO
    tile = (second, third)
    ratio_step = ALPHA_CORNER ** (1.0 / length)
    numbers = [2 * k for k in range(steps)] + [4 * k + 1 for k in range(steps)]
    angle = 2.0 * np.pi / length * np.array(numbers)
    table = np.stack(
        [
            (1.0 - ratio_step * np.cos(angle)) / STEP_SIZE,
            ratio_step * np.sin(angle) / STEP_SIZE,
            (1.0 - ratio_step * np.cos(angle)) / STEP_SIZE,
        ],
        axis=1,
    )
    table[0, 1], table[0, 2] = 0.0, (1.0 + ratio_step) / STEP_SIZE
    extents = level_extents(extent)
    vmem = lambda *shape: pltpu.VMEM(shape + tile, jnp.float32)
    sems = lambda *shape: pltpu.SemaphoreType.DMA(shape)
    one = pltpu.SemaphoreType.DMA
    layers, quarter = slabs // 2, thick // 4
    scratch = [
        vmem(steps, thick),
        vmem(half, steps),
        vmem(half, steps),
        vmem(half, 2 * steps),
        vmem(half, steps),
        vmem(wide, 2 * slots, 2),
        vmem(slots, wide, 3),
        vmem(wide, slots, 2),
        vmem(slots, quarter),
        vmem(slabs * quarter),
        vmem(slabs * quarter + 1),
        vmem(slots, quarter + 1),
        vmem(slots, thick, 2),
        vmem(2 * slots, half, 2),
        vmem(half, 2 * steps),
        vmem(half, steps),
        vmem(2, half, steps),
        pltpu.SMEM(table.shape, jnp.float32),
        vmem(6 * thick),
        *[vmem(n) for n in extents],
        *[vmem(n // 2, 4) for n in extents[1:]],
        sems(3),
        one,
        sems(half, PARTS),
        one,
        one,
        one,
        sems(half, PARTS),
        one,
        one,
        one,
        sems(2),
        sems(2),
        sems(2),
        one,
        one,
        one,
        sems(slots),
        one,
        one,
        one,
        sems(half, PARTS),
        sems(2),
        one,
        one,
        sems(layers),
        sems(2),
        sems(3),
        pltpu.SemaphoreType.REGULAR((layers - 1,)),
    ]
    return pl.pallas_call(
        functools.partial(whole_kernel, groups, slabs, table),
        out_shape=jax.ShapeDtypeStruct(residual.shape, jnp.float32),
        in_specs=[
            pl.BlockSpec(memory_space=pltpu.HBM),
            pl.BlockSpec(memory_space=pltpu.HBM),
        ],
        out_specs=pl.BlockSpec(memory_space=pltpu.VMEM),
        scratch_shapes=scratch,
        compiler_params=pltpu.CompilerParams(
            collective_id=0, has_side_effects=True, vmem_limit_bytes=32 * 2**20
        ),
    )(*[pltpu.with_memory_space_constraint(a, pltpu.HBM) for a in (residual, capacity)])


def fits_fused(groups, slabs, residual):
    steps, thick, second, third = residual.shape
    length = groups * steps
    power = length & (length - 1) == 0
    return (
        power
        and groups == 4
        and slabs % 2 == 0
        and slabs == length // 8
        and thick == 8
        and all(n % 2 == 0 and n % n == 0 for n in level_extents(slabs * thick))
        and (second, third) == (8, 128)
    )


def either(residual, capacity):
    groups, slabs = lax.axis_size("tm"), lax.axis_size("space")
    if fits_fused(groups, slabs, residual):
        return fused(groups, slabs, residual, capacity)
    return on_device(residual, capacity)


def solution(mesh):
    return jax.shard_map(
        either,
        mesh=mesh,
        in_specs=(P("tm", "space", None, None), P("space", None, None)),
        out_specs=P("tm", "space", None, None),
        check_vma=False,
    )
```

```python
import functools
import math

import jax
import jax.numpy as jnp
import numpy as np
from jax import lax
from jax.experimental import pallas as pl
from jax.experimental.pallas import tpu as pltpu
from jax.sharding import PartitionSpec as P

GRID_DEPTH = 4
SMOOTH = 2
COARSE_SWEEPS = 6


ALPHA_CORNER = 0.01
STEP_SIZE = 0.5
DIFFUSE = 2.0
ADVECT = (0.2, -0.15, 0.1)
OMEGA = 0.7
HIGHEST = lax.Precision.HIGHEST


def extended(array, sides, width):
    for axis, dim in sides:
        peers, length = (lax.axis_size(axis), array.shape[dim])
        up = [(i, (i + 1) % peers) for i in range(peers - 1)]
        down = [(j, i) for i, j in up]
        last = lax.slice_in_dim(array, length - width, length, axis=dim)
        initial = lax.slice_in_dim(array, 0, width, axis=dim)
        before = lax.ppermute(last, axis, up)
        after = lax.ppermute(initial, axis, down)
        array = jnp.concatenate([before, array, after], axis=dim)
    return array


def level_coefficients(per_level_values):
    spread = DIFFUSE / 4.0**per_level_values
    drifts = tuple((component / 2.0**per_level_values for component in ADVECT))
    return (spread, drifts)


def pad_second(volume, position):
    widths = [(0, 0)] * volume.ndim
    widths[position] = (1, 1)
    return jnp.pad(volume, widths)


def apply_operator(padded, current_capacity, spectral_shifts, per_level_values):
    spread, drifts = level_coefficients(per_level_values)
    centre = padded[:, :, 1:-1]
    upper_first = padded[:, :, 2:]
    lower_first = padded[:, :, :-2]
    wide_second = pad_second(centre, 3)
    upper_second = wide_second[:, :, :, 2:]
    lower_second = wide_second[:, :, :, :-2]
    wide_third = pad_second(centre, 4)
    upper_third = wide_third[:, :, :, :, 2:]
    lower_third = wide_third[:, :, :, :, :-2]
    stencil = spread * (
        6.0 * centre
        - upper_first
        - lower_first
        - upper_second
        - lower_second
        - upper_third
        - lower_third
    )
    stencil = (
        stencil
        + drifts[0] * (upper_first - lower_first)
        + drifts[1] * (upper_second - lower_second)
        + drifts[2] * (upper_third - lower_third)
    )
    first_shift, second_shift, third_shift = spectral_shifts
    real_part = centre[0]
    imag_part = centre[1]
    shifted = jnp.stack(
        [
            current_capacity * (first_shift * real_part - second_shift * imag_part),
            current_capacity * (second_shift * real_part + third_shift * imag_part),
        ]
    )
    return stencil + shifted


def inverse_diagonal(current_capacity, spectral_shifts, per_level_values):
    spread, drifts = level_coefficients(per_level_values)
    first_shift, second_shift, third_shift = spectral_shifts
    top_left = current_capacity * first_shift + 6.0 * spread
    coupling = current_capacity * second_shift
    bottom_right = current_capacity * third_shift + 6.0 * spread
    determinant = top_left * bottom_right + coupling * coupling
    return (bottom_right / determinant, coupling / determinant, top_left / determinant)


def damped_update(residual_now, inverse):
    diagonal_a, diagonal_b, diagonal_c = inverse
    return OMEGA * jnp.stack(
        [
            diagonal_a * residual_now[0] + diagonal_b * residual_now[1],
            diagonal_c * residual_now[1] - diagonal_b * residual_now[0],
        ]
    )


def restrict_to_coarse(volume):
    leading = volume.shape[:-3]
    first_extent, second_extent, third_extent = volume.shape[-3:]
    blocks = volume.reshape(
        leading + (first_extent // 2, 2, second_extent // 2, 2, third_extent // 2, 2)
    )
    lead_count = len(leading)
    return jnp.mean(blocks, axis=(lead_count + 1, lead_count + 3, lead_count + 5))


def prolong_cells(volume):
    leading = volume.shape[:-3]
    first_extent, second_extent, third_extent = volume.shape[-3:]
    expanded = jnp.broadcast_to(
        volume[..., :, None, :, None, :, None],
        leading + (first_extent, 2, second_extent, 2, third_extent, 2),
    )
    return expanded.reshape(leading + (2 * first_extent, 2 * second_extent, 2 * third_extent))


def shift_values(frequency, length):
    ratio_step = ALPHA_CORNER ** (1.0 / length)
    phases = 2.0 * math.pi / length * frequency.astype(jnp.float32)
    first_shift = (1.0 - ratio_step * jnp.cos(phases)) / STEP_SIZE
    second_shift = ratio_step * jnp.sin(phases) / STEP_SIZE
    leading = frequency == 0
    second_shift = jnp.where(leading, 0.0, second_shift)
    third_shift = jnp.where(leading, (1.0 + ratio_step) / STEP_SIZE, first_shift)
    return tuple(
        (column.reshape(-1, 1, 1, 1) for column in (first_shift, second_shift, third_shift))
    )


def phase_grid(row_count, length):
    integers = (
        jnp.arange(row_count, dtype=jnp.int32)[:, None]
        * jnp.arange(length, dtype=jnp.int32)[None, :]
        % length
    )
    return 2.0 * math.pi / length * integers.astype(jnp.float32)


def pad_faces(volume):
    return extended(volume, (("space", 2),), 1)


def multigrid_cycle(
    per_level_values,
    forcing_term,
    capacity_fields,
    spectral_shifts,
    shared_values,
    assemble_level,
    assemble_parts,
):
    current_capacity = capacity_fields[per_level_values]
    inverse = inverse_diagonal(current_capacity, spectral_shifts, per_level_values)
    coarsest = per_level_values == GRID_DEPTH - 1
    current = damped_update(forcing_term, inverse)
    for repeat in range((COARSE_SWEEPS if coarsest else SMOOTH) - 1):
        current = current + damped_update(
            forcing_term
            - apply_operator(
                pad_faces(current), current_capacity, spectral_shifts, per_level_values
            ),
            inverse,
        )
    if coarsest:
        return current
    coarse_right_hand = restrict_to_coarse(
        forcing_term
        - apply_operator(pad_faces(current), current_capacity, spectral_shifts, per_level_values)
    )
    coarse_solution = multigrid_cycle(
        per_level_values + 1,
        coarse_right_hand,
        capacity_fields,
        spectral_shifts,
        shared_values,
        assemble_level,
        assemble_parts,
    )
    current = current + prolong_cells(coarse_solution)
    for repeat in range(SMOOTH):
        current = current + damped_update(
            forcing_term
            - apply_operator(
                pad_faces(current), current_capacity, spectral_shifts, per_level_values
            ),
            inverse,
        )
    return current


def on_device(residual, capacity):
    steps_here, thickness, extent_second, extent_third = residual.shape
    length = lax.axis_size("tm") * steps_here
    ratio_step = ALPHA_CORNER ** (1.0 / length)
    moments = (lax.axis_index("tm") * steps_here + jnp.arange(steps_here, dtype=jnp.int32)).astype(
        jnp.float32
    )
    scaled = (residual * jnp.power(ratio_step, moments)[:, None, None, None]).reshape(
        steps_here, -1
    )
    series = lax.all_to_all(scaled, "tm", split_axis=1, concat_axis=0, tiled=True)
    all_weights = jnp.power(ratio_step, jnp.arange(length, dtype=jnp.float32))
    alternate = 1.0 - 2.0 * (jnp.arange(length, dtype=jnp.int32) % 2).astype(jnp.float32)
    capacity_fields = [capacity]
    for per_level_values in range(1, GRID_DEPTH):
        capacity_fields.append(restrict_to_coarse(capacity_fields[-1]))
    halves = length // 2
    phases = phase_grid(halves, length)
    first_row = jnp.arange(halves, dtype=jnp.int32)[:, None] == 0
    forward = jnp.concatenate(
        [jnp.cos(phases), jnp.where(first_row, alternate[None, :], -jnp.sin(phases))], axis=0
    )
    spectrum = jnp.dot(forward, series, precision=HIGHEST).reshape(2, halves, -1)
    received = lax.all_to_all(spectrum, "tm", split_axis=1, concat_axis=2, tiled=True)
    slot_count = steps_here // 2
    frequency = lax.axis_index("tm") * slot_count + jnp.arange(slot_count, dtype=jnp.int32)
    spectral_shifts = shift_values(frequency, length)
    field_list = received.reshape(2, slot_count, thickness, extent_second, extent_third)
    solved_fields = multigrid_cycle(
        0, field_list, capacity_fields, spectral_shifts, False, GRID_DEPTH, None
    )
    flattened = solved_fields.reshape(2, slot_count, -1)
    returned = lax.all_to_all(flattened, "tm", split_axis=2, concat_axis=1, tiled=True)
    halves = length // 2
    phases = jnp.transpose(phase_grid(halves, length))
    first_column = jnp.arange(halves, dtype=jnp.int32)[None, :] == 0
    real_columns = jnp.where(first_column, 1.0, 2.0 * jnp.cos(phases)) / length
    imag_columns = jnp.where(first_column, alternate[:, None], -2.0 * jnp.sin(phases)) / length
    inverse_table = jnp.concatenate([real_columns, imag_columns], axis=1)
    values = jnp.dot(
        inverse_table,
        returned.reshape(returned.shape[0] * returned.shape[1], -1),
        precision=HIGHEST,
    )
    values = values / all_weights[:, None]
    result = lax.all_to_all(values, "tm", split_axis=0, concat_axis=1, tiled=True)
    return result.reshape(residual.shape)


MESH = pl.DeviceIdType.MESH


def real_transform(values):
    count = len(values)
    if count == 1:
        return [(values[0], None)]
    evens, odds = real_transform(values[0::2]), real_transform(values[1::2])
    half = count // 2
    if count == 2:
        return [(evens[0][0] + odds[0][0], None), (evens[0][0] - odds[0][0], None)]
    found = [None] * (half + 1)
    found[0] = (evens[0][0] + odds[0][0], None)
    found[half] = (evens[0][0] - odds[0][0], None)
    found[half // 2] = (evens[half // 2][0], -odds[half // 2][0])
    for k in range(1, half // 2):
        cosine, sine = math.cos(2 * math.pi * k / count), -math.sin(2 * math.pi * k / count)
        (er, ei), (or_, oi) = evens[k], odds[k]
        tr, ti = cosine * or_ - sine * oi, cosine * oi + sine * or_
        found[k] = (er + tr, ei + ti)
        found[half - k] = (er - tr, ti - ei)
    return found


def real_inverse(modes):
    half = len(modes) - 1
    if half == 0:
        return [modes[0][0]]
    count = 2 * half
    if half == 1:
        return [modes[0][0] + modes[1][0], modes[0][0] - modes[1][0]]
    evens, odds = [None] * (half // 2 + 1), [None] * (half // 2 + 1)
    evens[0] = (modes[0][0] + modes[half][0], None)
    odds[0] = (modes[0][0] - modes[half][0], None)
    middle = modes[half // 2]
    evens[half // 2] = (2.0 * middle[0], None)
    odds[half // 2] = (-2.0 * middle[1], None)
    for k in range(1, half // 2):
        cosine, sine = math.cos(2 * math.pi * k / count), math.sin(2 * math.pi * k / count)
        (ar, ai), (br, bi) = modes[k], modes[half - k]
        dr, di = ar - br, ai + bi
        evens[k] = (ar + br, ai - bi)
        odds[k] = (cosine * dr - sine * di, cosine * di + sine * dr)
    first, second = real_inverse(evens), real_inverse(odds)
    return [part for pair in zip(first, second) for part in pair]


def pair_sum(value, distance):
    for axis in (-2, -1):
        dim = value.ndim + axis
        extent = value.shape[dim]
        upper = pltpu.roll(value, extent - distance, dim)
        lower = pltpu.roll(value, distance, dim)
        place = lax.broadcasted_iota(jnp.int32, value.shape, dim)
        value = value + jnp.where((place // distance) % 2 == 0, upper, lower)
    return value


def block_mean(value, distance):
    shape = (value.shape[0] // 2, 2) + value.shape[1:]
    paired = value.reshape(shape)
    return 0.125 * pair_sum(paired[:, 0] + paired[:, 1], distance)


def neighbour_weights(level, shape):
    spread, drifts = level_coefficients(level)
    distance = 2**level
    along_first = (drifts[0] - spread, -drifts[0] - spread)
    masked = []
    for dim in (0, 1):
        place = lax.broadcasted_iota(jnp.int32, shape, dim)
        upper = jnp.where(place < shape[dim] - distance, drifts[dim + 1] - spread, 0.0)
        lower = jnp.where(place >= distance, -drifts[dim + 1] - spread, 0.0)
        masked.append((upper, lower))
    return along_first, masked, distance


def complex_transform(values, sign):
    count = len(values)
    if count == 1:
        return values
    evens, odds = complex_transform(values[0::2], sign), complex_transform(values[1::2], sign)
    first, second = [], []
    for k in range(count // 2):
        (er, ei), (or_, oi) = evens[k], odds[k]
        tr, ti = turned(or_, oi, k, count, sign)
        first.append((er + tr, ei + ti))
        second.append((er - tr, ei - ti))
    return first + second


def turned(re, im, k, count, sign):
    if k == 0:
        return re, im
    if 4 * k == count:
        return (-im, re) if sign > 0 else (im, -re)
    cosine, sine = math.cos(2 * math.pi * k / count), sign * math.sin(2 * math.pi * k / count)
    return cosine * re - sine * im, cosine * im + sine * re


def odd_transform(values):
    half = len(values) // 2
    folded = [turned(values[s], -values[s + half], s, 4 * half, -1) for s in range(half)]
    return complex_transform(folded, -1)


def odd_inverse(modes):
    half = len(modes)
    folded = complex_transform(modes, 1)
    first, second = [], []
    for s, (re, im) in enumerate(folded):
        re, im = turned(re, im, s, 4 * half, 1)
        first.append(2.0 * re)
        second.append(-2.0 * im)
    return first + second


def parity(shape, dim):
    return lax.broadcasted_iota(jnp.int32, shape, dim) % 2 == 0


def shifted(value, step, dim):
    return pltpu.roll(value, step % value.shape[dim], dim)


def pack_means(first, second, even_row, even_lane):
    rows = []
    for a, b in zip(first, second):
        left = jnp.where(even_row, a, shifted(b, 1, 0))
        right = jnp.where(even_row, shifted(a, -1, 0), b)
        rows.append(left + right)
    re, im = rows
    left = jnp.where(even_lane, re, shifted(im, 1, 1))
    right = jnp.where(even_lane, shifted(re, -1, 1), im)
    return left + right


def unpack_cells(tile, even_row, even_lane):
    found = []
    for rows in (
        jnp.where(even_row, tile, shifted(tile, 1, 0)),
        jnp.where(even_row, shifted(tile, -1, 0), tile),
    ):
        re = jnp.where(even_lane, rows, shifted(rows, 1, 1))
        im = jnp.where(even_lane, shifted(rows, -1, 1), rows)
        found.append((re, im))
    return found


def around(value, weights):
    unused, masked, distance = weights
    total = 0.0
    for dim in (0, 1):
        upper, lower = masked[dim]
        total = total + upper * shifted(value, -distance, dim)
        total = total + lower * shifted(value, distance, dim)
    return total


def smoothed(first, columns, inverse, weights):
    ahead, behind = weights[0]
    below, here, above = columns
    n0, n1 = (
        ahead * above[k] + behind * below[k] + around(here[k], weights) for k in (0, 1)
    )
    a, b, c = inverse
    return (
        first[0] + (1.0 - OMEGA) * here[0] - (a * n0 + b * n1),
        first[1] + (1.0 - OMEGA) * here[1] - (c * n1 - b * n0),
    )


def compact_rest(forcing, values, weights, even_row):
    along_first, masked, distance = weights
    found = [[None, None] for here in forcing]
    for part in (0, 1):
        column = [value[part] for value in values]
        ups = [shifted(v, -1, 0) for v in column]
        downs = [shifted(v, 1, 0) for v in column]
        for j, value in enumerate(column):
            zero = jnp.zeros_like(value)
            after = downs[j + 1] if j + 1 < len(column) else zero
            before = ups[j - 1] if j > 0 else zero
            total = along_first[0] * jnp.where(even_row, ups[j], after)
            total = total + along_first[1] * jnp.where(even_row, before, downs[j])
            for dim in (0, 1):
                if distance < value.shape[dim]:
                    upper, lower = masked[dim]
                    total = total + upper * shifted(value, -distance, dim)
                    total = total + lower * shifted(value, distance, dim)
            found[j][part] = forcing[j][part] - total
    return found


def compact_sweep(forcing, values, table, weights, even_row):
    found = []
    for j, (r0, r1) in enumerate(compact_rest(forcing, values, weights, even_row)):
        a, b, c = (table[j, k] for k in range(3))
        re, im = values[j]
        found.append(
            (
                (1.0 - OMEGA) * re + (a * r0 + b * r1),
                (1.0 - OMEGA) * im + (c * r1 - b * r0),
            )
        )
    return found


def compact_restrict(values, distance, even_row):
    found = []
    for pair in zip(values[0::2], values[1::2]):
        parts = []
        for first, second in zip(*pair):
            left = jnp.where(even_row, first, shifted(second, 1, 0))
            total = left + jnp.where(even_row, shifted(first, -1, 0), second)
            for dim in (0, 1):
                place = lax.broadcasted_iota(jnp.int32, total.shape, dim)
                upper, lower = shifted(total, -distance, dim), shifted(total, distance, dim)
                total = total + jnp.where((place // distance) % 2 == 0, upper, lower)
            parts.append(0.125 * total)
        found.append(parts)
    return found


def compact_cycle(level, forcing, tables, shifts, even_row):
    table = tables[level]
    spread, unused = level_coefficients(level)
    s1, s2, s3 = shifts
    weights = neighbour_weights(level, forcing[0][0].shape)
    values = []
    for j, (re, im) in enumerate(forcing):
        a, b, c = (table[j, k] for k in range(3))
        values.append((a * re + b * im, c * im - b * re))
    coarsest = level == GRID_DEPTH - 1
    for repeat in range((COARSE_SWEEPS if coarsest else SMOOTH) - 1):
        values = compact_sweep(forcing, values, table, weights, even_row)
    if coarsest:
        return values
    rest = compact_rest(forcing, values, weights, even_row)
    for j, (re, im) in enumerate(values):
        cap = table[j, 3]
        rest[j][0] = rest[j][0] - (6.0 * spread * re + cap * (s1 * re - s2 * im))
        rest[j][1] = rest[j][1] - (6.0 * spread * im + cap * (s2 * re + s3 * im))
    coarse = compact_cycle(
        level + 1, compact_restrict(rest, 2**level, even_row), tables, shifts, even_row
    )
    for j, value in enumerate(coarse):
        values[2 * j] = tuple(
            old + jnp.where(even_row, v, shifted(v, 1, 0)) for old, v in zip(values[2 * j], value)
        )
        values[2 * j + 1] = tuple(
            old + jnp.where(even_row, shifted(v, -1, 0), v)
            for old, v in zip(values[2 * j + 1], value)
        )
    for repeat in range(SMOOTH):
        values = compact_sweep(forcing, values, table, weights, even_row)
    return values


def compact_table(level, caps, table, shifts, even_row):
    spread, unused = level_coefficients(level)
    s1, s2, s3 = shifts
    for j in range(table.shape[0]):
        cap = jnp.where(even_row, caps[2 * j], caps[2 * j + 1])
        top, coupling, bottom = cap * s1 + 6.0 * spread, cap * s2, cap * s3 + 6.0 * spread
        scale = OMEGA / (top * bottom + coupling * coupling)
        table[j, 0] = bottom * scale
        table[j, 1] = coupling * scale
        table[j, 2] = top * scale
        table[j, 3] = cap


HALO = 2
TOGETHER = 2
PARTS = 2


def whole_kernel(groups, slabs, shift_table, residual_hbm, capacity_hbm, out_ref, *scratch):
    (
        res, loc, far, seq, sendx, field, inverse0, vone, vtwo, coarse_out, gathered, back, edges,
        result, merged, wave, gotb, outgoing, table, near_cap,
    ) = scratch[:20]
    depth = GRID_DEPTH
    rest = scratch[20:]
    caps, rest = rest[:depth], rest[depth:]
    tables, rest = (None,) + rest[: depth - 1], rest[depth - 1 :]
    (
        own, far_send, far_recv, loc_send, loc_recv, x_send, x_recv, d_send, d_recv, h_send, h_recv,
        e_send, e_recv, g_send, g_recv, b_send, b_recv, r_send, r_recv, w_send, w_recv, o_send,
        o_recv, c_send, c_recv, n_send, n_recv, ready,
    ) = rest
    steps, thick = res.shape[:2]
    half = thick // 2
    slots = field.shape[1] // 2
    wide = thick + 2 * HALO
    length = groups * steps
    rate = ALPHA_CORNER ** (1.0 / length)
    tile = res.shape[-2:]
    m, s = lax.axis_index("tm"), lax.axis_index("space")
    y, x = m // 2, lax.rem(m, 2)
    z, c = s // 2, lax.rem(s, 2)
    layers = slabs // 2
    sig = lax.rem(y + z, 2)
    slab = 2 * z + sig
    keeper = sig == c
    side = lax.rem(c + x, 2)
    part_steps = steps // PARTS
    is_low, is_high = slab == 0, slab == slabs - 1

    def at(ty, tx, tz, tc):
        return (2 * ty + tx, 2 * tz + tc)

    def plane_of(h, i):
        return i if h == 0 else thick - 1 - i

    def drain(ref, semaphore):
        pltpu.make_async_copy(ref, ref, semaphore).wait()

    def send(source, target, send_sem, recv_sem, device):
        pltpu.make_async_remote_copy(
            src_ref=source,
            dst_ref=target,
            send_sem=send_sem,
            recv_sem=recv_sem,
            device_id=device,
            device_id_type=MESH,
        ).start()

    take_residual = pltpu.make_async_copy(residual_hbm, res, own.at[0])
    take_residual.start()
    own_slab = pl.ds(s * thick, thick)
    take_capacity = pltpu.make_async_copy(capacity_hbm, caps[0].at[own_slab], own.at[1])
    take_capacity.start()
    near_slab = pl.ds((2 + c) * thick, thick)
    take_near = pltpu.make_async_copy(capacity_hbm, near_cap.at[near_slab], own.at[2])
    take_near.start()

    barrier = pltpu.get_barrier_semaphore()
    below, above = z > 0, z < layers - 1
    sides = jnp.where(below, 1, 0) + jnp.where(above, 1, 0)

    def greet(device):
        pl.semaphore_signal(barrier, inc=1, device_id=device, device_id_type=MESH)

    greet(at(1 - y, x, z, 0))
    greet(at(1 - y, x, z, 1))
    for there, dz in ((below, -1), (above, 1)):

        @pl.when(there)
        def _():
            greet(at(y, x, z + dz, 0))
            greet(at(y, x, z + dz, 1))

    greet(at(y, 1 - x, z, 1 - c))
    greet(at(y, x, z, 1 - c))

    for k in range(shift_table.shape[0]):
        for column in range(3):
            table[k, column] = jnp.float32(shift_table[k, column])
    ones = jnp.ones((thick,) + tile, jnp.float32)

    @pl.when(jnp.logical_not(below))
    def _():
        near_cap[pl.ds(thick, thick)] = ones

    @pl.when(jnp.logical_not(above))
    def _():
        near_cap[pl.ds(4 * thick, thick)] = ones

    @pl.when(is_low)
    def _():
        for j in range(HALO):
            field[j] = jnp.zeros(field.shape[1:], jnp.float32)
        vtwo[0] = jnp.zeros(vtwo.shape[1:], jnp.float32)

    @pl.when(is_high)
    def _():
        for j in range(HALO):
            field[wide - 1 - j] = jnp.zeros(field.shape[1:], jnp.float32)
        vtwo[wide - 1] = jnp.zeros(vtwo.shape[1:], jnp.float32)

    pl.semaphore_wait(barrier, 4 + 2 * sides)

    take_residual.wait()
    for i in range(half):

        @pl.when(keeper)
        def _():
            for h in (0, 1):
                p = plane_of(h, i)

                @pl.when(side == h)
                def _():
                    pltpu.make_async_copy(res.at[:, p], loc.at[i], loc_recv).start()

                @pl.when(side != h)
                def _():
                    send(res.at[:, p], loc.at[i], loc_send, loc_recv, at(y, x, z, 1 - c))

        @pl.when(jnp.logical_not(keeper))
        def _():
            for k in range(PARTS):
                span = pl.ds(k * part_steps, part_steps)
                for h in (0, 1):
                    send(
                        res.at[span, plane_of(h, i)], far.at[i, span], far_send,
                        far_recv.at[i, k], at(1 - y, x, z, lax.rem(h + x, 2)),
                    )

    take_near.wait()
    send(
        near_cap.at[near_slab], near_cap.at[near_slab], n_send.at[0], n_recv.at[2],
        at(y, x, z, 1 - c),
    )
    near_there = jnp.where(c == 0, below, above)

    @pl.when(near_there)
    def _():
        for k in (0, 1):
            send(
                near_cap.at[near_slab],
                near_cap.at[pl.ds((4 - 3 * c) * thick, thick)],
                n_send.at[1],
                n_recv.at[1 - c],
                at(y, x, z + 2 * c - 1, k),
            )

    def tell_sides(turn):
        for there, dz in ((below, -1), (above, 1)):

            @pl.when(there)
            def _():
                pl.semaphore_signal(
                    ready.at[turn], inc=1, device_id=at(y, x, z + dz, c), device_id_type=MESH
                )

    def hear_sides(turn):
        pl.semaphore_wait(ready.at[turn], sides)

    def share_capacity():
        take_capacity.wait()
        for d in range(1, layers):
            send(
                caps[0].at[own_slab],
                caps[0].at[own_slab],
                c_send,
                c_recv.at[d],
                (m, lax.rem(s + 2 * d, slabs)),
            )
        forward_cap(0)

    def rows_from(d):
        return pl.ds(lax.rem(s + slabs - 2 * d, slabs) * thick, thick)

    def forward_cap(d):
        rows = rows_from(d)
        send(
            caps[0].at[rows],
            caps[0].at[rows],
            c_send,
            c_recv.at[0],
            at(y, x, z, 1 - c),
        )

    def power(ty):
        exponent = [rate ** (a * length // 2 + b * steps) for a in (0, 1) for b in (0, 1)]
        low = jnp.where(x == 0, jnp.float32(exponent[0]), jnp.float32(exponent[1]))
        high = jnp.where(x == 0, jnp.float32(exponent[2]), jnp.float32(exponent[3]))
        return jnp.where(ty == 0, low, high)

    here_power, there_power = power(y), power(1 - y)
    sign = jnp.where(y == 0, 1.0, -1.0).astype(jnp.float32)
    first_x = x == 0
    keep_own = jnp.where(first_x, here_power, sign * here_power)
    keep_far = jnp.where(first_x, there_power, -sign * there_power)
    give_own = jnp.where(first_x, sign * here_power, here_power)
    give_far = jnp.where(first_x, -sign * there_power, there_power)

    def combine(i):
        if i == 0:
            drain(loc, loc_recv)
        for k in range(PARTS):
            span = pl.ds(k * part_steps, part_steps)
            drain(far.at[i, span], far_recv.at[i, k])
            for t in range(k * part_steps, (k + 1) * part_steps):
                a, b = loc[i, t] * (rate**t), far[i, t] * (rate**t)
                sendx[i, t] = give_own * a + give_far * b
            send(
                sendx.at[i, span],
                seq.at[i, pl.ds(x * steps + k * part_steps, part_steps)],
                x_send,
                x_recv.at[i, k],
                at(y, 1 - x, z, 1 - c),
            )
            for t in range(k * part_steps, (k + 1) * part_steps):
                a, b = loc[i, t] * (rate**t), far[i, t] * (rate**t)
                seq[i, x * steps + t] = keep_own * a + keep_far * b

    in_layer = side != sig
    halo_y = jnp.where(in_layer, 1 - y, y)
    halo_z = jnp.where(in_layer, z, z + 2 * side - 1)
    halo_there = jnp.logical_or(in_layer, jnp.logical_and(halo_z >= 0, halo_z < layers))

    def transform(i):
        for k in range(PARTS):
            drain(sendx.at[i, pl.ds(0, part_steps)], x_recv.at[i, k])
        plane = jnp.where(side == 0, i, thick - 1 - i) + HALO

        @pl.when(x == 0)
        def _():
            modes = real_transform([seq[i, t] for t in range(2 * steps)])
            field[plane, 0, 0] = modes[0][0]
            field[plane, 0, 1] = modes[steps][0]
            for k in range(1, steps):
                field[plane, k, 0] = modes[k][0]
                field[plane, k, 1] = modes[k][1]

        @pl.when(x == 1)
        def _():
            modes = odd_transform([seq[i, t] for t in range(2 * steps)])
            for k in range(steps):
                field[plane, k, 0] = modes[k][0]
                field[plane, k, 1] = modes[k][1]

        given = field.at[plane, pl.ds((1 - c) * slots, slots)]
        send(given, given, d_send, d_recv, at(y, x, z, 1 - c))
        if i < HALO:
            target = plane + thick * (1 - 2 * side)

            @pl.when(halo_there)
            def _():
                for k in (0, 1):
                    part = pl.ds(k * slots, slots)
                    send(
                        field.at[plane, part],
                        field.at[target, part],
                        h_send,
                        h_recv.at[1 - side],
                        at(halo_y, x, halo_z, k),
                    )

    def shifts_of(slot):
        return tuple(table[slot, column] for column in range(3))

    even_row, even_lane = parity(tile, 0), parity(tile, 1)
    solver_shifts = shifts_of(x * 2 * slots + (1 - c) * slots + slab)

    def pass_capacity():
        for d in range(1, layers):
            drain(caps[0].at[rows_from(d)], c_recv.at[d])
            forward_cap(d)

    def coarse_tables():
        drain(caps[0].at[pl.ds(0, layers * thick)], c_recv.at[0])
        for level in range(1, depth):
            caps[level][...] = block_mean(caps[level - 1][...], 2 ** (level - 1))
            compact_table(level, caps[level], tables[level], solver_shifts, even_row)

    spread0, unused = level_coefficients(0)

    cap_base = (2 + sig) * thick - HALO

    def fine_tables():
        drain(near_cap.at[near_slab], n_recv.at[2])

        @pl.when(below)
        def _():
            drain(near_cap.at[near_slab], n_recv.at[0])

        @pl.when(above)
        def _():
            drain(near_cap.at[near_slab], n_recv.at[1])

        inside = [jnp.float32(1.0)] * wide
        for j in range(HALO):
            inside[j] = jnp.where(is_low, 0.0, 1.0).astype(jnp.float32)
            inside[wide - 1 - j] = jnp.where(is_high, 0.0, 1.0).astype(jnp.float32)

        def body(f, carry):
            s1, s2, s3 = shifts_of(x * 2 * slots + c * slots + f)
            for j in range(wide):
                cap = near_cap[cap_base + j]
                top, coupling = cap * s1 + 6.0 * spread0, cap * s2
                bottom = cap * s3 + 6.0 * spread0
                scale = (OMEGA * inside[j]) / (top * bottom + coupling * coupling)
                inverse0[f, j, 0] = bottom * scale
                inverse0[f, j, 1] = coupling * scale
                inverse0[f, j, 2] = top * scale
            return carry

        lax.fori_loop(0, slots, body, 0)

    for turn in range(layers - 1):
        tell_sides(turn)
        if turn > 0:
            combine(turn - 1)
        hear_sides(turn)
    share_capacity()
    for i in range(layers - 2, half - 1):
        combine(i)
    transform(0)
    combine(half - 1)
    for i in range(1, half):
        transform(i)
        if i == 1:
            fine_tables()
    pass_capacity()

    weights = neighbour_weights(0, tile)

    def slot_at(i):
        total, unit, rest_g, rest_i = 0, 1, slab, i
        while unit < slots:
            bit = lax.rem(lax.rem(rest_g, 2) + lax.rem(rest_i, 2), 2)
            total = total + unit * bit
            rest_g, rest_i = rest_g // 2, rest_i // 2
            unit *= 2
        return total

    def member(g):
        gz, gs = g // 2, lax.rem(g, 2)
        return at(lax.rem(gs + gz, 2), x, gz, 1 - c)

    given_planes = field.at[pl.ds(0, half), pl.ds(0, slots)]
    halo_planes = field.at[pl.ds(0, HALO), pl.ds(0, slots)]
    drain(given_planes, d_recv)
    for end, there in ((0, jnp.logical_not(is_low)), (1, jnp.logical_not(is_high))):

        @pl.when(there)
        def _():
            drain(halo_planes, h_recv.at[end])

    def load_inverse(f):
        return [[inverse0[f, j, k] for k in range(3)] for j in range(wide)]

    def residual_pair(forcing, second, j, shifts):
        s1, s2, s3 = shifts
        ahead, behind = weights[0]
        turned_sums = [0.0, 0.0]
        for k in (j, j + 1):
            re, im = second[k]
            cap = near_cap[cap_base + k]
            top, coupling, bottom = 6.0 * spread0 + cap * s1, cap * s2, 6.0 * spread0 + cap * s3
            turned_sums[0] = turned_sums[0] + (top * re - coupling * im)
            turned_sums[1] = turned_sums[1] + (coupling * re + bottom * im)
        found = []
        for part in (0, 1):
            near = [second[k][part] for k in (j - 1, j, j + 1, j + 2)]
            total = ahead * (near[2] + near[3]) + behind * (near[0] + near[1])
            total = total + around(near[1] + near[2], weights) + turned_sums[part]
            found.append(forcing[j][part] + forcing[j + 1][part] - total)
        return found

    def down(i, carry):
        chosen = [slot_at(slots - 1 - TOGETHER * i - k) for k in range(TOGETHER)]
        forcings = [
            [(field[j, c * slots + f, 0], field[j, c * slots + f, 1]) for j in range(wide)]
            for f in chosen
        ]
        inverses = [load_inverse(f) for f in chosen]
        shifts = [shifts_of(x * 2 * slots + c * slots + f) for f in chosen]
        first = [[] for f in chosen]
        second = [[None] for f in chosen]
        for j in range(wide):
            for n, f in enumerate(chosen):
                (re, im), (a, b, d) = forcings[n][j], inverses[n][j]
                first[n].append((a * re + b * im, d * im - b * re))
                for part in (0, 1):
                    vone[j, f, part] = first[n][j][part]
        for j in range(1, wide - 1):
            for n, f in enumerate(chosen):
                second[n].append(
                    smoothed(first[n][j], first[n][j - 1 : j + 2], inverses[n][j], weights)
                )
                for part in (0, 1):
                    vtwo[j, f, part] = second[n][j][part]
        for pair in range(thick // 4):
            packed = [[None, None] for f in chosen]
            for plane in (0, 1):
                for n, f in enumerate(chosen):
                    j = HALO + 4 * pair + 2 * plane
                    packed[n][plane] = residual_pair(forcings[n], second[n], j, shifts[n])
            for n, f in enumerate(chosen):
                coarse_out[f, pair] = 0.125 * pack_means(*packed[n], even_row, even_lane)

        tiles = pl.ds(slab * (thick // 4), thick // 4)
        for f in chosen:
            send(coarse_out.at[f], gathered.at[tiles], g_send, g_recv, member(f))

        return carry

    lax.fori_loop(0, slots // TOGETHER, down, 0)

    low_y, low_z = jnp.where(sig == 0, y, 1 - y), jnp.where(sig == 0, z - 1, z)
    high_y, high_z = jnp.where(sig == 0, 1 - y, y), jnp.where(sig == 0, z, z + 1)

    @pl.when(jnp.logical_not(is_low))
    def _():
        send(
            vtwo.at[HALO + 1], vtwo.at[wide - 1], e_send.at[0], e_recv.at[1], at(low_y, x, low_z, c)
        )

    @pl.when(jnp.logical_not(is_high))
    def _():
        send(
            vtwo.at[wide - HALO - 2], vtwo.at[0], e_send.at[1], e_recv.at[0],
            at(high_y, x, high_z, c),
        )

    coarse_tables()
    drain(gathered, g_recv)
    tiles_in = slabs * thick // 4
    unpacked = []
    for j in range(tiles_in):
        cells = gathered[j]
        re = jnp.where(even_lane, cells, shifted(cells, 1, 1))
        im = jnp.where(even_lane, shifted(cells, -1, 1), cells)
        unpacked.append((re, im))
    coarse = compact_cycle(1, unpacked, tables, solver_shifts, even_row)
    packed_cells = [jnp.where(even_lane, re, im) for re, im in coarse]
    empty = jnp.zeros(tile, jnp.float32)
    for j in range(tiles_in + 1):
        back[j] = jnp.where(
            even_row,
            packed_cells[j] if j < tiles_in else empty,
            packed_cells[j - 1] if j > 0 else empty,
        )
    span = thick // 4 + 1

    def give(i, carry):
        g = slot_at(slots - 1 - i)
        send(
            back.at[pl.ds(g * (thick // 4), span)], edges.at[slab], b_send, b_recv.at[slab],
            member(g),
        )
        return carry

    lax.fori_loop(0, slots, give, 0)

    for end, there in ((0, jnp.logical_not(is_low)), (1, jnp.logical_not(is_high))):

        @pl.when(there)
        def _():
            drain(vtwo.at[0], e_recv.at[end])
            drain(vtwo.at[0], e_send.at[end])

    def up(i, carry):
        chosen = [slot_at(TOGETHER * i + k) for k in range(TOGETHER)]
        for f in chosen:
            drain(edges.at[0], b_recv.at[f])

        inverses = [load_inverse(f) for f in chosen]
        start = [[] for f in chosen]
        third = [[None] for f in chosen]
        for k in range(span):
            for n, f in enumerate(chosen):
                for u, extra in enumerate(unpack_cells(edges[f, k], even_row, even_lane)[::-1]):
                    for j in (4 * k + 2 * u, 4 * k + 2 * u + 1):
                        start[n].append([vtwo[j, f, part] + extra[part] for part in (0, 1)])
        for j in range(1, wide - 1):
            for n, f in enumerate(chosen):
                first = (vone[j, f, 0], vone[j, f, 1])
                third[n].append(smoothed(first, start[n][j - 1 : j + 2], inverses[n][j], weights))
        for j in range(HALO, wide - HALO):
            for n, f in enumerate(chosen):
                first = (vone[j, f, 0], vone[j, f, 1])
                parts = smoothed(first, third[n][j - 1 : j + 2], inverses[n][j], weights)
                for part in (0, 1):
                    result[f, j - HALO, part] = parts[part]
        for f in chosen:
            q = c * slots + f
            send(
                result.at[f, pl.ds((1 - side) * half, half)], merged.at[q], r_send, r_recv,
                at(y, x, z, 1 - c),
            )
            for k in range(half):
                merged[q, k] = result[f, side * half + k]
        return carry

    lax.fori_loop(0, slots // TOGETHER, up, 0)
    drain(merged.at[pl.ds(0, slots)], r_recv)

    def invert(i):
        @pl.when(x == 0)
        def _():
            modes = [(merged[0, i, 0], None)]
            modes += [(merged[k, i, 0], merged[k, i, 1]) for k in range(1, steps)]
            modes += [(merged[0, i, 1], None)]
            for t, value in enumerate(real_inverse(modes)):
                wave[i, t] = value

        @pl.when(x == 1)
        def _():
            modes = [(merged[k, i, 0], merged[k, i, 1]) for k in range(steps)]
            for t, value in enumerate(odd_inverse(modes)):
                wave[i, t] = value

        for k in range(PARTS):
            send(
                wave.at[i, pl.ds((1 - x) * steps + k * part_steps, part_steps)],
                gotb.at[i, pl.ds(k * part_steps, part_steps)], w_send, w_recv.at[i, k],
                at(y, 1 - x, z, 1 - c),
            )

    inverse_here = 1.0 / (here_power * length)
    inverse_there = 1.0 / (there_power * length)
    own_sign = jnp.where(first_x, 1.0, sign).astype(jnp.float32)
    got_sign = jnp.where(first_x, sign, 1.0).astype(jnp.float32)
    far_own = jnp.where(first_x, 1.0, -sign).astype(jnp.float32)
    far_got = jnp.where(first_x, -sign, 1.0).astype(jnp.float32)

    def finish(i, k):
        span = pl.ds(k * part_steps, part_steps)
        drain(gotb.at[i, span], w_recv.at[i, k])
        p = side * half + i
        for t in range(k * part_steps, (k + 1) * part_steps):
            mine = wave[i, x * steps + t] * (rate**-t)
            got = gotb[i, t] * (rate**-t)
            outgoing[1, i, t] = (far_own * inverse_there) * mine + (far_got * inverse_there) * got
        send(
            outgoing.at[1, i, span], out_ref.at[span, p], o_send.at[1], o_recv,
            at(1 - y, x, z, sig),
        )

        def own_value(t):
            mine = wave[i, x * steps + t] * (rate**-t)
            got = gotb[i, t] * (rate**-t)
            return (own_sign * inverse_here) * mine + (got_sign * inverse_here) * got

        @pl.when(keeper)
        def _():
            for t in range(k * part_steps, (k + 1) * part_steps):
                out_ref[t, p] = own_value(t)

        @pl.when(jnp.logical_not(keeper))
        def _():
            for t in range(k * part_steps, (k + 1) * part_steps):
                outgoing[0, i, t] = own_value(t)
            send(
                outgoing.at[0, i, span], out_ref.at[span, p], o_send.at[0], o_recv,
                at(y, x, z, 1 - c),
            )

    for i in range(half):
        invert(i)
    for i in range(half):
        for k in range(PARTS):
            finish(i, k)

    @pl.when(keeper)
    def _():
        drain(loc, o_recv)
        drain(loc, loc_send)

    @pl.when(jnp.logical_not(keeper))
    def _():
        drain(res, o_recv)
        drain(res, far_send)
        drain(loc, o_send.at[0])

    drain(loc, o_send.at[1])
    drain(loc, x_send)
    drain(loc, w_send)
    drain(given_planes, d_send)

    @pl.when(halo_there)
    def _():
        drain(field.at[pl.ds(0, 2 * HALO), pl.ds(0, slots)], h_send)

    drain(gathered, g_send)
    drain(edges, b_send)
    drain(merged.at[pl.ds(0, slots)], r_send)
    drain(near_cap.at[near_slab], n_send.at[0])

    @pl.when(near_there)
    def _():
        drain(near_cap.at[pl.ds(0, 2 * thick)], n_send.at[1])

    drain(caps[0].at[pl.ds(0, (2 * layers - 1) * thick)], c_send)


def level_extents(extent):
    return [extent // 2**level for level in range(GRID_DEPTH)]


def fused(groups, slabs, residual, capacity):
    steps, thick, second, third = residual.shape
    length = groups * steps
    half, slots = thick // 2, steps // 2
    extent, wide = slabs * thick, thick + 2 * HALO
    tile = (second, third)
    ratio_step = ALPHA_CORNER ** (1.0 / length)
    numbers = [2 * k for k in range(steps)] + [4 * k + 1 for k in range(steps)]
    angle = 2.0 * np.pi / length * np.array(numbers)
    table = np.stack(
        [
            (1.0 - ratio_step * np.cos(angle)) / STEP_SIZE,
            ratio_step * np.sin(angle) / STEP_SIZE,
            (1.0 - ratio_step * np.cos(angle)) / STEP_SIZE,
        ],
        axis=1,
    )
    table[0, 1], table[0, 2] = 0.0, (1.0 + ratio_step) / STEP_SIZE
    extents = level_extents(extent)
    vmem = lambda *shape: pltpu.VMEM(shape + tile, jnp.float32)
    sems = lambda *shape: pltpu.SemaphoreType.DMA(shape)
    one = pltpu.SemaphoreType.DMA
    layers, quarter = slabs // 2, thick // 4
    scratch = [
        vmem(steps, thick),
        vmem(half, steps),
        vmem(half, steps),
        vmem(half, 2 * steps),
        vmem(half, steps),
        vmem(wide, 2 * slots, 2),
        vmem(slots, wide, 3),
        vmem(wide, slots, 2),
        vmem(wide, slots, 2),
        vmem(slots, quarter),
        vmem(slabs * quarter),
        vmem(slabs * quarter + 1),
        vmem(slots, quarter + 1),
        vmem(slots, thick, 2),
        vmem(2 * slots, half, 2),
        vmem(half, 2 * steps),
        vmem(half, steps),
        vmem(2, half, steps),
        pltpu.SMEM(table.shape, jnp.float32),
        vmem(6 * thick),
        *[vmem(n) for n in extents],
        *[vmem(n // 2, 4) for n in extents[1:]],
        sems(3),
        one,
        sems(half, PARTS),
        one,
        one,
        one,
        sems(half, PARTS),
        one,
        one,
        one,
        sems(2),
        sems(2),
        sems(2),
        one,
        one,
        one,
        sems(slots),
        one,
        one,
        one,
        sems(half, PARTS),
        sems(2),
        one,
        one,
        sems(layers),
        sems(2),
        sems(3),
        pltpu.SemaphoreType.REGULAR((layers - 1,)),
    ]
    return pl.pallas_call(
        functools.partial(whole_kernel, groups, slabs, table),
        out_shape=jax.ShapeDtypeStruct(residual.shape, jnp.float32),
        in_specs=[
            pl.BlockSpec(memory_space=pltpu.HBM),
            pl.BlockSpec(memory_space=pltpu.HBM),
        ],
        out_specs=pl.BlockSpec(memory_space=pltpu.VMEM),
        scratch_shapes=scratch,
        compiler_params=pltpu.CompilerParams(
            collective_id=0, has_side_effects=True, vmem_limit_bytes=32 * 2**20
        ),
    )(*[pltpu.with_memory_space_constraint(a, pltpu.HBM) for a in (residual, capacity)])


def fits_fused(groups, slabs, residual):
    steps, thick, second, third = residual.shape
    length = groups * steps
    power = length & (length - 1) == 0
    return (
        power
        and groups == 4
        and slabs % 2 == 0
        and slabs == length // 8
        and thick == 8
        and all(n % 2 == 0 and n % n == 0 for n in level_extents(slabs * thick))
        and (second, third) == (8, 128)
    )


def either(residual, capacity):
    groups, slabs = lax.axis_size("tm"), lax.axis_size("space")
    if fits_fused(groups, slabs, residual):
        return fused(groups, slabs, residual, capacity)
    return on_device(residual, capacity)


def solution(mesh):
    return jax.shard_map(
        either,
        mesh=mesh,
        in_specs=(P("tm", "space", None, None), P("space", None, None)),
        out_specs=P("tm", "space", None, None),
        check_vma=False,
    )
```

```python
import functools
import math

import jax
import jax.numpy as jnp
import numpy as np
from jax import lax
from jax.experimental import pallas as pl
from jax.experimental.pallas import tpu as pltpu
from jax.sharding import PartitionSpec as P

GRID_DEPTH = 4
SMOOTH = 2
COARSE_SWEEPS = 6


ALPHA_CORNER = 0.01
STEP_SIZE = 0.5
DIFFUSE = 2.0
ADVECT = (0.2, -0.15, 0.1)
OMEGA = 0.7
HIGHEST = lax.Precision.HIGHEST


def extended(array, sides, width):
    for axis, dim in sides:
        peers, length = (lax.axis_size(axis), array.shape[dim])
        up = [(i, (i + 1) % peers) for i in range(peers - 1)]
        down = [(j, i) for i, j in up]
        last = lax.slice_in_dim(array, length - width, length, axis=dim)
        initial = lax.slice_in_dim(array, 0, width, axis=dim)
        before = lax.ppermute(last, axis, up)
        after = lax.ppermute(initial, axis, down)
        array = jnp.concatenate([before, array, after], axis=dim)
    return array


def level_coefficients(per_level_values):
    spread = DIFFUSE / 4.0**per_level_values
    drifts = tuple((component / 2.0**per_level_values for component in ADVECT))
    return (spread, drifts)


def pad_second(volume, position):
    widths = [(0, 0)] * volume.ndim
    widths[position] = (1, 1)
    return jnp.pad(volume, widths)


def apply_operator(padded, current_capacity, spectral_shifts, per_level_values):
    spread, drifts = level_coefficients(per_level_values)
    centre = padded[:, :, 1:-1]
    upper_first = padded[:, :, 2:]
    lower_first = padded[:, :, :-2]
    wide_second = pad_second(centre, 3)
    upper_second = wide_second[:, :, :, 2:]
    lower_second = wide_second[:, :, :, :-2]
    wide_third = pad_second(centre, 4)
    upper_third = wide_third[:, :, :, :, 2:]
    lower_third = wide_third[:, :, :, :, :-2]
    stencil = spread * (
        6.0 * centre
        - upper_first
        - lower_first
        - upper_second
        - lower_second
        - upper_third
        - lower_third
    )
    stencil = (
        stencil
        + drifts[0] * (upper_first - lower_first)
        + drifts[1] * (upper_second - lower_second)
        + drifts[2] * (upper_third - lower_third)
    )
    first_shift, second_shift, third_shift = spectral_shifts
    real_part = centre[0]
    imag_part = centre[1]
    shifted = jnp.stack(
        [
            current_capacity * (first_shift * real_part - second_shift * imag_part),
            current_capacity * (second_shift * real_part + third_shift * imag_part),
        ]
    )
    return stencil + shifted


def inverse_diagonal(current_capacity, spectral_shifts, per_level_values):
    spread, drifts = level_coefficients(per_level_values)
    first_shift, second_shift, third_shift = spectral_shifts
    top_left = current_capacity * first_shift + 6.0 * spread
    coupling = current_capacity * second_shift
    bottom_right = current_capacity * third_shift + 6.0 * spread
    determinant = top_left * bottom_right + coupling * coupling
    return (bottom_right / determinant, coupling / determinant, top_left / determinant)


def damped_update(residual_now, inverse):
    diagonal_a, diagonal_b, diagonal_c = inverse
    return OMEGA * jnp.stack(
        [
            diagonal_a * residual_now[0] + diagonal_b * residual_now[1],
            diagonal_c * residual_now[1] - diagonal_b * residual_now[0],
        ]
    )


def restrict_to_coarse(volume):
    leading = volume.shape[:-3]
    first_extent, second_extent, third_extent = volume.shape[-3:]
    blocks = volume.reshape(
        leading + (first_extent // 2, 2, second_extent // 2, 2, third_extent // 2, 2)
    )
    lead_count = len(leading)
    return jnp.mean(blocks, axis=(lead_count + 1, lead_count + 3, lead_count + 5))


def prolong_cells(volume):
    leading = volume.shape[:-3]
    first_extent, second_extent, third_extent = volume.shape[-3:]
    expanded = jnp.broadcast_to(
        volume[..., :, None, :, None, :, None],
        leading + (first_extent, 2, second_extent, 2, third_extent, 2),
    )
    return expanded.reshape(leading + (2 * first_extent, 2 * second_extent, 2 * third_extent))


def shift_values(frequency, length):
    ratio_step = ALPHA_CORNER ** (1.0 / length)
    phases = 2.0 * math.pi / length * frequency.astype(jnp.float32)
    first_shift = (1.0 - ratio_step * jnp.cos(phases)) / STEP_SIZE
    second_shift = ratio_step * jnp.sin(phases) / STEP_SIZE
    leading = frequency == 0
    second_shift = jnp.where(leading, 0.0, second_shift)
    third_shift = jnp.where(leading, (1.0 + ratio_step) / STEP_SIZE, first_shift)
    return tuple(
        (column.reshape(-1, 1, 1, 1) for column in (first_shift, second_shift, third_shift))
    )


def phase_grid(row_count, length):
    integers = (
        jnp.arange(row_count, dtype=jnp.int32)[:, None]
        * jnp.arange(length, dtype=jnp.int32)[None, :]
        % length
    )
    return 2.0 * math.pi / length * integers.astype(jnp.float32)


def pad_faces(volume):
    return extended(volume, (("space", 2),), 1)


def multigrid_cycle(
    per_level_values,
    forcing_term,
    capacity_fields,
    spectral_shifts,
    shared_values,
    assemble_level,
    assemble_parts,
):
    current_capacity = capacity_fields[per_level_values]
    inverse = inverse_diagonal(current_capacity, spectral_shifts, per_level_values)
    coarsest = per_level_values == GRID_DEPTH - 1
    current = damped_update(forcing_term, inverse)
    for repeat in range((COARSE_SWEEPS if coarsest else SMOOTH) - 1):
        current = current + damped_update(
            forcing_term
            - apply_operator(
                pad_faces(current), current_capacity, spectral_shifts, per_level_values
            ),
            inverse,
        )
    if coarsest:
        return current
    coarse_right_hand = restrict_to_coarse(
        forcing_term
        - apply_operator(pad_faces(current), current_capacity, spectral_shifts, per_level_values)
    )
    coarse_solution = multigrid_cycle(
        per_level_values + 1,
        coarse_right_hand,
        capacity_fields,
        spectral_shifts,
        shared_values,
        assemble_level,
        assemble_parts,
    )
    current = current + prolong_cells(coarse_solution)
    for repeat in range(SMOOTH):
        current = current + damped_update(
            forcing_term
            - apply_operator(
                pad_faces(current), current_capacity, spectral_shifts, per_level_values
            ),
            inverse,
        )
    return current


def on_device(residual, capacity):
    steps_here, thickness, extent_second, extent_third = residual.shape
    length = lax.axis_size("tm") * steps_here
    ratio_step = ALPHA_CORNER ** (1.0 / length)
    moments = (lax.axis_index("tm") * steps_here + jnp.arange(steps_here, dtype=jnp.int32)).astype(
        jnp.float32
    )
    scaled = (residual * jnp.power(ratio_step, moments)[:, None, None, None]).reshape(
        steps_here, -1
    )
    series = lax.all_to_all(scaled, "tm", split_axis=1, concat_axis=0, tiled=True)
    all_weights = jnp.power(ratio_step, jnp.arange(length, dtype=jnp.float32))
    alternate = 1.0 - 2.0 * (jnp.arange(length, dtype=jnp.int32) % 2).astype(jnp.float32)
    capacity_fields = [capacity]
    for per_level_values in range(1, GRID_DEPTH):
        capacity_fields.append(restrict_to_coarse(capacity_fields[-1]))
    halves = length // 2
    phases = phase_grid(halves, length)
    first_row = jnp.arange(halves, dtype=jnp.int32)[:, None] == 0
    forward = jnp.concatenate(
        [jnp.cos(phases), jnp.where(first_row, alternate[None, :], -jnp.sin(phases))], axis=0
    )
    spectrum = jnp.dot(forward, series, precision=HIGHEST).reshape(2, halves, -1)
    received = lax.all_to_all(spectrum, "tm", split_axis=1, concat_axis=2, tiled=True)
    slot_count = steps_here // 2
    frequency = lax.axis_index("tm") * slot_count + jnp.arange(slot_count, dtype=jnp.int32)
    spectral_shifts = shift_values(frequency, length)
    field_list = received.reshape(2, slot_count, thickness, extent_second, extent_third)
    solved_fields = multigrid_cycle(
        0, field_list, capacity_fields, spectral_shifts, False, GRID_DEPTH, None
    )
    flattened = solved_fields.reshape(2, slot_count, -1)
    returned = lax.all_to_all(flattened, "tm", split_axis=2, concat_axis=1, tiled=True)
    halves = length // 2
    phases = jnp.transpose(phase_grid(halves, length))
    first_column = jnp.arange(halves, dtype=jnp.int32)[None, :] == 0
    real_columns = jnp.where(first_column, 1.0, 2.0 * jnp.cos(phases)) / length
    imag_columns = jnp.where(first_column, alternate[:, None], -2.0 * jnp.sin(phases)) / length
    inverse_table = jnp.concatenate([real_columns, imag_columns], axis=1)
    values = jnp.dot(
        inverse_table,
        returned.reshape(returned.shape[0] * returned.shape[1], -1),
        precision=HIGHEST,
    )
    values = values / all_weights[:, None]
    result = lax.all_to_all(values, "tm", split_axis=0, concat_axis=1, tiled=True)
    return result.reshape(residual.shape)


MESH = pl.DeviceIdType.MESH


def real_transform(values):
    count = len(values)
    if count == 1:
        return [(values[0], None)]
    evens, odds = real_transform(values[0::2]), real_transform(values[1::2])
    half = count // 2
    if count == 2:
        return [(evens[0][0] + odds[0][0], None), (evens[0][0] - odds[0][0], None)]
    found = [None] * (half + 1)
    found[0] = (evens[0][0] + odds[0][0], None)
    found[half] = (evens[0][0] - odds[0][0], None)
    found[half // 2] = (evens[half // 2][0], -odds[half // 2][0])
    for k in range(1, half // 2):
        cosine, sine = math.cos(2 * math.pi * k / count), -math.sin(2 * math.pi * k / count)
        (er, ei), (or_, oi) = evens[k], odds[k]
        tr, ti = cosine * or_ - sine * oi, cosine * oi + sine * or_
        found[k] = (er + tr, ei + ti)
        found[half - k] = (er - tr, ti - ei)
    return found


def real_inverse(modes):
    half = len(modes) - 1
    if half == 0:
        return [modes[0][0]]
    count = 2 * half
    if half == 1:
        return [modes[0][0] + modes[1][0], modes[0][0] - modes[1][0]]
    evens, odds = [None] * (half // 2 + 1), [None] * (half // 2 + 1)
    evens[0] = (modes[0][0] + modes[half][0], None)
    odds[0] = (modes[0][0] - modes[half][0], None)
    middle = modes[half // 2]
    evens[half // 2] = (2.0 * middle[0], None)
    odds[half // 2] = (-2.0 * middle[1], None)
    for k in range(1, half // 2):
        cosine, sine = math.cos(2 * math.pi * k / count), math.sin(2 * math.pi * k / count)
        (ar, ai), (br, bi) = modes[k], modes[half - k]
        dr, di = ar - br, ai + bi
        evens[k] = (ar + br, ai - bi)
        odds[k] = (cosine * dr - sine * di, cosine * di + sine * dr)
    first, second = real_inverse(evens), real_inverse(odds)
    return [part for pair in zip(first, second) for part in pair]


def pair_sum(value, distance):
    for axis in (-2, -1):
        dim = value.ndim + axis
        extent = value.shape[dim]
        upper = pltpu.roll(value, extent - distance, dim)
        lower = pltpu.roll(value, distance, dim)
        place = lax.broadcasted_iota(jnp.int32, value.shape, dim)
        value = value + jnp.where((place // distance) % 2 == 0, upper, lower)
    return value


def block_mean(value, distance):
    shape = (value.shape[0] // 2, 2) + value.shape[1:]
    paired = value.reshape(shape)
    return 0.125 * pair_sum(paired[:, 0] + paired[:, 1], distance)


def neighbour_weights(level, shape):
    spread, drifts = level_coefficients(level)
    distance = 2**level
    along_first = (drifts[0] - spread, -drifts[0] - spread)
    masked = []
    for dim in (0, 1):
        place = lax.broadcasted_iota(jnp.int32, shape, dim)
        upper = jnp.where(place < shape[dim] - distance, drifts[dim + 1] - spread, 0.0)
        lower = jnp.where(place >= distance, -drifts[dim + 1] - spread, 0.0)
        masked.append((upper, lower))
    return along_first, masked, distance


def complex_transform(values, sign):
    count = len(values)
    if count == 1:
        return values
    evens, odds = complex_transform(values[0::2], sign), complex_transform(values[1::2], sign)
    first, second = [], []
    for k in range(count // 2):
        (er, ei), (or_, oi) = evens[k], odds[k]
        tr, ti = turned(or_, oi, k, count, sign)
        first.append((er + tr, ei + ti))
        second.append((er - tr, ei - ti))
    return first + second


def turned(re, im, k, count, sign):
    if k == 0:
        return re, im
    if 4 * k == count:
        return (-im, re) if sign > 0 else (im, -re)
    cosine, sine = math.cos(2 * math.pi * k / count), sign * math.sin(2 * math.pi * k / count)
    return cosine * re - sine * im, cosine * im + sine * re


def odd_transform(values):
    half = len(values) // 2
    folded = [turned(values[s], -values[s + half], s, 4 * half, -1) for s in range(half)]
    return complex_transform(folded, -1)


def odd_inverse(modes):
    half = len(modes)
    folded = complex_transform(modes, 1)
    first, second = [], []
    for s, (re, im) in enumerate(folded):
        re, im = turned(re, im, s, 4 * half, 1)
        first.append(2.0 * re)
        second.append(-2.0 * im)
    return first + second


def parity(shape, dim):
    return lax.broadcasted_iota(jnp.int32, shape, dim) % 2 == 0


def shifted(value, step, dim):
    return pltpu.roll(value, step % value.shape[dim], dim)


def pack_means(first, second, even_row, even_lane):
    rows = []
    for a, b in zip(first, second):
        left = jnp.where(even_row, a, shifted(b, 1, 0))
        right = jnp.where(even_row, shifted(a, -1, 0), b)
        rows.append(left + right)
    re, im = rows
    left = jnp.where(even_lane, re, shifted(im, 1, 1))
    right = jnp.where(even_lane, shifted(re, -1, 1), im)
    return left + right


def unpack_cells(tile, even_row, even_lane):
    found = []
    for rows in (
        jnp.where(even_row, tile, shifted(tile, 1, 0)),
        jnp.where(even_row, shifted(tile, -1, 0), tile),
    ):
        re = jnp.where(even_lane, rows, shifted(rows, 1, 1))
        im = jnp.where(even_lane, shifted(rows, -1, 1), rows)
        found.append((re, im))
    return found


def around(value, weights):
    unused, masked, distance = weights
    total = 0.0
    for dim in (0, 1):
        upper, lower = masked[dim]
        total = total + upper * shifted(value, -distance, dim)
        total = total + lower * shifted(value, distance, dim)
    return total


def smoothed(first, columns, inverse, weights):
    ahead, behind = weights[0]
    below, here, above = columns
    n0, n1 = (
        ahead * above[k] + behind * below[k] + around(here[k], weights) for k in (0, 1)
    )
    a, b, c = inverse
    return (
        first[0] + (1.0 - OMEGA) * here[0] - (a * n0 + b * n1),
        first[1] + (1.0 - OMEGA) * here[1] - (c * n1 - b * n0),
    )


def compact_rest(forcing, values, weights, even_row):
    along_first, masked, distance = weights
    found = [[None, None] for here in forcing]
    for part in (0, 1):
        column = [value[part] for value in values]
        ups = [shifted(v, -1, 0) for v in column]
        downs = [shifted(v, 1, 0) for v in column]
        for j, value in enumerate(column):
            zero = jnp.zeros_like(value)
            after = downs[j + 1] if j + 1 < len(column) else zero
            before = ups[j - 1] if j > 0 else zero
            total = along_first[0] * jnp.where(even_row, ups[j], after)
            total = total + along_first[1] * jnp.where(even_row, before, downs[j])
            for dim in (0, 1):
                if distance < value.shape[dim]:
                    upper, lower = masked[dim]
                    total = total + upper * shifted(value, -distance, dim)
                    total = total + lower * shifted(value, distance, dim)
            found[j][part] = forcing[j][part] - total
    return found


def compact_sweep(forcing, values, table, weights, even_row):
    found = []
    for j, (r0, r1) in enumerate(compact_rest(forcing, values, weights, even_row)):
        a, b, c = (table[j, k] for k in range(3))
        re, im = values[j]
        found.append(
            (
                (1.0 - OMEGA) * re + (a * r0 + b * r1),
                (1.0 - OMEGA) * im + (c * r1 - b * r0),
            )
        )
    return found


def compact_restrict(values, distance, even_row):
    found = []
    for pair in zip(values[0::2], values[1::2]):
        parts = []
        for first, second in zip(*pair):
            left = jnp.where(even_row, first, shifted(second, 1, 0))
            total = left + jnp.where(even_row, shifted(first, -1, 0), second)
            for dim in (0, 1):
                place = lax.broadcasted_iota(jnp.int32, total.shape, dim)
                upper, lower = shifted(total, -distance, dim), shifted(total, distance, dim)
                total = total + jnp.where((place // distance) % 2 == 0, upper, lower)
            parts.append(0.125 * total)
        found.append(parts)
    return found


def compact_cycle(level, forcing, tables, shifts, even_row):
    table = tables[level]
    spread, unused = level_coefficients(level)
    s1, s2, s3 = shifts
    weights = neighbour_weights(level, forcing[0][0].shape)
    values = []
    for j, (re, im) in enumerate(forcing):
        a, b, c = (table[j, k] for k in range(3))
        values.append((a * re + b * im, c * im - b * re))
    coarsest = level == GRID_DEPTH - 1
    for repeat in range((COARSE_SWEEPS if coarsest else SMOOTH) - 1):
        values = compact_sweep(forcing, values, table, weights, even_row)
    if coarsest:
        return values
    rest = compact_rest(forcing, values, weights, even_row)
    for j, (re, im) in enumerate(values):
        cap = table[j, 3]
        rest[j][0] = rest[j][0] - (6.0 * spread * re + cap * (s1 * re - s2 * im))
        rest[j][1] = rest[j][1] - (6.0 * spread * im + cap * (s2 * re + s3 * im))
    coarse = compact_cycle(
        level + 1, compact_restrict(rest, 2**level, even_row), tables, shifts, even_row
    )
    for j, value in enumerate(coarse):
        values[2 * j] = tuple(
            old + jnp.where(even_row, v, shifted(v, 1, 0)) for old, v in zip(values[2 * j], value)
        )
        values[2 * j + 1] = tuple(
            old + jnp.where(even_row, shifted(v, -1, 0), v)
            for old, v in zip(values[2 * j + 1], value)
        )
    for repeat in range(SMOOTH):
        values = compact_sweep(forcing, values, table, weights, even_row)
    return values


def compact_table(level, caps, table, shifts, even_row):
    spread, unused = level_coefficients(level)
    s1, s2, s3 = shifts
    for j in range(table.shape[0]):
        cap = jnp.where(even_row, caps[2 * j], caps[2 * j + 1])
        top, coupling, bottom = cap * s1 + 6.0 * spread, cap * s2, cap * s3 + 6.0 * spread
        scale = OMEGA / (top * bottom + coupling * coupling)
        table[j, 0] = bottom * scale
        table[j, 1] = coupling * scale
        table[j, 2] = top * scale
        table[j, 3] = cap


HALO = 2
TOGETHER = 2
PARTS = 2


def whole_kernel(groups, slabs, shift_table, residual_hbm, capacity_hbm, out_ref, *scratch):
    (
        res, loc, far, seq, sendx, field, inverse0, vone, vtwo, coarse_out, gathered, back, edges,
        result, merged, wave, gotb, outgoing, table, near_cap,
    ) = scratch[:20]
    depth = GRID_DEPTH
    rest = scratch[20:]
    caps, rest = rest[:depth], rest[depth:]
    tables, rest = (None,) + rest[: depth - 1], rest[depth - 1 :]
    (
        own, far_send, far_recv, loc_send, loc_recv, x_send, x_recv, d_send, d_recv, h_send, h_recv,
        e_send, e_recv, g_send, g_recv, b_send, b_recv, r_send, r_recv, w_send, w_recv, o_send,
        o_recv, c_send, c_recv, n_send, n_recv, ready,
    ) = rest
    steps, thick = res.shape[:2]
    half = thick // 2
    slots = field.shape[1] // 2
    wide = thick + 2 * HALO
    length = groups * steps
    rate = ALPHA_CORNER ** (1.0 / length)
    tile = res.shape[-2:]
    m, s = lax.axis_index("tm"), lax.axis_index("space")
    y, x = m // 2, lax.rem(m, 2)
    z, c = s // 2, lax.rem(s, 2)
    layers = slabs // 2
    sig = lax.rem(y + z, 2)
    slab = 2 * z + sig
    keeper = sig == c
    side = lax.rem(c + x, 2)
    part_steps = steps // PARTS
    is_low, is_high = slab == 0, slab == slabs - 1

    def at(ty, tx, tz, tc):
        return (2 * ty + tx, 2 * tz + tc)

    def plane_of(h, i):
        return i if h == 0 else thick - 1 - i

    def drain(ref, semaphore):
        pltpu.make_async_copy(ref, ref, semaphore).wait()

    def send(source, target, send_sem, recv_sem, device):
        pltpu.make_async_remote_copy(
            src_ref=source,
            dst_ref=target,
            send_sem=send_sem,
            recv_sem=recv_sem,
            device_id=device,
            device_id_type=MESH,
        ).start()

    take_residual = pltpu.make_async_copy(residual_hbm, res, own.at[0])
    take_residual.start()
    own_slab = pl.ds(s * thick, thick)
    take_capacity = pltpu.make_async_copy(capacity_hbm, caps[0].at[own_slab], own.at[1])
    take_capacity.start()
    near_slab = pl.ds((2 + c) * thick, thick)
    take_near = pltpu.make_async_copy(capacity_hbm, near_cap.at[near_slab], own.at[2])
    take_near.start()

    barrier = pltpu.get_barrier_semaphore()
    below, above = z > 0, z < layers - 1
    sides = jnp.where(below, 1, 0) + jnp.where(above, 1, 0)

    def greet(device):
        pl.semaphore_signal(barrier, inc=1, device_id=device, device_id_type=MESH)

    greet(at(1 - y, x, z, 0))
    greet(at(1 - y, x, z, 1))
    for there, dz in ((below, -1), (above, 1)):

        @pl.when(there)
        def _():
            greet(at(y, x, z + dz, 0))
            greet(at(y, x, z + dz, 1))

    greet(at(y, 1 - x, z, 1 - c))
    greet(at(y, x, z, 1 - c))

    for k in range(shift_table.shape[0]):
        for column in range(3):
            table[k, column] = jnp.float32(shift_table[k, column])
    ones = jnp.ones((thick,) + tile, jnp.float32)

    @pl.when(jnp.logical_not(below))
    def _():
        near_cap[pl.ds(thick, thick)] = ones

    @pl.when(jnp.logical_not(above))
    def _():
        near_cap[pl.ds(4 * thick, thick)] = ones

    @pl.when(is_low)
    def _():
        for j in range(HALO):
            field[j] = jnp.zeros(field.shape[1:], jnp.float32)
        vtwo[0] = jnp.zeros(vtwo.shape[1:], jnp.float32)

    @pl.when(is_high)
    def _():
        for j in range(HALO):
            field[wide - 1 - j] = jnp.zeros(field.shape[1:], jnp.float32)
        vtwo[wide - 1] = jnp.zeros(vtwo.shape[1:], jnp.float32)

    pl.semaphore_wait(barrier, 4 + 2 * sides)

    take_residual.wait()
    for i in range(half):

        @pl.when(keeper)
        def _():
            for h in (0, 1):
                p = plane_of(h, i)

                @pl.when(side == h)
                def _():
                    pltpu.make_async_copy(res.at[:, p], loc.at[i], loc_recv).start()

                @pl.when(side != h)
                def _():
                    send(res.at[:, p], loc.at[i], loc_send, loc_recv, at(y, x, z, 1 - c))

        @pl.when(jnp.logical_not(keeper))
        def _():
            for k in range(PARTS):
                span = pl.ds(k * part_steps, part_steps)
                for h in (0, 1):
                    send(
                        res.at[span, plane_of(h, i)], far.at[i, span], far_send,
                        far_recv.at[i, k], at(1 - y, x, z, lax.rem(h + x, 2)),
                    )

    take_near.wait()
    send(
        near_cap.at[near_slab], near_cap.at[near_slab], n_send.at[0], n_recv.at[2],
        at(y, x, z, 1 - c),
    )
    near_there = jnp.where(c == 0, below, above)

    @pl.when(near_there)
    def _():
        for k in (0, 1):
            send(
                near_cap.at[near_slab],
                near_cap.at[pl.ds((4 - 3 * c) * thick, thick)],
                n_send.at[1],
                n_recv.at[1 - c],
                at(y, x, z + 2 * c - 1, k),
            )

    def tell_sides(turn):
        for there, dz in ((below, -1), (above, 1)):

            @pl.when(there)
            def _():
                pl.semaphore_signal(
                    ready.at[turn], inc=1, device_id=at(y, x, z + dz, c), device_id_type=MESH
                )

    def hear_sides(turn):
        pl.semaphore_wait(ready.at[turn], sides)

    def share_capacity():
        take_capacity.wait()
        for d in range(1, layers):
            send(
                caps[0].at[own_slab],
                caps[0].at[own_slab],
                c_send,
                c_recv.at[d],
                (m, lax.rem(s + 2 * d, slabs)),
            )
        forward_cap(0)

    def rows_from(d):
        return pl.ds(lax.rem(s + slabs - 2 * d, slabs) * thick, thick)

    def forward_cap(d):
        rows = rows_from(d)
        send(
            caps[0].at[rows],
            caps[0].at[rows],
            c_send,
            c_recv.at[0],
            at(y, x, z, 1 - c),
        )

    def power(ty):
        exponent = [rate ** (a * length // 2 + b * steps) for a in (0, 1) for b in (0, 1)]
        low = jnp.where(x == 0, jnp.float32(exponent[0]), jnp.float32(exponent[1]))
        high = jnp.where(x == 0, jnp.float32(exponent[2]), jnp.float32(exponent[3]))
        return jnp.where(ty == 0, low, high)

    here_power, there_power = power(y), power(1 - y)
    sign = jnp.where(y == 0, 1.0, -1.0).astype(jnp.float32)
    first_x = x == 0
    keep_own = jnp.where(first_x, here_power, sign * here_power)
    keep_far = jnp.where(first_x, there_power, -sign * there_power)
    give_own = jnp.where(first_x, sign * here_power, here_power)
    give_far = jnp.where(first_x, -sign * there_power, there_power)

    def combine(i):
        if i == 0:
            drain(loc, loc_recv)
        for k in range(PARTS):
            span = pl.ds(k * part_steps, part_steps)
            drain(far.at[i, span], far_recv.at[i, k])
            for t in range(k * part_steps, (k + 1) * part_steps):
                a, b = loc[i, t] * (rate**t), far[i, t] * (rate**t)
                sendx[i, t] = give_own * a + give_far * b
            send(
                sendx.at[i, span],
                seq.at[i, pl.ds(x * steps + k * part_steps, part_steps)],
                x_send,
                x_recv.at[i, k],
                at(y, 1 - x, z, 1 - c),
            )
            for t in range(k * part_steps, (k + 1) * part_steps):
                a, b = loc[i, t] * (rate**t), far[i, t] * (rate**t)
                seq[i, x * steps + t] = keep_own * a + keep_far * b

    in_layer = side != sig
    halo_y = jnp.where(in_layer, 1 - y, y)
    halo_z = jnp.where(in_layer, z, z + 2 * side - 1)
    halo_there = jnp.logical_or(in_layer, jnp.logical_and(halo_z >= 0, halo_z < layers))

    def transform(i):
        for k in range(PARTS):
            drain(sendx.at[i, pl.ds(0, part_steps)], x_recv.at[i, k])
        plane = jnp.where(side == 0, i, thick - 1 - i) + HALO

        @pl.when(x == 0)
        def _():
            modes = real_transform([seq[i, t] for t in range(2 * steps)])
            field[plane, 0, 0] = modes[0][0]
            field[plane, 0, 1] = modes[steps][0]
            for k in range(1, steps):
                field[plane, k, 0] = modes[k][0]
                field[plane, k, 1] = modes[k][1]

        @pl.when(x == 1)
        def _():
            modes = odd_transform([seq[i, t] for t in range(2 * steps)])
            for k in range(steps):
                field[plane, k, 0] = modes[k][0]
                field[plane, k, 1] = modes[k][1]

        given = field.at[plane, pl.ds((1 - c) * slots, slots)]
        send(given, given, d_send, d_recv, at(y, x, z, 1 - c))
        if i < HALO:
            target = plane + thick * (1 - 2 * side)

            @pl.when(halo_there)
            def _():
                for k in (0, 1):
                    part = pl.ds(k * slots, slots)
                    send(
                        field.at[plane, part],
                        field.at[target, part],
                        h_send,
                        h_recv.at[1 - side],
                        at(halo_y, x, halo_z, k),
                    )

    def shifts_of(slot):
        return tuple(table[slot, column] for column in range(3))

    even_row, even_lane = parity(tile, 0), parity(tile, 1)
    solver_shifts = shifts_of(x * 2 * slots + (1 - c) * slots + slab)

    def pass_capacity():
        for d in range(1, layers):
            drain(caps[0].at[rows_from(d)], c_recv.at[d])
            forward_cap(d)

    def coarse_tables():
        drain(caps[0].at[pl.ds(0, layers * thick)], c_recv.at[0])
        for level in range(1, depth):
            caps[level][...] = block_mean(caps[level - 1][...], 2 ** (level - 1))
            compact_table(level, caps[level], tables[level], solver_shifts, even_row)

    spread0, unused = level_coefficients(0)

    cap_base = (2 + sig) * thick - HALO

    def fine_tables():
        drain(near_cap.at[near_slab], n_recv.at[2])

        @pl.when(below)
        def _():
            drain(near_cap.at[near_slab], n_recv.at[0])

        @pl.when(above)
        def _():
            drain(near_cap.at[near_slab], n_recv.at[1])

        inside = [jnp.float32(1.0)] * wide
        for j in range(HALO):
            inside[j] = jnp.where(is_low, 0.0, 1.0).astype(jnp.float32)
            inside[wide - 1 - j] = jnp.where(is_high, 0.0, 1.0).astype(jnp.float32)

        def body(f, carry):
            s1, s2, s3 = shifts_of(x * 2 * slots + c * slots + f)
            for j in range(wide):
                cap = near_cap[cap_base + j]
                top, coupling = cap * s1 + 6.0 * spread0, cap * s2
                bottom = cap * s3 + 6.0 * spread0
                scale = (OMEGA * inside[j]) / (top * bottom + coupling * coupling)
                inverse0[f, j, 0] = bottom * scale
                inverse0[f, j, 1] = coupling * scale
                inverse0[f, j, 2] = top * scale
            return carry

        lax.fori_loop(0, slots, body, 0)

    for turn in range(layers - 1):
        tell_sides(turn)
        if turn > 0:
            combine(turn - 1)
        hear_sides(turn)
    share_capacity()
    for i in range(layers - 2, half - 1):
        combine(i)
    transform(0)
    combine(half - 1)
    for i in range(1, half):
        transform(i)
        if i == 1:
            fine_tables()
    pass_capacity()

    weights = neighbour_weights(0, tile)

    def slot_at(i):
        total, unit, rest_g, rest_i = 0, 1, slab, i
        while unit < slots:
            bit = lax.rem(lax.rem(rest_g, 2) + lax.rem(rest_i, 2), 2)
            total = total + unit * bit
            rest_g, rest_i = rest_g // 2, rest_i // 2
            unit *= 2
        return total

    def member(g):
        gz, gs = g // 2, lax.rem(g, 2)
        return at(lax.rem(gs + gz, 2), x, gz, 1 - c)

    given_planes = field.at[pl.ds(0, half), pl.ds(0, slots)]
    halo_planes = field.at[pl.ds(0, HALO), pl.ds(0, slots)]
    drain(given_planes, d_recv)
    for end, there in ((0, jnp.logical_not(is_low)), (1, jnp.logical_not(is_high))):

        @pl.when(there)
        def _():
            drain(halo_planes, h_recv.at[end])

    def load_inverse(f):
        return [[inverse0[f, j, k] for k in range(3)] for j in range(wide)]

    def residual_pair(forcing, second, j, shifts):
        s1, s2, s3 = shifts
        ahead, behind = weights[0]
        turned_sums = [0.0, 0.0]
        for k in (j, j + 1):
            re, im = second[k]
            cap = near_cap[cap_base + k]
            top, coupling, bottom = 6.0 * spread0 + cap * s1, cap * s2, 6.0 * spread0 + cap * s3
            turned_sums[0] = turned_sums[0] + (top * re - coupling * im)
            turned_sums[1] = turned_sums[1] + (coupling * re + bottom * im)
        found = []
        for part in (0, 1):
            near = [second[k][part] for k in (j - 1, j, j + 1, j + 2)]
            total = ahead * (near[2] + near[3]) + behind * (near[0] + near[1])
            total = total + around(near[1] + near[2], weights) + turned_sums[part]
            found.append(forcing[j][part] + forcing[j + 1][part] - total)
        return found

    def down(i, carry):
        chosen = [slot_at(slots - 1 - TOGETHER * i - k) for k in range(TOGETHER)]
        forcings = [
            [(field[j, c * slots + f, 0], field[j, c * slots + f, 1]) for j in range(wide)]
            for f in chosen
        ]
        inverses = [load_inverse(f) for f in chosen]
        shifts = [shifts_of(x * 2 * slots + c * slots + f) for f in chosen]
        first = [[] for f in chosen]
        second = [[None] for f in chosen]
        for j in range(wide):
            for n, f in enumerate(chosen):
                (re, im), (a, b, d) = forcings[n][j], inverses[n][j]
                first[n].append((a * re + b * im, d * im - b * re))
                for part in (0, 1):
                    vone[j, f, part] = first[n][j][part]
        for j in range(1, wide - 1):
            for n, f in enumerate(chosen):
                second[n].append(
                    smoothed(first[n][j], first[n][j - 1 : j + 2], inverses[n][j], weights)
                )
                for part in (0, 1):
                    vtwo[j, f, part] = second[n][j][part]
        for pair in range(thick // 4):
            packed = [[None, None] for f in chosen]
            for plane in (0, 1):
                for n, f in enumerate(chosen):
                    j = HALO + 4 * pair + 2 * plane
                    packed[n][plane] = residual_pair(forcings[n], second[n], j, shifts[n])
            for n, f in enumerate(chosen):
                coarse_out[f, pair] = 0.125 * pack_means(*packed[n], even_row, even_lane)

        tiles = pl.ds(slab * (thick // 4), thick // 4)
        for f in chosen:
            send(coarse_out.at[f], gathered.at[tiles], g_send, g_recv, member(f))

        return carry

    for turn in range(slots // TOGETHER):
        down(turn, 0)

    low_y, low_z = jnp.where(sig == 0, y, 1 - y), jnp.where(sig == 0, z - 1, z)
    high_y, high_z = jnp.where(sig == 0, 1 - y, y), jnp.where(sig == 0, z, z + 1)

    @pl.when(jnp.logical_not(is_low))
    def _():
        send(
            vtwo.at[HALO + 1], vtwo.at[wide - 1], e_send.at[0], e_recv.at[1], at(low_y, x, low_z, c)
        )

    @pl.when(jnp.logical_not(is_high))
    def _():
        send(
            vtwo.at[wide - HALO - 2], vtwo.at[0], e_send.at[1], e_recv.at[0],
            at(high_y, x, high_z, c),
        )

    coarse_tables()
    drain(gathered, g_recv)
    tiles_in = slabs * thick // 4
    unpacked = []
    for j in range(tiles_in):
        cells = gathered[j]
        re = jnp.where(even_lane, cells, shifted(cells, 1, 1))
        im = jnp.where(even_lane, shifted(cells, -1, 1), cells)
        unpacked.append((re, im))
    coarse = compact_cycle(1, unpacked, tables, solver_shifts, even_row)
    packed_cells = [jnp.where(even_lane, re, im) for re, im in coarse]
    empty = jnp.zeros(tile, jnp.float32)
    for j in range(tiles_in + 1):
        back[j] = jnp.where(
            even_row,
            packed_cells[j] if j < tiles_in else empty,
            packed_cells[j - 1] if j > 0 else empty,
        )
    span = thick // 4 + 1

    def give(i, carry):
        g = slot_at(slots - 1 - i)
        send(
            back.at[pl.ds(g * (thick // 4), span)], edges.at[slab], b_send, b_recv.at[slab],
            member(g),
        )
        return carry

    for turn in range(slots):
        give(turn, 0)

    for end, there in ((0, jnp.logical_not(is_low)), (1, jnp.logical_not(is_high))):

        @pl.when(there)
        def _():
            drain(vtwo.at[0], e_recv.at[end])
            drain(vtwo.at[0], e_send.at[end])

    def up(i, carry):
        chosen = [slot_at(TOGETHER * i + k) for k in range(TOGETHER)]
        for f in chosen:
            drain(edges.at[0], b_recv.at[f])

        inverses = [load_inverse(f) for f in chosen]
        start = [[] for f in chosen]
        third = [[None] for f in chosen]
        for k in range(span):
            for n, f in enumerate(chosen):
                for u, extra in enumerate(unpack_cells(edges[f, k], even_row, even_lane)[::-1]):
                    for j in (4 * k + 2 * u, 4 * k + 2 * u + 1):
                        start[n].append([vtwo[j, f, part] + extra[part] for part in (0, 1)])
        for j in range(1, wide - 1):
            for n, f in enumerate(chosen):
                first = (vone[j, f, 0], vone[j, f, 1])
                third[n].append(smoothed(first, start[n][j - 1 : j + 2], inverses[n][j], weights))
        for j in range(HALO, wide - HALO):
            for n, f in enumerate(chosen):
                first = (vone[j, f, 0], vone[j, f, 1])
                parts = smoothed(first, third[n][j - 1 : j + 2], inverses[n][j], weights)
                for part in (0, 1):
                    result[f, j - HALO, part] = parts[part]
        for f in chosen:
            q = c * slots + f
            send(
                result.at[f, pl.ds((1 - side) * half, half)], merged.at[q], r_send, r_recv,
                at(y, x, z, 1 - c),
            )
            for k in range(half):
                merged[q, k] = result[f, side * half + k]
        return carry

    lax.fori_loop(0, slots // TOGETHER, up, 0)
    drain(merged.at[pl.ds(0, slots)], r_recv)

    def invert(i):
        @pl.when(x == 0)
        def _():
            modes = [(merged[0, i, 0], None)]
            modes += [(merged[k, i, 0], merged[k, i, 1]) for k in range(1, steps)]
            modes += [(merged[0, i, 1], None)]
            for t, value in enumerate(real_inverse(modes)):
                wave[i, t] = value

        @pl.when(x == 1)
        def _():
            modes = [(merged[k, i, 0], merged[k, i, 1]) for k in range(steps)]
            for t, value in enumerate(odd_inverse(modes)):
                wave[i, t] = value

        for k in range(PARTS):
            send(
                wave.at[i, pl.ds((1 - x) * steps + k * part_steps, part_steps)],
                gotb.at[i, pl.ds(k * part_steps, part_steps)], w_send, w_recv.at[i, k],
                at(y, 1 - x, z, 1 - c),
            )

    inverse_here = 1.0 / (here_power * length)
    inverse_there = 1.0 / (there_power * length)
    own_sign = jnp.where(first_x, 1.0, sign).astype(jnp.float32)
    got_sign = jnp.where(first_x, sign, 1.0).astype(jnp.float32)
    far_own = jnp.where(first_x, 1.0, -sign).astype(jnp.float32)
    far_got = jnp.where(first_x, -sign, 1.0).astype(jnp.float32)

    def finish(i, k):
        span = pl.ds(k * part_steps, part_steps)
        drain(gotb.at[i, span], w_recv.at[i, k])
        p = side * half + i
        for t in range(k * part_steps, (k + 1) * part_steps):
            mine = wave[i, x * steps + t] * (rate**-t)
            got = gotb[i, t] * (rate**-t)
            outgoing[1, i, t] = (far_own * inverse_there) * mine + (far_got * inverse_there) * got
        send(
            outgoing.at[1, i, span], out_ref.at[span, p], o_send.at[1], o_recv,
            at(1 - y, x, z, sig),
        )

        def own_value(t):
            mine = wave[i, x * steps + t] * (rate**-t)
            got = gotb[i, t] * (rate**-t)
            return (own_sign * inverse_here) * mine + (got_sign * inverse_here) * got

        @pl.when(keeper)
        def _():
            for t in range(k * part_steps, (k + 1) * part_steps):
                out_ref[t, p] = own_value(t)

        @pl.when(jnp.logical_not(keeper))
        def _():
            for t in range(k * part_steps, (k + 1) * part_steps):
                outgoing[0, i, t] = own_value(t)
            send(
                outgoing.at[0, i, span], out_ref.at[span, p], o_send.at[0], o_recv,
                at(y, x, z, 1 - c),
            )

    for i in range(half):
        invert(i)
    for i in range(half):
        for k in range(PARTS):
            finish(i, k)

    @pl.when(keeper)
    def _():
        drain(loc, o_recv)
        drain(loc, loc_send)

    @pl.when(jnp.logical_not(keeper))
    def _():
        drain(res, o_recv)
        drain(res, far_send)
        drain(loc, o_send.at[0])

    drain(loc, o_send.at[1])
    drain(loc, x_send)
    drain(loc, w_send)
    drain(given_planes, d_send)

    @pl.when(halo_there)
    def _():
        drain(field.at[pl.ds(0, 2 * HALO), pl.ds(0, slots)], h_send)

    drain(gathered, g_send)
    drain(edges, b_send)
    drain(merged.at[pl.ds(0, slots)], r_send)
    drain(near_cap.at[near_slab], n_send.at[0])

    @pl.when(near_there)
    def _():
        drain(near_cap.at[pl.ds(0, 2 * thick)], n_send.at[1])

    drain(caps[0].at[pl.ds(0, (2 * layers - 1) * thick)], c_send)


def level_extents(extent):
    return [extent // 2**level for level in range(GRID_DEPTH)]


def fused(groups, slabs, residual, capacity):
    steps, thick, second, third = residual.shape
    length = groups * steps
    half, slots = thick // 2, steps // 2
    extent, wide = slabs * thick, thick + 2 * HALO
    tile = (second, third)
    ratio_step = ALPHA_CORNER ** (1.0 / length)
    numbers = [2 * k for k in range(steps)] + [4 * k + 1 for k in range(steps)]
    angle = 2.0 * np.pi / length * np.array(numbers)
    table = np.stack(
        [
            (1.0 - ratio_step * np.cos(angle)) / STEP_SIZE,
            ratio_step * np.sin(angle) / STEP_SIZE,
            (1.0 - ratio_step * np.cos(angle)) / STEP_SIZE,
        ],
        axis=1,
    )
    table[0, 1], table[0, 2] = 0.0, (1.0 + ratio_step) / STEP_SIZE
    extents = level_extents(extent)
    vmem = lambda *shape: pltpu.VMEM(shape + tile, jnp.float32)
    sems = lambda *shape: pltpu.SemaphoreType.DMA(shape)
    one = pltpu.SemaphoreType.DMA
    layers, quarter = slabs // 2, thick // 4
    scratch = [
        vmem(steps, thick),
        vmem(half, steps),
        vmem(half, steps),
        vmem(half, 2 * steps),
        vmem(half, steps),
        vmem(wide, 2 * slots, 2),
        vmem(slots, wide, 3),
        vmem(wide, slots, 2),
        vmem(wide, slots, 2),
        vmem(slots, quarter),
        vmem(slabs * quarter),
        vmem(slabs * quarter + 1),
        vmem(slots, quarter + 1),
        vmem(slots, thick, 2),
        vmem(2 * slots, half, 2),
        vmem(half, 2 * steps),
        vmem(half, steps),
        vmem(2, half, steps),
        pltpu.SMEM(table.shape, jnp.float32),
        vmem(6 * thick),
        *[vmem(n) for n in extents],
        *[vmem(n // 2, 4) for n in extents[1:]],
        sems(3),
        one,
        sems(half, PARTS),
        one,
        one,
        one,
        sems(half, PARTS),
        one,
        one,
        one,
        sems(2),
        sems(2),
        sems(2),
        one,
        one,
        one,
        sems(slots),
        one,
        one,
        one,
        sems(half, PARTS),
        sems(2),
        one,
        one,
        sems(layers),
        sems(2),
        sems(3),
        pltpu.SemaphoreType.REGULAR((layers - 1,)),
    ]
    return pl.pallas_call(
        functools.partial(whole_kernel, groups, slabs, table),
        out_shape=jax.ShapeDtypeStruct(residual.shape, jnp.float32),
        in_specs=[
            pl.BlockSpec(memory_space=pltpu.HBM),
            pl.BlockSpec(memory_space=pltpu.HBM),
        ],
        out_specs=pl.BlockSpec(memory_space=pltpu.VMEM),
        scratch_shapes=scratch,
        compiler_params=pltpu.CompilerParams(
            collective_id=0, has_side_effects=True, vmem_limit_bytes=32 * 2**20
        ),
    )(*[pltpu.with_memory_space_constraint(a, pltpu.HBM) for a in (residual, capacity)])


def fits_fused(groups, slabs, residual):
    steps, thick, second, third = residual.shape
    length = groups * steps
    power = length & (length - 1) == 0
    return (
        power
        and groups == 4
        and slabs % 2 == 0
        and slabs == length // 8
        and thick == 8
        and all(n % 2 == 0 and n % n == 0 for n in level_extents(slabs * thick))
        and (second, third) == (8, 128)
    )


def either(residual, capacity):
    groups, slabs = lax.axis_size("tm"), lax.axis_size("space")
    if fits_fused(groups, slabs, residual):
        return fused(groups, slabs, residual, capacity)
    return on_device(residual, capacity)


def solution(mesh):
    return jax.shard_map(
        either,
        mesh=mesh,
        in_specs=(P("tm", "space", None, None), P("space", None, None)),
        out_specs=P("tm", "space", None, None),
        check_vma=False,
    )
```
